32 devices in a mesh: clients: 16 (over z, y, core), fsdp: 2 (over x).
Axes of the slice: x: 2, y: 2, z: 4, core: 2. Of those that a mesh axis runs over, the one named last changes fastest.
Arguments:
- token_ids: int32 [16, 1280], P('clients', 'fsdp'), may hold values from 0 to 16383
- target: bfloat16 [16, 1280, 768], P('clients', 'fsdp'), may hold values from -6 to 6
- embedding: bfloat16 [16384, 768], P(None, 'fsdp'), may hold values from -6 to 6
- norm_gain: float32 [768], replicated, may hold values from 0.1 to 1.9
- global_model: float32 [3, 768, 1024], P(None, 'fsdp', 'clients'), may hold values from -0.21875 to 0.21875
- global_control: float32 [3, 768, 1024], P(None, 'fsdp', 'clients'), may hold values from -140 to 140
- client_control: float32 [16, 3, 768, 1024], P('clients', None, 'fsdp'), may hold values from -150 to 150
- local_steps: int32 [16], replicated, may hold values from 1 to 2
- client_weight: int32 [16], replicated, may hold values from 1 to 4
Outputs:
- server_step: float32 [3, 768, 1024], P(None, 'fsdp', 'clients')
- server_control: float32 [3, 768, 1024], P(None, 'fsdp', 'clients')
- client_update: float32 [16, 3, 768, 1024], P('clients', None, 'fsdp')
The draws below stay inside these ranges and needn't reach their ends.
All inputs are finite; a program needn't handle non-finite values.
Results may differ from the reference program's by a relative error of at most 0.025.
Values may be sent and summed in bfloat16 or wider, within the bound.
A program may use at most 128 MiB of HBM per device.

```python
import math
import jax
import jax.numpy as jnp
import numpy as np
from jax import lax

D = 768
FF = 1024
VOCAB = 16384
LOCAL = 2
TOK_DEV = 640
GROUP_TOK = 1280
CLIENTS = 16
N_FSDP = 2


def control_common(key):
    row_key, col_key, jitter_key = jax.random.split(jax.random.fold_in(key, 7001), 3)
    lowest = 0.5
    highest = 2.0
    jitter = jax.random.truncated_normal(jitter_key, -4.0, 4.0, (3, D, FF), jnp.float32)
    row_scale = jnp.exp(jax.random.uniform(row_key, (1, D, 1), jnp.float32, math.log(lowest), math.log(highest)))
    col_scale = jnp.exp(jax.random.uniform(col_key, (1, 1, FF), jnp.float32, math.log(lowest), math.log(highest)))
    return 5.0 * row_scale * col_scale * jitter


def draw_global_control(key, part):
    return control_common(key)


def draw_client_control(key, part):
    common = control_common(key)
    drift_key, pair_key = jax.random.split(jax.random.fold_in(key, 7002), 2)
    drifts = 0.5 * jax.random.truncated_normal(drift_key, -4.0, 4.0, (CLIENTS, 3, D, FF), jnp.float32)
    pairing = jax.random.permutation(pair_key, CLIENTS)
    span_width = FF // CLIENTS
    owners = jnp.arange(FF) // span_width
    spike_factor = jnp.where(owners[None, :] == pairing[:, None], 4.0, 1.0).astype(jnp.float32)
    return common[None] + drifts * spike_factor[:, None, None, :]


def place_ends(values, own_key, low, largest):
    longest = values.shape.index(max(values.shape))
    spots = []
    for shift in (0, 1):
        where = [jax.random.randint(jax.random.fold_in(own_key, axis), (), 0, length) for axis, length in enumerate(values.shape)]
        where[longest] = (where[longest] + shift) % values.shape[longest]
        spots.append(tuple(where))
    return values.at[spots[0]].set(low).at[spots[1]].set(largest)


def block_scale(own_key, dims, shards, least, high):
    gain, own = 1.0, jax.random.fold_in(own_key, 6)
    for position, shards_of in shards:
        heights = jnp.exp(jax.random.uniform(jax.random.fold_in(own, position), (shards_of,), jnp.float32, least / len(shards), high / len(shards)))
        gain = gain * jnp.repeat(heights, dims[position] // shards_of).reshape([-1 if axis == position else 1 for axis in range(len(dims))])
    return gain


def rank_bounds(amount, slope):
    loads = [(1 << 20) // math.isqrt(standing ** slope) + 1 for standing in range(1, amount + 1)]
    spread = 1 + sum(loads) // (1 << 30)
    return np.cumsum(np.array([max(1, weight // spread) for weight in loads]))


def ranked_ids(stream_key, dims, number_of, lean):
    grid = rank_bounds(number_of, lean)
    lot = jax.random.randint(jax.random.fold_in(stream_key, 1), dims, 0, int(grid[number_of - 1]))
    grade = jnp.searchsorted(jnp.asarray(grid, jnp.int32), lot, side="right")
    return jax.random.permutation(jax.random.fold_in(stream_key, 2), number_of)[grade].astype(jnp.int32)


def centred(rng, dims, spread, reach, cuts=(), held_as=jnp.bfloat16):
    array = spread * jax.random.normal(rng, dims, jnp.float32)
    if cuts:
        array = array * block_scale(rng, dims, cuts, -0.22, 0.18)
    return jnp.clip(array, -reach, reach).astype(held_as)


def setup_inputs(seed: int = 0) -> dict:
    arg_keys = jax.random.split(jax.random.key(seed), 10)
    token_ids = place_ends(ranked_ids(arg_keys[0], (CLIENTS, GROUP_TOK), VOCAB, 2), jax.random.fold_in(arg_keys[0], 3), 0, VOCAB - 1).astype(jnp.int32)
    target = centred(arg_keys[1], (CLIENTS, GROUP_TOK, D), 1.0, 6.0, ((0, 16), (1, 2)))
    embedding = centred(arg_keys[2], (VOCAB, D), 1.0, 6.0, ((1, 2),))
    norm_gain = jnp.clip(1.0 + 0.18 * jax.random.normal(arg_keys[3], (D,), jnp.float32), 0.1, 1.9)
    global_model = centred(arg_keys[4], (3, D, FF), D ** -0.5, 0.21875, ((1, 2), (2, 16)), jnp.float32)
    global_control = draw_global_control(jax.random.fold_in(arg_keys[9], 71), 0)
    client_control = draw_client_control(jax.random.fold_in(arg_keys[9], 71), 0)
    local_steps = place_ends(jax.random.randint(arg_keys[7], (CLIENTS,), 1, LOCAL + 1), jax.random.fold_in(arg_keys[7], 1), 1, LOCAL).astype(jnp.int32)
    client_weight = place_ends(jax.random.randint(arg_keys[8], (CLIENTS,), 1, 5), jax.random.fold_in(arg_keys[8], 1), 1, 4).astype(jnp.int32)
    return {"token_ids": token_ids, "target": target, "embedding": embedding, "norm_gain": norm_gain, "global_model": global_model, "global_control": global_control, "client_control": client_control, "local_steps": local_steps, "client_weight": client_weight}


learning_rate = 0.005
norm_eps = 1e-06

def gelu_pair(pre_act):
    return jax.vjp(lambda inputs: jax.nn.gelu(inputs, approximate=True), pre_act)

def shard_grads(normed, embedded, target, current, loss_scale):
    gate_pre = jnp.dot(normed, current[0], preferred_element_type=jnp.float32)
    up_pre = jnp.dot(normed, current[1], preferred_element_type=jnp.float32)
    gate_act, gelu_back = gelu_pair(gate_pre)
    hidden = (gate_act * up_pre).astype(jnp.bfloat16)
    projected = lax.dot_general(hidden, current[2], (((1,), (1,)), ((), ())), preferred_element_type=jnp.float32)
    out_grad = ((embedded.astype(jnp.float32) + projected - target.astype(jnp.float32)) * loss_scale).astype(jnp.bfloat16)
    grad_outer = lax.dot_general(out_grad, hidden, (((0,), (0,)), ((), ())), preferred_element_type=jnp.float32)
    hidden_grad = jnp.dot(out_grad, current[2], preferred_element_type=jnp.float32)
    gate_grad = gelu_back(hidden_grad * up_pre)[0].astype(jnp.bfloat16)
    up_grad = (hidden_grad * gate_act).astype(jnp.bfloat16)
    grad_gate = lax.dot_general(normed, gate_grad, (((0,), (0,)), ((), ())), preferred_element_type=jnp.float32)
    grad_up = lax.dot_general(normed, up_grad, (((0,), (0,)), ((), ())), preferred_element_type=jnp.float32)
    return jnp.stack([grad_gate, grad_up, grad_outer])

def client_round(inputs, embedding, norm_gain, global_model, global_control):
    ids_row, target_rows, own_control, step_count = inputs
    embedded = jnp.take(embedding, ids_row, axis=0)
    widened = embedded.astype(jnp.float32)
    inv_norm = lax.rsqrt(lax.optimization_barrier(jnp.mean(widened * widened, axis=1, keepdims=True)) + norm_eps)
    normed = (widened * inv_norm * norm_gain).astype(jnp.bfloat16)
    loss_scale = 1.0 / math.sqrt(TOK_DEV * N_FSDP)
    shard_normed = normed.reshape(N_FSDP, TOK_DEV, -1)
    shard_embedded = embedded.reshape(N_FSDP, TOK_DEV, -1)
    shard_target = target_rows.reshape(N_FSDP, TOK_DEV, -1)
    correction = global_control - own_control
    pseudo = jnp.zeros(global_model.shape, jnp.float32)
    for local_step in range(LOCAL):
        current = (global_model - learning_rate * pseudo).astype(jnp.bfloat16)

        def add_shard(running, pieces):
            term = shard_grads(pieces[0], pieces[1], pieces[2], current, loss_scale)
            rounded = lax.optimization_barrier(term.astype(jnp.bfloat16))
            return (running + rounded.astype(jnp.float32), None)
        grads, _ = lax.scan(add_shard, jnp.zeros(global_model.shape, jnp.float32), (shard_normed, shard_embedded, shard_target))
        step_mask = (local_step < step_count).astype(jnp.float32)
        pseudo = pseudo + step_mask * (grads + correction)
    update = own_control - global_control + pseudo / step_count.astype(jnp.float32)
    return (pseudo, update)

def reference(token_ids, target, embedding, norm_gain, global_model, global_control, client_control, local_steps, client_weight):

    def one_client(inputs):
        return client_round(inputs, embedding, norm_gain, global_model, global_control)
    pseudo_all, client_update = lax.map(one_client, (token_ids, target, client_control, local_steps))
    weights = client_weight.astype(jnp.float32)
    weight_total = jnp.sum(weights)
    server_step = lax.optimization_barrier(jnp.sum(weights[:, None, None, None] * pseudo_all, axis=0)) / weight_total
    server_control = lax.optimization_barrier(jnp.sum(weights[:, None, None, None] * client_update, axis=0)) / weight_total
    return (server_step, server_control, client_update)
```

```python
import functools
import math

import jax
import jax.numpy as jnp
from jax import lax
from jax.experimental import pallas as pl
from jax.experimental.pallas import tpu as pltpu
from jax.sharding import PartitionSpec as P

LOCAL = 2


learning_rate = 0.005
norm_eps = 1e-06


def gelu_pair(pre_act):
    return jax.vjp(lambda inputs: jax.nn.gelu(inputs, approximate=True), pre_act)


def contract_rows(left, right):
    return lax.dot_general(
        left, right, (((0,), (0,)), ((), ())), preferred_element_type=jnp.float32
    )


def pack_owners(array, owners):
    parts, rows, columns = array.shape
    width = columns // owners
    split = array.reshape(parts, 2, rows // 2, owners, width)
    return split.transpose(3, 0, 2, 1, 4).reshape(owners, parts, rows // 2, 2 * width)


def unpack_owner(array):
    parts, half, width = array.shape
    split = array.reshape(parts, half, 2, width // 2)
    return split.transpose(0, 2, 1, 3).reshape(parts, 2 * half, width // 2)


def general_body(
    token_ids,
    target,
    embedding,
    norm_gain,
    global_model,
    global_control,
    client_control,
    local_steps,
    client_weight,
):
    n_clients = lax.axis_size("clients")
    n_fsdp = lax.axis_size("fsdp")
    client_index = lax.axis_index("clients")
    fsdp_index = lax.axis_index("fsdp")
    paired = n_fsdp == 2 and n_clients % 2 == 0
    if paired:
        core = client_index % 2
        role_client = client_index - core + fsdp_index
        block = core
        swap_pairs = [
            (c * 2 + f, ((c - c % 2) + f) * 2 + c % 2) for c in range(n_clients) for f in range(2)
        ]
        core_pairs = [(c, c ^ 1) for c in range(n_clients)]
    else:
        role_client = client_index
        block = fsdp_index

    def swap_roles(array):
        if not paired:
            return array
        return lax.ppermute(array, ("clients", "fsdp"), swap_pairs)

    def gather_rows(array):
        if not paired:
            return lax.all_gather(array, "fsdp", axis=0, tiled=True)
        other = lax.ppermute(array, "clients", core_pairs)
        return jnp.concatenate(
            [jnp.where(core == 0, array, other), jnp.where(core == 0, other, array)], axis=0
        )

    def reduce_rows(term):
        if not paired:
            return lax.psum_scatter(term, "fsdp", scatter_dimension=0, tiled=True).astype(
                jnp.float32
            )
        rows = term.shape[0] // 2
        own = lax.dynamic_slice_in_dim(term, core * rows, rows, axis=0)
        sent = lax.dynamic_slice_in_dim(term, (1 - core) * rows, rows, axis=0)
        received = lax.ppermute(sent, "clients", core_pairs)
        return own.astype(jnp.float32) + received.astype(jnp.float32)

    tok_rows = target.shape[1]
    group_rows = tok_rows * n_fsdp
    loss_scale = 1.0 / math.sqrt(group_rows)
    all_ids = lax.all_gather(swap_roles(token_ids), "fsdp", axis=1, tiled=True)
    emb_columns = jnp.take(embedding, all_ids[0], axis=0)
    embedded = lax.all_to_all(emb_columns, "fsdp", split_axis=0, concat_axis=1, tiled=True)
    widened = embedded.astype(jnp.float32)
    inv_norm = lax.rsqrt(jnp.mean(widened * widened, axis=1, keepdims=True) + norm_eps)
    normed = (widened * inv_norm * norm_gain).astype(jnp.bfloat16)
    target_rows = swap_roles(target[0]).astype(jnp.float32)
    model_columns = lax.all_gather(
        global_model.astype(jnp.bfloat16), "fsdp", axis=1, tiled=True
    )
    model_full = lax.all_gather(model_columns, "clients", axis=2, tiled=True)
    control_rows = lax.all_gather(
        global_control.astype(jnp.bfloat16), "clients", axis=2, tiled=True
    ).astype(global_control.dtype)
    slots = jnp.arange(local_steps.shape[0])
    step_count = jnp.sum(jnp.where(slots == client_index, local_steps, 0))
    role_steps = jnp.sum(jnp.where(slots == role_client, local_steps, 0))
    own_weight = jnp.sum(jnp.where(slots == client_index, client_weight, 0)).astype(jnp.float32)
    weight_total = jnp.sum(client_weight).astype(jnp.float32)
    correction = control_rows - client_control[0]
    parts, rows = correction.shape[0], correction.shape[1]
    role_correction = [
        swap_roles(correction[part].astype(jnp.bfloat16)).astype(jnp.float32)
        for part in range(parts)
    ]
    role_model = lax.dynamic_slice_in_dim(model_full, block * rows, rows, axis=1).astype(
        jnp.float32
    )
    gathered = [model_full[part] for part in range(parts)]
    pseudo = [jnp.zeros_like(role_correction[part]) for part in range(parts)]
    summed = [jnp.zeros_like(role_correction[part]) for part in range(parts)]
    for local_step in range(LOCAL):
        if local_step > 0:
            gathered = [
                gather_rows(
                    (role_model[part] - learning_rate * pseudo[part]).astype(jnp.bfloat16)
                )
                for part in range(parts)
            ]
        gate_pre = jnp.dot(normed, gathered[0], preferred_element_type=jnp.float32)
        up_pre = jnp.dot(normed, gathered[1], preferred_element_type=jnp.float32)
        gate_act, gelu_back = gelu_pair(gate_pre)
        hidden = (gate_act * up_pre).astype(jnp.bfloat16)
        projected = lax.dot_general(
            hidden, gathered[2], (((1,), (1,)), ((), ())), preferred_element_type=jnp.float32
        )
        out_grad = ((widened + projected - target_rows) * loss_scale).astype(jnp.bfloat16)
        outer_term = contract_rows(out_grad, hidden).astype(jnp.bfloat16)
        hidden_grad = jnp.dot(out_grad, gathered[2], preferred_element_type=jnp.float32)
        gate_grad = gelu_back(hidden_grad * up_pre)[0].astype(jnp.bfloat16)
        up_grad = (hidden_grad * gate_act).astype(jnp.bfloat16)
        gate_term = contract_rows(normed, gate_grad).astype(jnp.bfloat16)
        up_term = contract_rows(normed, up_grad).astype(jnp.bfloat16)
        grads = [reduce_rows(term) for term in (gate_term, up_term, outer_term)]
        step_mask = (local_step < role_steps).astype(jnp.float32)
        for part in range(parts):
            pseudo[part] = pseudo[part] + step_mask * (grads[part] + role_correction[part])
            summed[part] = summed[part] + step_mask * grads[part]
    own_grads = jnp.stack(
        [swap_roles(summed[part].astype(jnp.bfloat16)).astype(jnp.float32) for part in range(parts)]
    )
    taken = jnp.sum((jnp.arange(LOCAL) < step_count).astype(jnp.float32))
    own_pseudo = own_grads + taken * correction
    update = client_control[0] - control_rows + own_pseudo / step_count.astype(jnp.float32)
    packed = jnp.concatenate(
        [
            pack_owners((own_weight * own_pseudo).astype(jnp.bfloat16), n_clients),
            pack_owners((own_weight * update).astype(jnp.bfloat16), n_clients),
        ],
        axis=1,
    )
    sums = lax.psum_scatter(packed, "clients", scatter_dimension=0, tiled=True)[0]
    sums = unpack_owner(sums).astype(jnp.float32) / weight_total
    return (sums[:parts], sums[parts:], update[None])


MESH = pl.DeviceIdType.MESH
TILE = 256
BF = jnp.bfloat16
F32 = jnp.float32


def gelu_parts(x):
    cubic = 0.044715
    scale = math.sqrt(2.0 / math.pi)
    square = x * x
    t = jnp.tanh(scale * x * (1.0 + cubic * square))
    half = 0.5 * (1.0 + t)
    slope = half + (0.5 * scale) * x * (1.0 - t * t) * (1.0 + (3.0 * cubic) * square)
    return x * half, slope


def dot(left, right, left_dim=1, right_dim=0):
    return lax.dot_general(
        left, right, (((left_dim,), (right_dim,)), ((), ())), preferred_element_type=F32
    )


def round_kernel(
    n_pos,
    steps_ref,
    weights_ref,
    emb_ref,
    target_ref,
    gain_ref,
    model_ref,
    control_ref,
    own_ref,
    step_out,
    control_out,
    grad_out,
    packed,
    packed_in,
    model,
    current,
    g_rows,
    c_rows,
    corr,
    role_corr,
    sa_in,
    sa_out,
    sa_tiles,
    emb,
    target,
    normed,
    normed_t,
    act,
    slope_up,
    hidden,
    out_grad,
    out_grad_t,
    gate_grad,
    up_grad,
    term_out,
    term_own,
    term_in,
    tiles,
    sums_out,
    sums_in,
    final,
    final_in,
    local_sem,
    send_sem,
    recv_sem,
):
    parts, half, width = own_ref.shape
    rows = emb.shape[0]
    span = width // n_pos
    owner_span = span // 2
    n_other = n_pos - 1
    client = lax.axis_index("clients")
    x = lax.axis_index("fsdp")
    b = lax.rem(client, 2)
    p = client // 2
    home = b == x
    away = b != x
    role_client = 2 * p + x
    half_at = pl.multiple_of(b * half, half)
    other_at = pl.multiple_of((1 - b) * half, half)
    own_rows = pl.ds(half_at, half)
    other_rows = pl.ds(other_at, half)

    partner = {"clients": 2 * p + 1 - b, "fsdp": x}
    across = {"clients": client, "fsdp": 1 - x}
    swap = {"clients": 2 * p + 1 - b, "fsdp": 1 - x}

    def position(offset):
        return lax.rem(p + offset, n_pos)

    def plane(offset):
        return {"clients": 2 * position(offset) + b, "fsdp": x}

    def columns(pos):
        return pl.ds(pl.multiple_of(pos * span, span), span)

    counts = dict(
        pack=1, emb=1, target=1, cross=1, model=n_pos, g=n_pos, gfwd=n_pos, mfwd=n_pos,
        corr=parts, sain=parts, sa=n_pos, term0=parts, term1=parts, cur=parts, ret=parts,
        grad=n_pos * parts, sums=parts, final=1,
    )
    base = {}
    total = 0
    for name, count in counts.items():
        base[name] = total
        total += count

    def remote(src, dst, name, index, device):
        k = base[name] + index
        return pltpu.make_async_remote_copy(
            src_ref=src, dst_ref=dst, send_sem=send_sem.at[k], recv_sem=recv_sem.at[k],
            device_id=device, device_id_type=MESH,
        )

    def pack_copy():
        return remote(packed, packed_in, "pack", 0, partner)

    def emb_copy():
        return remote(
            emb_ref.at[pl.ds(rows, rows), :],
            emb.at[:, pl.ds(pl.multiple_of(x * half, half), half)],
            "emb", 0, across,
        )

    def target_copy():
        return remote(target_ref, target, "target", 0, swap)

    def model_window(row_window, pos):
        return model.at[:, row_window, columns(pos)]

    def cross_copy():
        window = model_window(own_rows, p)
        return remote(window, window, "cross", 0, across)

    def model_copy(d):
        window = model_window(own_rows, p)
        return remote(window, window, "model", d, plane(d))

    def model_arrival(d):
        window = model_window(own_rows, position(n_pos - d))
        return remote(window, window, "model", d, plane(d))

    def g_window(pos):
        return g_rows.at[:, :, columns(pos)]

    def g_copy(d):
        return remote(g_window(p), g_window(p), "g", d, plane(d))

    def g_arrival(d):
        pos = position(n_pos - d)
        return remote(g_window(pos), g_window(pos), "g", d, plane(d))

    def g_forward(d):
        pos = position(n_pos - d)
        return remote(g_window(pos), g_window(pos), "gfwd", d, partner)

    def model_forward(d):
        window = model_window(own_rows, position(n_pos - d))
        return remote(window, window, "mfwd", d, partner)

    def corr_copy(part):
        return remote(corr.at[part], role_corr.at[part], "corr", part, swap)

    def sain_copy(part):
        return remote(sa_out.at[part], sa_in.at[part], "sain", part, partner)

    def sa_copy(d):
        return remote(
            sa_out.at[:, :, columns(position(d))], sa_tiles.at[p], "sa", d, plane(d)
        )

    def sa_arrival(d):
        return remote(
            sa_out.at[:, :, columns(position(d))], sa_tiles.at[position(n_pos - d)],
            "sa", d, plane(d),
        )

    def term_copy(step, part):
        return remote(
            term_out.at[part], term_in.at[step, part], "term%d" % step, part, partner
        )

    def current_copy(part):
        window = current.at[part, own_rows, :]
        return remote(window, window, "cur", part, partner)

    def return_copy(part):
        return remote(role_corr.at[part], g_rows.at[part], "ret", part, swap)

    def grad_copy(d, part):
        return remote(
            role_corr.at[part, :, columns(position(d))], tiles.at[p, part],
            "grad", d * parts + part, plane(d),
        )

    def grad_arrival(d, part):
        pos = position(n_pos - d)
        return remote(
            role_corr.at[part, :, columns(position(d))], tiles.at[pos, part],
            "grad", d * parts + part, plane(d),
        )

    def sums_copy(part):
        return remote(sums_out.at[part], sums_in.at[part], "sums", part, across)

    def final_copy():
        return remote(final, final_in, "final", 0, partner)

    barrier = pltpu.get_barrier_semaphore()
    peers = [partner, across, swap] + [plane(d) for d in range(1, n_pos)]
    for peer in peers:
        pl.semaphore_signal(barrier, inc=1, device_id=peer, device_id_type=MESH)
    pl.semaphore_wait(barrier, len(peers))

    own_load = pltpu.make_async_copy(own_ref, c_rows, local_sem.at[0])
    emb_load = pltpu.make_async_copy(
        emb_ref.at[pl.ds(0, rows), :],
        emb.at[:, pl.ds(pl.multiple_of(x * half, half), half)],
        local_sem.at[1],
    )
    target_load = pltpu.make_async_copy(target_ref, target, local_sem.at[2])
    own_load.start()
    emb_load.start()

    packed[...] = jnp.concatenate(
        [model_ref[...].astype(BF), control_ref[...].astype(BF)], axis=-1
    )

    @pl.when(away)
    def _():
        pack_copy().start()
        emb_copy().start()
        target_copy().start()
        cross_copy().wait_recv()
        for d in range(1, n_pos):
            model_copy(d).start()

    @pl.when(home)
    def _():
        target_load.start()
        pack_copy().wait_recv()
        mine = packed[...]
        theirs = packed_in[...]
        first = jnp.where(b == 0, mine, theirs)
        second = jnp.where(b == 0, theirs, mine)
        model[:, own_rows, columns(p)] = jnp.concatenate(
            [first[:, :, :owner_span], second[:, :, :owner_span]], axis=-1
        )
        g_rows[:, :, columns(p)] = jnp.concatenate(
            [first[:, :, owner_span:], second[:, :, owner_span:]], axis=-1
        )
        cross_copy().start()
        for d in range(1, n_pos):
            g_copy(d).start()
        emb_copy().start()
        for d in range(1, n_pos):
            model_copy(d).start()
        g_forward(0).start()
        for d in range(1, n_pos):
            g_arrival(d).wait_recv()
            g_forward(d).start()

    model_forward(0).start()
    own_load.wait()

    @pl.when(away)
    def _():
        for d in range(n_pos):
            g_forward(d).wait_recv()

    own_steps = steps_ref[client]
    own_scale = (weights_ref[client] * own_steps).astype(F32)
    chunk = half // 6

    for part in range(parts):

        def correct(i, carry):
            at = pl.ds(pl.multiple_of(i * chunk, chunk), chunk)
            value = g_rows[part, at, :].astype(F32) - c_rows[part, at, :]
            rounded = value.astype(BF)
            corr[part, at, :] = rounded
            sa_out[part, at, :] = (own_scale * value).astype(BF)
            return carry

        lax.fori_loop(0, 6, correct, 0)

        @pl.when(away)
        def _():
            corr_copy(part).start()
            sain_copy(part).start()

    @pl.when(home)
    def _():
        for part in range(parts):

            def place(i, carry):
                at = pl.ds(pl.multiple_of(i * chunk, chunk), chunk)
                role_corr[part, at, :] = corr[part, at, :]
                return carry

            lax.fori_loop(0, 6, place, 0)
            sain_copy(part).wait_recv()

            def merge(i, carry):
                at = pl.ds(pl.multiple_of(i * chunk, chunk), chunk)
                sa_out[part, at, :] = (
                    sa_out[part, at, :].astype(F32) + sa_in[part, at, :].astype(F32)
                ).astype(BF)
                return carry

            lax.fori_loop(0, 6, merge, 0)
        for d in range(1, n_pos):
            sa_copy(d).start()

    emb_load.wait()
    emb_copy().wait_recv()
    widened = emb[...].astype(F32)
    inv_norm = lax.rsqrt(jnp.mean(widened * widened, axis=1, keepdims=True) + norm_eps)
    normed[...] = (widened * inv_norm * gain_ref[...]).astype(BF)
    depth = 2 * half
    for at in range(0, depth, 128):
        normed_t[at : at + 128, :] = normed[:, at : at + 128].T

    for d in range(1, n_pos):
        model_arrival(d).wait_recv()
        model_forward(d).start()
    for d in range(n_pos):
        model_forward(d).wait_recv()

    loss_scale = 1.0 / math.sqrt(2 * rows)
    n_tiles = width // TILE

    def tile_at(j):
        return pl.ds(pl.multiple_of(j * TILE, TILE), TILE)

    def half_product(left, left_rows, right, store):
        def product(j, carry):
            store(j, dot(left[left_rows, :], right[:, tile_at(j)]).astype(BF))
            return carry

        lax.fori_loop(0, n_tiles, product, 0)

    def local_step(step, weights, finish):
        def forward(j, carry):
            cols = tile_at(j)
            gate_act, slope = gelu_parts(dot(normed[...], weights[0, :, cols]))
            up_pre = dot(normed[...], weights[1, :, cols])
            act[:, cols] = gate_act
            slope_up[:, cols] = slope * up_pre
            hidden[:, cols] = (gate_act * up_pre).astype(BF)
            return carry

        lax.fori_loop(0, n_tiles, forward, 0)
        if step == 0:

            @pl.when(away)
            def _():
                target_copy().wait_recv()

            @pl.when(home)
            def _():
                target_load.wait()

        def project(j, carry):
            cols = tile_at(j)
            projected = dot(hidden[...], weights[2, cols, :], 1, 1)
            value = (
                (emb[:, cols].astype(F32) + projected - target[:, cols].astype(F32)) * loss_scale
            ).astype(BF)
            out_grad[:, cols] = value
            out_grad_t[cols, :] = value.T
            return carry

        lax.fori_loop(0, depth // TILE, project, 0)

        def term(part, left, right):
            def store_out(j, value):
                term_out[part, :, tile_at(j)] = value

            def store_own(j, value):
                term_own[part, :, tile_at(j)] = value

            if step > 0:
                term_copy(step - 1, part).wait_send()
            half_product(left, other_rows, right, store_out)
            term_copy(step, part).start()
            half_product(left, own_rows, right, store_own)

        term(2, out_grad_t, hidden)

        def backward(j, carry):
            cols = tile_at(j)
            hidden_grad = dot(out_grad[...], weights[2, :, cols])
            gate_grad[:, cols] = (hidden_grad * slope_up[:, cols]).astype(BF)
            up_grad[:, cols] = (hidden_grad * act[:, cols]).astype(BF)
            return carry

        lax.fori_loop(0, n_tiles, backward, 0)
        finish(2)
        term(0, normed_t, gate_grad)
        term(1, normed_t, up_grad)
        finish(0)
        finish(1)

    def update(part):
        term_copy(0, part).wait_recv()

        @pl.when(away)
        def _():
            corr_copy(part).wait_recv()

        def apply(i, carry):
            at = pl.ds(pl.multiple_of(i * chunk, chunk), chunk)
            model_at = pl.ds(pl.multiple_of(half_at + i * chunk, chunk), chunk)
            grads = term_own[part, at, :].astype(F32) + term_in[0, part, at, :].astype(F32)
            c_rows[part, at, :] = grads
            pseudo = grads + role_corr[part, at, :].astype(F32)
            current[part, model_at, :] = (
                model[part, model_at, :].astype(F32) - learning_rate * pseudo
            ).astype(BF)
            return carry

        lax.fori_loop(0, 6, apply, 0)
        current_copy(part).start()

    second = (steps_ref[role_client] > 1).astype(F32)

    def collect(part):
        term_copy(1, part).wait_recv()

        def apply(i, carry):
            at = pl.ds(pl.multiple_of(i * chunk, chunk), chunk)
            grads = term_own[part, at, :].astype(F32) + term_in[1, part, at, :].astype(F32)
            role_corr[part, at, :] = (c_rows[part, at, :] + second * grads).astype(BF)
            return carry

        lax.fori_loop(0, 6, apply, 0)

        @pl.when(away)
        def _():
            return_copy(part).start()

        @pl.when(home)
        def _():
            pltpu.make_async_copy(
                role_corr.at[part], grad_out.at[part], local_sem.at[3 + part]
            ).start()

        for d in range(1, n_pos):
            grad_copy(d, part).start()

    local_step(0, model, update)
    for part in range(parts):
        current_copy(part).wait_recv()
    local_step(1, current, collect)

    for part in (2, 0, 1):
        for d in range(1, n_pos):
            grad_arrival(d, part).wait_recv()
        weighted = jnp.zeros((half, span), F32)
        averaged = jnp.zeros((half, span), F32)
        for d in range(n_pos):
            pos = position(d)
            index = 2 * pos + x
            value = (
                role_corr[part, :, columns(p)] if d == 0 else tiles[pos, part]
            ).astype(F32)
            weight = weights_ref[index].astype(F32)
            taken = steps_ref[index].astype(F32)
            scaled = weight * value
            weighted += scaled
            averaged += scaled / taken
        final[part, 0] = weighted
        final[part, 1] = averaged

        @pl.when(away)
        def _():
            sums_out[part] = final[part].astype(BF)
            sums_copy(part).start()

    @pl.when(home)
    def _():
        for d in range(1, n_pos):
            sa_arrival(d).wait_recv()
        for part in (2, 0, 1):
            sums_copy(part).wait_recv()
            shift = sa_out[part, :, columns(p)].astype(F32)
            for d in range(1, n_pos):
                shift += sa_tiles[position(d), part].astype(F32)
            final[part, 0] = final[part, 0] + sums_in[part, 0].astype(F32) + shift
            final[part, 1] = final[part, 1] + sums_in[part, 1].astype(F32)
        final_copy().start()

    @pl.when(away)
    def _():
        final_copy().wait_recv()

    n_clients = 2 * n_pos
    weight_total = weights_ref[0]
    step_total = weights_ref[0] * steps_ref[0]
    for i in range(1, n_clients):
        weight_total += weights_ref[i]
        step_total += weights_ref[i] * steps_ref[i]
    weight_total = weight_total.astype(F32)
    step_total = step_total.astype(F32)

    def write(source):
        whole = source[...]
        own = jnp.where(b == 0, whole[..., :owner_span], whole[..., owner_span:])
        control = control_ref[...]
        lost = control - control.astype(BF).astype(F32)
        step_out[...] = (own[:, 0] + step_total * lost) / weight_total
        control_out[...] = own[:, 1] / weight_total

    @pl.when(home)
    def _():
        write(final)

    @pl.when(away)
    def _():
        write(final_in)

    @pl.when(away)
    def _():
        pack_copy().wait_send()
        target_copy().wait_send()
        for part in range(parts):
            corr_copy(part).wait_send()
            sain_copy(part).wait_send()
        for part in (2, 0, 1):
            return_copy(part).wait_recv()
            pltpu.make_async_copy(
                g_rows.at[part], grad_out.at[part], local_sem.at[3 + part]
            ).start()
        for part in range(parts):
            return_copy(part).wait_send()
            sums_copy(part).wait_send()

    @pl.when(home)
    def _():
        cross_copy().wait_send()
        for d in range(n_pos):
            g_forward(d).wait_send()
        for d in range(1, n_pos):
            g_copy(d).wait_send()
            sa_copy(d).wait_send()
        final_copy().wait_send()

    emb_copy().wait_send()
    for d in range(1, n_pos):
        model_copy(d).wait_send()
    for d in range(n_pos):
        model_forward(d).wait_send()
    for part in range(parts):
        term_copy(1, part).wait_send()
        current_copy(part).wait_send()
        for d in range(1, n_pos):
            grad_copy(d, part).wait_send()
    for part in range(parts):
        pltpu.make_async_copy(
            role_corr.at[part], grad_out.at[part], local_sem.at[3 + part]
        ).wait()


def paired_body(
    token_ids,
    target,
    embedding,
    norm_gain,
    global_model,
    global_control,
    client_control,
    local_steps,
    client_weight,
):
    n_clients = lax.axis_size("clients")
    n_pos = n_clients // 2
    parts, half, owner_span = global_model.shape
    width = owner_span * n_clients
    span = 2 * owner_span
    rows = token_ids.shape[1]
    depth = 2 * half
    pairs = [(c, f) for c in range(n_clients) for f in range(2)]
    to_role = [(c * 2 + f, (c - c % 2 + f) * 2 + c % 2) for c, f in pairs]
    to_across = [(c * 2 + f, (c - c % 2 + f) * 2 + 1 - c % 2) for c, f in pairs]
    ids = jnp.concatenate(
        [
            lax.ppermute(token_ids[0], ("clients", "fsdp"), to_role),
            lax.ppermute(token_ids[0], ("clients", "fsdp"), to_across),
        ]
    )
    emb_columns = embedding.at[ids].get(mode="promise_in_bounds")

    n_sem = 5 + 5 * n_pos + 7 * parts + n_pos * parts
    vmem = pltpu.VMEM
    scratch = [
        vmem((parts, half, span), BF),
        vmem((parts, half, span), BF),
        vmem((parts, depth, width), BF),
        vmem((parts, depth, width), BF),
        vmem((parts, half, width), BF),
        vmem((parts, half, width), F32),
        vmem((parts, half, width), BF),
        vmem((parts, half, width), BF),
        vmem((parts, half, width), BF),
        vmem((parts, half, width), BF),
        vmem((n_pos, parts, half, span), BF),
        vmem((rows, depth), BF),
        vmem((rows, depth), BF),
        vmem((rows, depth), BF),
        vmem((depth, rows), BF),
        vmem((rows, width), F32),
        vmem((rows, width), F32),
        vmem((rows, width), BF),
        vmem((rows, depth), BF),
        vmem((depth, rows), BF),
        vmem((rows, width), BF),
        vmem((rows, width), BF),
        vmem((parts, half, width), BF),
        vmem((parts, half, width), BF),
        vmem((2, parts, half, width), BF),
        vmem((n_pos, parts, half, span), BF),
        vmem((parts, 2, half, span), BF),
        vmem((parts, 2, half, span), BF),
        vmem((parts, 2, half, span), F32),
        vmem((parts, 2, half, span), F32),
        pltpu.SemaphoreType.DMA((3 + parts,)),
        pltpu.SemaphoreType.DMA((n_sem,)),
        pltpu.SemaphoreType.DMA((n_sem,)),
    ]
    smem = pl.BlockSpec(memory_space=pltpu.SMEM)
    anywhere = pl.BlockSpec(memory_space=pl.ANY)
    inside = pl.BlockSpec(memory_space=pltpu.VMEM)
    step_sum, control_sum, grad_rows = pl.pallas_call(
        functools.partial(round_kernel, n_pos),
        out_shape=(
            jax.ShapeDtypeStruct((parts, half, owner_span), F32),
            jax.ShapeDtypeStruct((parts, half, owner_span), F32),
            jax.ShapeDtypeStruct((parts, half, width), BF),
        ),
        in_specs=[smem, smem, anywhere, anywhere, inside, inside, inside, anywhere],
        out_specs=(inside, inside, anywhere),
        scratch_shapes=scratch,
        compiler_params=pltpu.CompilerParams(
            collective_id=0, has_side_effects=True, vmem_limit_bytes=67043328
        ),
    )(
        local_steps,
        client_weight,
        emb_columns,
        target[0],
        norm_gain[None, :],
        global_model,
        global_control,
        client_control[0],
    )
    slots = jnp.arange(n_clients)
    own_steps = jnp.sum(jnp.where(slots == lax.axis_index("clients"), local_steps, 0))
    update = grad_rows.astype(F32) / own_steps.astype(F32)
    return (step_sum, control_sum, update[None])


def solution(mesh):
    placed = (
        P("clients", "fsdp"),
        P("clients", "fsdp", None),
        P(None, "fsdp"),
        P(),
        P(None, "fsdp", "clients"),
        P(None, "fsdp", "clients"),
        P("clients", None, "fsdp", None),
        P(),
        P(),
    )
    paired = mesh.shape["fsdp"] == 2 and mesh.shape["clients"] % 2 == 0
    return jax.shard_map(
        paired_body if paired else general_body,
        mesh=mesh,
        in_specs=placed,
        out_specs=(
            P(None, "fsdp", "clients"),
            P(None, "fsdp", "clients"),
            P("clients", None, "fsdp", None),
        ),
        check_vma=False,
    )
```

```python
import functools
import math

import jax
import jax.numpy as jnp
from jax import lax
from jax.experimental import pallas as pl
from jax.experimental.pallas import tpu as pltpu
from jax.sharding import PartitionSpec as P

LOCAL = 2


learning_rate = 0.005
norm_eps = 1e-06


def gelu_pair(pre_act):
    return jax.vjp(lambda inputs: jax.nn.gelu(inputs, approximate=True), pre_act)


def contract_rows(left, right):
    return lax.dot_general(
        left, right, (((0,), (0,)), ((), ())), preferred_element_type=jnp.float32
    )


def pack_owners(array, owners):
    parts, rows, columns = array.shape
    width = columns // owners
    split = array.reshape(parts, 2, rows // 2, owners, width)
    return split.transpose(3, 0, 2, 1, 4).reshape(owners, parts, rows // 2, 2 * width)


def unpack_owner(array):
    parts, half, width = array.shape
    split = array.reshape(parts, half, 2, width // 2)
    return split.transpose(0, 2, 1, 3).reshape(parts, 2 * half, width // 2)


def general_body(
    token_ids,
    target,
    embedding,
    norm_gain,
    global_model,
    global_control,
    client_control,
    local_steps,
    client_weight,
):
    n_clients = lax.axis_size("clients")
    n_fsdp = lax.axis_size("fsdp")
    client_index = lax.axis_index("clients")
    fsdp_index = lax.axis_index("fsdp")
    paired = n_fsdp == 2 and n_clients % 2 == 0
    if paired:
        core = client_index % 2
        role_client = client_index - core + fsdp_index
        block = core
        swap_pairs = [
            (c * 2 + f, ((c - c % 2) + f) * 2 + c % 2) for c in range(n_clients) for f in range(2)
        ]
        core_pairs = [(c, c ^ 1) for c in range(n_clients)]
    else:
        role_client = client_index
        block = fsdp_index

    def swap_roles(array):
        if not paired:
            return array
        return lax.ppermute(array, ("clients", "fsdp"), swap_pairs)

    def gather_rows(array):
        if not paired:
            return lax.all_gather(array, "fsdp", axis=0, tiled=True)
        other = lax.ppermute(array, "clients", core_pairs)
        return jnp.concatenate(
            [jnp.where(core == 0, array, other), jnp.where(core == 0, other, array)], axis=0
        )

    def reduce_rows(term):
        if not paired:
            return lax.psum_scatter(term, "fsdp", scatter_dimension=0, tiled=True).astype(
                jnp.float32
            )
        rows = term.shape[0] // 2
        own = lax.dynamic_slice_in_dim(term, core * rows, rows, axis=0)
        sent = lax.dynamic_slice_in_dim(term, (1 - core) * rows, rows, axis=0)
        received = lax.ppermute(sent, "clients", core_pairs)
        return own.astype(jnp.float32) + received.astype(jnp.float32)

    tok_rows = target.shape[1]
    group_rows = tok_rows * n_fsdp
    loss_scale = 1.0 / math.sqrt(group_rows)
    all_ids = lax.all_gather(swap_roles(token_ids), "fsdp", axis=1, tiled=True)
    emb_columns = jnp.take(embedding, all_ids[0], axis=0)
    embedded = lax.all_to_all(emb_columns, "fsdp", split_axis=0, concat_axis=1, tiled=True)
    widened = embedded.astype(jnp.float32)
    inv_norm = lax.rsqrt(jnp.mean(widened * widened, axis=1, keepdims=True) + norm_eps)
    normed = (widened * inv_norm * norm_gain).astype(jnp.bfloat16)
    target_rows = swap_roles(target[0]).astype(jnp.float32)
    model_columns = lax.all_gather(
        global_model.astype(jnp.bfloat16), "fsdp", axis=1, tiled=True
    )
    model_full = lax.all_gather(model_columns, "clients", axis=2, tiled=True)
    control_rows = lax.all_gather(
        global_control.astype(jnp.bfloat16), "clients", axis=2, tiled=True
    ).astype(global_control.dtype)
    slots = jnp.arange(local_steps.shape[0])
    step_count = jnp.sum(jnp.where(slots == client_index, local_steps, 0))
    role_steps = jnp.sum(jnp.where(slots == role_client, local_steps, 0))
    own_weight = jnp.sum(jnp.where(slots == client_index, client_weight, 0)).astype(jnp.float32)
    weight_total = jnp.sum(client_weight).astype(jnp.float32)
    correction = control_rows - client_control[0]
    parts, rows = correction.shape[0], correction.shape[1]
    role_correction = [
        swap_roles(correction[part].astype(jnp.bfloat16)).astype(jnp.float32)
        for part in range(parts)
    ]
    role_model = lax.dynamic_slice_in_dim(model_full, block * rows, rows, axis=1).astype(
        jnp.float32
    )
    gathered = [model_full[part] for part in range(parts)]
    pseudo = [jnp.zeros_like(role_correction[part]) for part in range(parts)]
    summed = [jnp.zeros_like(role_correction[part]) for part in range(parts)]
    for local_step in range(LOCAL):
        if local_step > 0:
            gathered = [
                gather_rows(
                    (role_model[part] - learning_rate * pseudo[part]).astype(jnp.bfloat16)
                )
                for part in range(parts)
            ]
        gate_pre = jnp.dot(normed, gathered[0], preferred_element_type=jnp.float32)
        up_pre = jnp.dot(normed, gathered[1], preferred_element_type=jnp.float32)
        gate_act, gelu_back = gelu_pair(gate_pre)
        hidden = (gate_act * up_pre).astype(jnp.bfloat16)
        projected = lax.dot_general(
            hidden, gathered[2], (((1,), (1,)), ((), ())), preferred_element_type=jnp.float32
        )
        out_grad = ((widened + projected - target_rows) * loss_scale).astype(jnp.bfloat16)
        outer_term = contract_rows(out_grad, hidden).astype(jnp.bfloat16)
        hidden_grad = jnp.dot(out_grad, gathered[2], preferred_element_type=jnp.float32)
        gate_grad = gelu_back(hidden_grad * up_pre)[0].astype(jnp.bfloat16)
        up_grad = (hidden_grad * gate_act).astype(jnp.bfloat16)
        gate_term = contract_rows(normed, gate_grad).astype(jnp.bfloat16)
        up_term = contract_rows(normed, up_grad).astype(jnp.bfloat16)
        grads = [reduce_rows(term) for term in (gate_term, up_term, outer_term)]
        step_mask = (local_step < role_steps).astype(jnp.float32)
        for part in range(parts):
            pseudo[part] = pseudo[part] + step_mask * (grads[part] + role_correction[part])
            summed[part] = summed[part] + step_mask * grads[part]
    own_grads = jnp.stack(
        [swap_roles(summed[part].astype(jnp.bfloat16)).astype(jnp.float32) for part in range(parts)]
    )
    taken = jnp.sum((jnp.arange(LOCAL) < step_count).astype(jnp.float32))
    own_pseudo = own_grads + taken * correction
    update = client_control[0] - control_rows + own_pseudo / step_count.astype(jnp.float32)
    packed = jnp.concatenate(
        [
            pack_owners((own_weight * own_pseudo).astype(jnp.bfloat16), n_clients),
            pack_owners((own_weight * update).astype(jnp.bfloat16), n_clients),
        ],
        axis=1,
    )
    sums = lax.psum_scatter(packed, "clients", scatter_dimension=0, tiled=True)[0]
    sums = unpack_owner(sums).astype(jnp.float32) / weight_total
    return (sums[:parts], sums[parts:], update[None])


MESH = pl.DeviceIdType.MESH
TILE = 256
BF = jnp.bfloat16
F32 = jnp.float32


def gelu_parts(x):
    cubic = 0.044715
    scale = math.sqrt(2.0 / math.pi)
    square = x * x
    t = jnp.tanh(scale * x * (1.0 + cubic * square))
    half = 0.5 * (1.0 + t)
    slope = half + (0.5 * scale) * x * (1.0 - t * t) * (1.0 + (3.0 * cubic) * square)
    return x * half, slope


def dot(left, right, left_dim=1, right_dim=0):
    return lax.dot_general(
        left, right, (((left_dim,), (right_dim,)), ((), ())), preferred_element_type=F32
    )


def round_kernel(
    n_z,
    steps_ref,
    weights_ref,
    emb_ref,
    target_ref,
    gain_ref,
    model_ref,
    control_ref,
    own_ref,
    step_out,
    control_out,
    grad_out,
    packed,
    model,
    current,
    g_rows,
    c_rows,
    corr,
    role_corr,
    emb,
    target,
    normed,
    normed_t,
    act,
    slope_up,
    hidden,
    out_grad,
    out_grad_t,
    gate_grad,
    up_grad,
    term_out,
    term_own,
    term_in,
    share_in,
    kept,
    y_out,
    y_in,
    z_in,
    final,
    final_in,
    local_sem,
    send_sem,
    recv_sem,
):
    parts, half, width = own_ref.shape
    rows = emb.shape[0]
    depth = 2 * half
    n_pos = 2 * n_z
    span = width // n_pos
    owner_span = span // 2
    sub = kept.shape[2]
    n_sub = half // sub
    client = lax.axis_index("clients")
    x = lax.axis_index("fsdp")
    b = lax.rem(client, 2)
    p = client // 2
    y = lax.rem(p, 2)
    z = p // 2
    home = b == x
    away = b != x
    role_client = 2 * p + x
    half_at = pl.multiple_of(b * half, half)
    other_at = pl.multiple_of((1 - b) * half, half)
    own_rows = pl.ds(half_at, half)
    other_rows = pl.ds(other_at, half)
    owner_at = pl.multiple_of(b * owner_span, owner_span)

    partner = {"clients": 2 * p + 1 - b, "fsdp": x}
    across = {"clients": client, "fsdp": 1 - x}
    swap = {"clients": 2 * p + 1 - b, "fsdp": 1 - x}
    beside = {"clients": 2 * (2 * z + 1 - y) + b, "fsdp": x}

    def along(d):
        return {"clients": 2 * (2 * lax.rem(z + d, n_z) + y) + b, "fsdp": x}

    def behind(d):
        return lax.rem(z + n_z - d, n_z)

    def position(line, d):
        row = y if line == 0 else 1 - y
        return 2 * behind(d) + row

    def columns(pos):
        return pl.ds(pl.multiple_of(pos * span, span), span)

    n_chunks = parts * n_sub
    groups = ((0, parts - 1), (parts - 1, 1))
    counts = dict(
        pack=1, emb=1, target=1, cross=2, gz=n_z, gy=n_z, gp=n_pos, mz=2 * n_z, my=2 * n_z,
        mp=2 * n_pos, corr=parts, term0=parts, term1=parts, cur=parts, ret=n_chunks,
        share=n_chunks, ry=n_chunks, rz=n_chunks * n_z, final=1,
    )
    base = {}
    total = 0
    for name, count in counts.items():
        base[name] = total
        total += count

    def remote(src, dst, name, index, device):
        k = base[name] + index
        return pltpu.make_async_remote_copy(
            src_ref=src, dst_ref=dst, send_sem=send_sem.at[k], recv_sem=recv_sem.at[k],
            device_id=device, device_id_type=MESH,
        )

    def pack_copy():
        window = packed.at[:, :, pl.ds(owner_at, owner_span), :]
        return remote(window, window, "pack", 0, partner)

    def emb_copy():
        return remote(
            emb_ref.at[pl.ds(rows, rows), :],
            emb.at[:, pl.ds(pl.multiple_of(x * half, half), half)],
            "emb", 0, across,
        )

    def target_copy():
        return remote(target_ref, target, "target", 0, swap)

    def g_window(pos):
        return g_rows.at[:, :, columns(pos)]

    def model_window(group, pos):
        first, count = groups[group]
        return model.at[pl.ds(first, count), own_rows, columns(pos)]

    def g_along(d, source):
        window = g_window(source)
        return remote(window, window, "gz", d, along(d))

    def g_beside(d, source):
        window = g_window(source)
        return remote(window, window, "gy", d, beside)

    def g_partner(line, d):
        window = g_window(position(line, d))
        return remote(window, window, "gp", line * n_z + d, partner)

    def cross_copy(group):
        window = model_window(group, p)
        return remote(window, window, "cross", group, across)

    def model_along(group, d, source):
        window = model_window(group, source)
        return remote(window, window, "mz", group * n_z + d, along(d))

    def model_beside(group, d, source):
        window = model_window(group, source)
        return remote(window, window, "my", group * n_z + d, beside)

    def model_partner(group, line, d):
        window = model_window(group, position(line, d))
        return remote(window, window, "mp", group * n_pos + line * n_z + d, partner)

    def corr_copy(part):
        return remote(corr.at[part], role_corr.at[part], "corr", part, swap)

    def term_copy(step, part):
        return remote(
            term_out.at[part], term_in.at[step, part], "term%d" % step, part, partner
        )

    def current_copy(part):
        window = current.at[part, own_rows, :]
        return remote(window, window, "cur", part, partner)

    def sub_rows(s):
        return pl.ds(s * sub, sub)

    def return_copy(part, s):
        return remote(
            role_corr.at[part, sub_rows(s), :], g_rows.at[part, sub_rows(s), :],
            "ret", part * n_sub + s, swap,
        )

    def share_copy(part, s):
        return remote(
            term_out.at[part, sub_rows(s), :], share_in.at[part, sub_rows(s), :],
            "share", part * n_sub + s, partner,
        )

    def y_copy(k):
        return remote(y_out.at[k], y_in.at[k], "ry", k, beside)

    def z_copy(k, d):
        return remote(
            kept.at[k, lax.rem(z + d, n_z)], z_in.at[k, d], "rz", k * n_z + d, along(d)
        )

    def final_copy():
        return remote(
            final.at[:, pl.ds(pl.multiple_of((1 - b) * owner_span, owner_span), owner_span), :],
            final_in, "final", 0, partner,
        )

    def grad_store(part, s):
        return pltpu.make_async_copy(
            term_in.at[0, part, sub_rows(s), :], grad_out.at[part, sub_rows(s), :],
            local_sem.at[3 + part * n_sub + s],
        )

    barrier = pltpu.get_barrier_semaphore()
    for peer in [partner, across, swap, beside]:
        pl.semaphore_signal(barrier, inc=1, device_id=peer, device_id_type=MESH)
    for d in range(1, n_z):
        pl.semaphore_signal(barrier, inc=1, device_id=along(d), device_id_type=MESH)
    pl.semaphore_wait(barrier, 3 + n_z)

    own_load = pltpu.make_async_copy(own_ref, c_rows, local_sem.at[0])
    emb_load = pltpu.make_async_copy(
        emb_ref.at[pl.ds(0, rows), :],
        emb.at[:, pl.ds(pl.multiple_of(x * half, half), half)],
        local_sem.at[1],
    )
    target_load = pltpu.make_async_copy(target_ref, target, local_sem.at[2])

    packed[0, :, pl.ds(owner_at, owner_span), :] = model_ref[...].astype(BF)
    packed[1, :, pl.ds(owner_at, owner_span), :] = control_ref[...].astype(BF)

    @pl.when(away)
    def _():
        pack_copy().start()
        emb_copy().start()
        target_copy().start()

    own_load.start()
    emb_load.start()

    @pl.when(home)
    def _():
        target_load.start()
        partner_pack = packed.at[
            :, :, pl.ds(pl.multiple_of((1 - b) * owner_span, owner_span), owner_span), :
        ]
        remote(partner_pack, partner_pack, "pack", 0, partner).wait_recv()
        for part in range(parts):
            g_rows[part, :, columns(p)] = packed[1, part].T
        for d in range(1, n_z):
            g_along(d, p).start()
        g_beside(0, p).start()
        for part in range(parts):
            model[part, own_rows, columns(p)] = packed[0, part].T
        for group in range(2):
            cross_copy(group).start()
        emb_copy().start()
        for group in range(2):
            for d in range(1, n_z):
                model_along(group, d, p).start()
        g_partner(0, 0).start()
        for d in range(1, n_z):
            g_along(d, position(0, d)).wait_recv()
            g_beside(d, position(0, d)).start()
            g_partner(0, d).start()
        model_beside(0, 0, p).start()
        model_beside(1, 0, p).start()
        for d in range(n_z):
            g_beside(d, position(1, d)).wait_recv()
            g_partner(1, d).start()

    @pl.when(away)
    def _():
        for group in range(2):
            cross_copy(group).wait_recv()
            for d in range(1, n_z):
                model_along(group, d, p).start()
            model_beside(group, 0, p).start()

    for group in range(2):
        model_partner(group, 0, 0).start()
    own_load.wait()

    @pl.when(away)
    def _():
        for line in range(2):
            for d in range(n_z):
                g_partner(line, d).wait_recv()

    chunk = half // 6
    for part in range(parts):

        def correct(i, carry):
            at = pl.ds(pl.multiple_of(i * chunk, chunk), chunk)
            value = (g_rows[part, at, :].astype(F32) - c_rows[part, at, :]).astype(BF)
            corr[part, at, :] = value

            @pl.when(home)
            def _():
                role_corr[part, at, :] = value

            return carry

        lax.fori_loop(0, 6, correct, 0)

        @pl.when(away)
        def _():
            corr_copy(part).start()

    emb_load.wait()
    emb_copy().wait_recv()
    block = rows // 5

    def normalise(i, carry):
        at = pl.ds(pl.multiple_of(i * block, block), block)
        widened = emb[at, :].astype(F32)
        inv_norm = lax.rsqrt(jnp.mean(widened * widened, axis=1, keepdims=True) + norm_eps)
        value = (widened * inv_norm * gain_ref[...]).astype(BF)
        normed[at, :] = value
        normed_t[:, at] = value.T
        return carry

    lax.fori_loop(0, 5, normalise, 0)

    def relay(group, d):
        model_along(group, d, position(0, d)).wait_recv()
        model_beside(group, d, position(0, d)).start()
        model_partner(group, 0, d).start()

    def settle(group):
        for d in range(n_z):
            model_beside(group, d, position(1, d)).wait_recv()
            model_partner(group, 1, d).start()
        for line in range(2):
            for d in range(n_z):
                model_partner(group, line, d).wait_recv()

    for d in range(1, n_z):
        relay(0, d)
    settle(0)

    loss_scale = 1.0 / math.sqrt(2 * rows)
    n_tiles = width // TILE

    def tile_at(j):
        return pl.ds(pl.multiple_of(j * TILE, TILE), TILE)

    def half_product(left, left_rows, right, store):
        def product(j, carry):
            store(j, dot(left[left_rows, :], right[:, tile_at(j)]).astype(BF))
            return carry

        lax.fori_loop(0, n_tiles, product, 0)

    def local_step(step, weights, finish):
        def forward(j, carry):
            cols = tile_at(j)
            gate_act, slope = gelu_parts(dot(normed[...], weights[0, :, cols]))
            up_pre = dot(normed[...], weights[1, :, cols])
            act[:, cols] = gate_act
            slope_up[:, cols] = slope * up_pre
            hidden[:, cols] = (gate_act * up_pre).astype(BF)
            return carry

        lax.fori_loop(0, n_tiles, forward, 0)
        if step == 0:
            for d in range(1, n_z):
                relay(1, d)
            settle(1)

            @pl.when(away)
            def _():
                target_copy().wait_recv()

            @pl.when(home)
            def _():
                target_load.wait()

        def project(j, carry):
            cols = tile_at(j)
            projected = dot(hidden[...], weights[2, cols, :], 1, 1)
            value = (
                (emb[:, cols].astype(F32) + projected - target[:, cols].astype(F32)) * loss_scale
            ).astype(BF)
            out_grad[:, cols] = value
            out_grad_t[cols, :] = value.T
            return carry

        lax.fori_loop(0, depth // TILE, project, 0)

        def term(part, left, right):
            def store_out(j, value):
                term_out[part, :, tile_at(j)] = value

            def store_own(j, value):
                term_own[part, :, tile_at(j)] = value

            if step > 0:
                term_copy(step - 1, part).wait_send()
            half_product(left, other_rows, right, store_out)
            term_copy(step, part).start()
            half_product(left, own_rows, right, store_own)

        term(2, out_grad_t, hidden)

        def backward(j, carry):
            cols = tile_at(j)
            hidden_grad = dot(out_grad[...], weights[2, :, cols])
            gate_grad[:, cols] = (hidden_grad * slope_up[:, cols]).astype(BF)
            up_grad[:, cols] = (hidden_grad * act[:, cols]).astype(BF)
            return carry

        lax.fori_loop(0, n_tiles, backward, 0)
        finish(2)
        term(0, normed_t, gate_grad)
        term(1, normed_t, up_grad)
        finish(0)
        finish(1)

    def update(part):
        term_copy(0, part).wait_recv()

        @pl.when(away)
        def _():
            corr_copy(part).wait_recv()

        def apply(i, carry):
            at = pl.ds(pl.multiple_of(i * chunk, chunk), chunk)
            model_at = pl.ds(pl.multiple_of(half_at + i * chunk, chunk), chunk)
            grads = term_own[part, at, :].astype(F32) + term_in[0, part, at, :].astype(F32)
            c_rows[part, at, :] = grads
            pseudo = grads + role_corr[part, at, :].astype(F32)
            current[part, model_at, :] = (
                model[part, model_at, :].astype(F32) - learning_rate * pseudo
            ).astype(BF)
            return carry

        lax.fori_loop(0, 6, apply, 0)
        current_copy(part).start()

    second = (steps_ref[role_client] > 1).astype(F32)

    def collect(part):
        term_copy(1, part).wait_recv()
        for s in range(n_sub):
            at = sub_rows(s)
            grads = term_own[part, at, :].astype(F32) + term_in[1, part, at, :].astype(F32)
            role_corr[part, at, :] = (c_rows[part, at, :] + second * grads).astype(BF)

            @pl.when(away)
            def _():
                return_copy(part, s).start()

    local_step(0, model, update)
    for part in range(parts):
        current_copy(part).wait_recv()
    local_step(1, current, collect)

    weight = weights_ref[client].astype(F32)
    taken = steps_ref[client].astype(F32)
    inverse = 1.0 / taken
    order = [(part, s) for part in (2, 0, 1) for s in range(n_sub)]

    def share(part, s):
        at = sub_rows(s)
        if s == 0:
            term_copy(1, part).wait_send()

        def spread(source):
            value = source[part, at, :].astype(F32)
            averaged = inverse * value
            summed = value + taken * corr[part, at, :].astype(F32)
            term_in[0, part, at, :] = averaged.astype(BF)
            mine = jnp.where(b == 0, summed, averaged)
            theirs = jnp.where(b == 0, averaged, summed)
            term_own[part, at, :] = (weight * mine).astype(BF)
            term_out[part, at, :] = (weight * theirs).astype(BF)

        @pl.when(home)
        def _():
            spread(role_corr)

        @pl.when(away)
        def _():
            return_copy(part, s).wait_recv()
            spread(g_rows)

        share_copy(part, s).start()
        grad_store(part, s).start()

    def split(k):
        part, s = order[k]
        at = sub_rows(s)
        share_copy(part, s).wait_recv()
        for row in range(n_z):
            for line in range(2):
                cols = columns(2 * row + (y if line == 0 else 1 - y))
                value = (
                    term_own[part, at, cols].astype(F32) + share_in[part, at, cols].astype(F32)
                ).astype(BF)
                if line == 0:
                    kept[k, row] = value
                else:
                    y_out[k, row] = value
        y_copy(k).start()

    def spread_z(k):
        y_copy(k).wait_recv()
        kept[k] = (kept[k].astype(F32) + y_in[k].astype(F32)).astype(BF)
        for d in range(1, n_z):
            z_copy(k, d).start()

    def gather_z(k):
        part, s = order[k]
        value = kept[k, z].astype(F32)
        for d in range(1, n_z):
            z_copy(k, d).wait_recv()
            value += z_in[k, d].astype(F32)
        final[part, :, sub_rows(s)] = value.T

    for k in range(n_chunks + 2):
        if k < n_chunks:
            share(*order[k])
            split(k)
        if 0 <= k - 1 < n_chunks:
            spread_z(k - 1)
        if 0 <= k - 2:
            gather_z(k - 2)
    final_copy().start()

    weight_total = weights_ref[0]
    step_total = weights_ref[0] * steps_ref[0]
    for i in range(1, 2 * n_pos):
        weight_total += weights_ref[i]
        step_total += weights_ref[i] * steps_ref[i]
    weight_total = weight_total.astype(F32)
    step_total = step_total.astype(F32)
    control = control_ref[...]
    lost = step_total * (control - control.astype(BF).astype(F32))
    final_copy().wait_recv()
    mine = final[:, pl.ds(owner_at, owner_span), :]
    theirs = final_in[...]
    step_out[...] = (jnp.where(b == 0, mine, theirs) + lost) / weight_total
    control_out[...] = jnp.where(b == 0, theirs, mine) / weight_total

    @pl.when(away)
    def _():
        pack_copy().wait_send()
        target_copy().wait_send()
        for part in range(parts):
            corr_copy(part).wait_send()
            for s in range(n_sub):
                return_copy(part, s).wait_send()

    @pl.when(home)
    def _():
        for group in range(2):
            cross_copy(group).wait_send()
        for d in range(n_z):
            if d > 0:
                g_along(d, p).wait_send()
            g_beside(d, position(0, d)).wait_send()
            for line in range(2):
                g_partner(line, d).wait_send()

    emb_copy().wait_send()
    for group in range(2):
        for d in range(n_z):
            if d > 0:
                model_along(group, d, p).wait_send()
            model_beside(group, d, position(0, d)).wait_send()
            for line in range(2):
                model_partner(group, line, d).wait_send()
    for part in range(parts):
        current_copy(part).wait_send()
        for s in range(n_sub):
            share_copy(part, s).wait_send()
            grad_store(part, s).wait()
    for k in range(n_chunks):
        y_copy(k).wait_send()
        for d in range(1, n_z):
            z_copy(k, d).wait_send()
    final_copy().wait_send()


def paired_body(
    token_ids,
    target,
    embedding,
    norm_gain,
    global_model,
    global_control,
    client_control,
    local_steps,
    client_weight,
):
    n_clients = lax.axis_size("clients")
    n_pos = n_clients // 2
    n_z = n_pos // 2
    parts, half, owner_span = global_model.shape
    width = owner_span * n_clients
    span = 2 * owner_span
    rows = token_ids.shape[1]
    depth = 2 * half
    sub = 128
    n_chunks = parts * (half // sub)
    pairs = [(c, f) for c in range(n_clients) for f in range(2)]
    to_role = [(c * 2 + f, (c - c % 2 + f) * 2 + c % 2) for c, f in pairs]
    to_across = [(c * 2 + f, (c - c % 2 + f) * 2 + 1 - c % 2) for c, f in pairs]
    ids = jnp.concatenate(
        [
            lax.ppermute(token_ids[0], ("clients", "fsdp"), to_role),
            lax.ppermute(token_ids[0], ("clients", "fsdp"), to_across),
        ]
    )
    emb_columns = embedding.at[ids].get(mode="promise_in_bounds")

    n_sem = 6 + 6 * n_z + 3 * n_pos + 4 * parts + n_chunks * (3 + n_z)
    vmem = pltpu.VMEM
    scratch = [
        vmem((2, parts, span, half), BF),
        vmem((parts, depth, width), BF),
        vmem((parts, depth, width), BF),
        vmem((parts, half, width), BF),
        vmem((parts, half, width), F32),
        vmem((parts, half, width), BF),
        vmem((parts, half, width), BF),
        vmem((rows, depth), BF),
        vmem((rows, depth), BF),
        vmem((rows, depth), BF),
        vmem((depth, rows), BF),
        vmem((rows, width), F32),
        vmem((rows, width), F32),
        vmem((rows, width), BF),
        vmem((rows, depth), BF),
        vmem((depth, rows), BF),
        vmem((rows, width), BF),
        vmem((rows, width), BF),
        vmem((parts, half, width), BF),
        vmem((parts, half, width), BF),
        vmem((2, parts, half, width), BF),
        vmem((parts, half, width), BF),
        vmem((n_chunks, n_z, sub, span), BF),
        vmem((n_chunks, n_z, sub, span), BF),
        vmem((n_chunks, n_z, sub, span), BF),
        vmem((n_chunks, n_z, sub, span), BF),
        vmem((parts, span, half), F32),
        vmem((parts, owner_span, half), F32),
        pltpu.SemaphoreType.DMA((3 + n_chunks,)),
        pltpu.SemaphoreType.DMA((n_sem,)),
        pltpu.SemaphoreType.DMA((n_sem,)),
    ]
    smem = pl.BlockSpec(memory_space=pltpu.SMEM)
    anywhere = pl.BlockSpec(memory_space=pl.ANY)
    inside = pl.BlockSpec(memory_space=pltpu.VMEM)
    step_sum, control_sum, grad_rows = pl.pallas_call(
        functools.partial(round_kernel, n_z),
        out_shape=(
            jax.ShapeDtypeStruct((parts, owner_span, half), F32),
            jax.ShapeDtypeStruct((parts, owner_span, half), F32),
            jax.ShapeDtypeStruct((parts, half, width), BF),
        ),
        in_specs=[smem, smem, anywhere, anywhere, inside, inside, inside, anywhere],
        out_specs=(inside, inside, anywhere),
        scratch_shapes=scratch,
        compiler_params=pltpu.CompilerParams(
            collective_id=0, has_side_effects=True, vmem_limit_bytes=67043328
        ),
    )(
        local_steps,
        client_weight,
        emb_columns,
        target[0],
        norm_gain[None, :],
        jnp.swapaxes(global_model, 1, 2),
        jnp.swapaxes(global_control, 1, 2),
        client_control[0],
    )
    return (
        jnp.swapaxes(step_sum, 1, 2),
        jnp.swapaxes(control_sum, 1, 2),
        grad_rows.astype(F32)[None],
    )


def solution(mesh):
    placed = (
        P("clients", "fsdp"),
        P("clients", "fsdp", None),
        P(None, "fsdp"),
        P(),
        P(None, "fsdp", "clients"),
        P(None, "fsdp", "clients"),
        P("clients", None, "fsdp", None),
        P(),
        P(),
    )
    paired = mesh.shape["fsdp"] == 2 and mesh.shape["clients"] % 4 == 0
    return jax.shard_map(
        paired_body if paired else general_body,
        mesh=mesh,
        in_specs=placed,
        out_specs=(
            P(None, "fsdp", "clients"),
            P(None, "fsdp", "clients"),
            P("clients", None, "fsdp", None),
        ),
        check_vma=False,
    )
```

```python
import functools
import math

import jax
import jax.numpy as jnp
from jax import lax
from jax.experimental import pallas as pl
from jax.experimental.pallas import tpu as pltpu
from jax.sharding import PartitionSpec as P

LOCAL = 2


learning_rate = 0.005
norm_eps = 1e-06


def gelu_pair(pre_act):
    return jax.vjp(lambda inputs: jax.nn.gelu(inputs, approximate=True), pre_act)


def contract_rows(left, right):
    return lax.dot_general(
        left, right, (((0,), (0,)), ((), ())), preferred_element_type=jnp.float32
    )


def pack_owners(array, owners):
    parts, rows, columns = array.shape
    width = columns // owners
    split = array.reshape(parts, 2, rows // 2, owners, width)
    return split.transpose(3, 0, 2, 1, 4).reshape(owners, parts, rows // 2, 2 * width)


def unpack_owner(array):
    parts, half, width = array.shape
    split = array.reshape(parts, half, 2, width // 2)
    return split.transpose(0, 2, 1, 3).reshape(parts, 2 * half, width // 2)


def general_body(
    token_ids,
    target,
    embedding,
    norm_gain,
    global_model,
    global_control,
    client_control,
    local_steps,
    client_weight,
):
    n_clients = lax.axis_size("clients")
    n_fsdp = lax.axis_size("fsdp")
    client_index = lax.axis_index("clients")
    fsdp_index = lax.axis_index("fsdp")
    paired = n_fsdp == 2 and n_clients % 2 == 0
    if paired:
        core = client_index % 2
        role_client = client_index - core + fsdp_index
        block = core
        swap_pairs = [
            (c * 2 + f, ((c - c % 2) + f) * 2 + c % 2) for c in range(n_clients) for f in range(2)
        ]
        core_pairs = [(c, c ^ 1) for c in range(n_clients)]
    else:
        role_client = client_index
        block = fsdp_index

    def swap_roles(array):
        if not paired:
            return array
        return lax.ppermute(array, ("clients", "fsdp"), swap_pairs)

    def gather_rows(array):
        if not paired:
            return lax.all_gather(array, "fsdp", axis=0, tiled=True)
        other = lax.ppermute(array, "clients", core_pairs)
        return jnp.concatenate(
            [jnp.where(core == 0, array, other), jnp.where(core == 0, other, array)], axis=0
        )

    def reduce_rows(term):
        if not paired:
            return lax.psum_scatter(term, "fsdp", scatter_dimension=0, tiled=True).astype(
                jnp.float32
            )
        rows = term.shape[0] // 2
        own = lax.dynamic_slice_in_dim(term, core * rows, rows, axis=0)
        sent = lax.dynamic_slice_in_dim(term, (1 - core) * rows, rows, axis=0)
        received = lax.ppermute(sent, "clients", core_pairs)
        return own.astype(jnp.float32) + received.astype(jnp.float32)

    tok_rows = target.shape[1]
    group_rows = tok_rows * n_fsdp
    loss_scale = 1.0 / math.sqrt(group_rows)
    all_ids = lax.all_gather(swap_roles(token_ids), "fsdp", axis=1, tiled=True)
    emb_columns = jnp.take(embedding, all_ids[0], axis=0)
    embedded = lax.all_to_all(emb_columns, "fsdp", split_axis=0, concat_axis=1, tiled=True)
    widened = embedded.astype(jnp.float32)
    inv_norm = lax.rsqrt(jnp.mean(widened * widened, axis=1, keepdims=True) + norm_eps)
    normed = (widened * inv_norm * norm_gain).astype(jnp.bfloat16)
    target_rows = swap_roles(target[0]).astype(jnp.float32)
    model_columns = lax.all_gather(
        global_model.astype(jnp.bfloat16), "fsdp", axis=1, tiled=True
    )
    model_full = lax.all_gather(model_columns, "clients", axis=2, tiled=True)
    control_rows = lax.all_gather(
        global_control.astype(jnp.bfloat16), "clients", axis=2, tiled=True
    ).astype(global_control.dtype)
    slots = jnp.arange(local_steps.shape[0])
    step_count = jnp.sum(jnp.where(slots == client_index, local_steps, 0))
    role_steps = jnp.sum(jnp.where(slots == role_client, local_steps, 0))
    own_weight = jnp.sum(jnp.where(slots == client_index, client_weight, 0)).astype(jnp.float32)
    weight_total = jnp.sum(client_weight).astype(jnp.float32)
    correction = control_rows - client_control[0]
    parts, rows = correction.shape[0], correction.shape[1]
    role_correction = [
        swap_roles(correction[part].astype(jnp.bfloat16)).astype(jnp.float32)
        for part in range(parts)
    ]
    role_model = lax.dynamic_slice_in_dim(model_full, block * rows, rows, axis=1).astype(
        jnp.float32
    )
    gathered = [model_full[part] for part in range(parts)]
    pseudo = [jnp.zeros_like(role_correction[part]) for part in range(parts)]
    summed = [jnp.zeros_like(role_correction[part]) for part in range(parts)]
    for local_step in range(LOCAL):
        if local_step > 0:
            gathered = [
                gather_rows(
                    (role_model[part] - learning_rate * pseudo[part]).astype(jnp.bfloat16)
                )
                for part in range(parts)
            ]
        gate_pre = jnp.dot(normed, gathered[0], preferred_element_type=jnp.float32)
        up_pre = jnp.dot(normed, gathered[1], preferred_element_type=jnp.float32)
        gate_act, gelu_back = gelu_pair(gate_pre)
        hidden = (gate_act * up_pre).astype(jnp.bfloat16)
        projected = lax.dot_general(
            hidden, gathered[2], (((1,), (1,)), ((), ())), preferred_element_type=jnp.float32
        )
        out_grad = ((widened + projected - target_rows) * loss_scale).astype(jnp.bfloat16)
        outer_term = contract_rows(out_grad, hidden).astype(jnp.bfloat16)
        hidden_grad = jnp.dot(out_grad, gathered[2], preferred_element_type=jnp.float32)
        gate_grad = gelu_back(hidden_grad * up_pre)[0].astype(jnp.bfloat16)
        up_grad = (hidden_grad * gate_act).astype(jnp.bfloat16)
        gate_term = contract_rows(normed, gate_grad).astype(jnp.bfloat16)
        up_term = contract_rows(normed, up_grad).astype(jnp.bfloat16)
        grads = [reduce_rows(term) for term in (gate_term, up_term, outer_term)]
        step_mask = (local_step < role_steps).astype(jnp.float32)
        for part in range(parts):
            pseudo[part] = pseudo[part] + step_mask * (grads[part] + role_correction[part])
            summed[part] = summed[part] + step_mask * grads[part]
    own_grads = jnp.stack(
        [swap_roles(summed[part].astype(jnp.bfloat16)).astype(jnp.float32) for part in range(parts)]
    )
    taken = jnp.sum((jnp.arange(LOCAL) < step_count).astype(jnp.float32))
    own_pseudo = own_grads + taken * correction
    update = client_control[0] - control_rows + own_pseudo / step_count.astype(jnp.float32)
    packed = jnp.concatenate(
        [
            pack_owners((own_weight * own_pseudo).astype(jnp.bfloat16), n_clients),
            pack_owners((own_weight * update).astype(jnp.bfloat16), n_clients),
        ],
        axis=1,
    )
    sums = lax.psum_scatter(packed, "clients", scatter_dimension=0, tiled=True)[0]
    sums = unpack_owner(sums).astype(jnp.float32) / weight_total
    return (sums[:parts], sums[parts:], update[None])


MESH = pl.DeviceIdType.MESH
TILE = 256
BF = jnp.bfloat16
F32 = jnp.float32


def gelu_parts(x):
    cubic = 0.044715
    scale = math.sqrt(2.0 / math.pi)
    square = x * x
    t = jnp.tanh(scale * x * (1.0 + cubic * square))
    half = 0.5 * (1.0 + t)
    slope = half + (0.5 * scale) * x * (1.0 - t * t) * (1.0 + (3.0 * cubic) * square)
    return x * half, slope


def dot(left, right, left_dim=1, right_dim=0):
    return lax.dot_general(
        left, right, (((left_dim,), (right_dim,)), ((), ())), preferred_element_type=F32
    )


def round_kernel(
    n_z,
    steps_ref,
    weights_ref,
    emb_ref,
    target_ref,
    gain_ref,
    model_ref,
    control_ref,
    own_ref,
    step_out,
    control_out,
    grad_out,
    packed,
    model,
    current,
    g_rows,
    c_rows,
    corr,
    role_corr,
    emb,
    target,
    normed,
    normed_t,
    act,
    slope_up,
    hidden,
    out_grad,
    out_grad_t,
    gate_grad,
    up_grad,
    term_out,
    term_own,
    term_in,
    share_in,
    kept,
    y_out,
    y_in,
    z_in,
    summed,
    final,
    final_in,
    local_sem,
    send_sem,
    recv_sem,
):
    parts, half, width = own_ref.shape
    rows = emb.shape[0]
    depth = 2 * half
    n_pos = 2 * n_z
    span = width // n_pos
    owner_span = span // 2
    sub = kept.shape[2]
    n_sub = half // sub
    client = lax.axis_index("clients")
    x = lax.axis_index("fsdp")
    b = lax.rem(client, 2)
    p = client // 2
    y = lax.rem(p, 2)
    z = p // 2
    home = b == x
    away = b != x
    role_client = 2 * p + x
    half_at = pl.multiple_of(b * half, half)
    other_at = pl.multiple_of((1 - b) * half, half)
    own_rows = pl.ds(half_at, half)
    other_rows = pl.ds(other_at, half)
    owner_at = pl.multiple_of(b * owner_span, owner_span)

    partner = {"clients": 2 * p + 1 - b, "fsdp": x}
    across = {"clients": client, "fsdp": 1 - x}
    swap = {"clients": 2 * p + 1 - b, "fsdp": 1 - x}
    beside = {"clients": 2 * (2 * z + 1 - y) + b, "fsdp": x}

    def along(d):
        return {"clients": 2 * (2 * lax.rem(z + d, n_z) + y) + b, "fsdp": x}

    def behind(d):
        return lax.rem(z + n_z - d, n_z)

    def position(line, row):
        return 2 * row + (y if line == 0 else 1 - y)

    def columns(pos):
        return pl.ds(pl.multiple_of(pos * span, span), span)

    n_chunks = parts * n_sub
    groups = ((0, parts - 1), (parts - 1, 1))
    counts = dict(
        pack=1, emb=1, target=1, cross=2, gz=n_z, gy=n_z, gp=n_pos, mz=2 * n_z, my=2 * n_z,
        mp=2 * n_pos, corr=parts, term0=parts, term1=parts, cur=parts, ret=n_chunks,
        share=n_chunks, ry=n_chunks, rz=n_chunks * n_z, final=1,
    )
    base = {}
    total = 0
    for name, count in counts.items():
        base[name] = total
        total += count

    def remote(src, dst, name, index, device):
        k = base[name] + index
        return pltpu.make_async_remote_copy(
            src_ref=src, dst_ref=dst, send_sem=send_sem.at[k], recv_sem=recv_sem.at[k],
            device_id=device, device_id_type=MESH,
        )

    def pack_copy():
        window = packed.at[:, :, pl.ds(owner_at, owner_span), :]
        return remote(window, window, "pack", 0, partner)

    def emb_copy():
        return remote(
            emb_ref.at[pl.ds(rows, rows), :],
            emb.at[:, pl.ds(pl.multiple_of(x * half, half), half)],
            "emb", 0, across,
        )

    def target_copy():
        return remote(target_ref, target, "target", 0, swap)

    quarter = half // 2
    g_own = pl.ds(pl.multiple_of(jnp.where(home, 0, quarter), quarter), quarter)

    def g_window(pos):
        return g_rows.at[:, g_own, columns(pos)]

    def model_window(group, pos):
        first, count = groups[group]
        return model.at[pl.ds(first, count), own_rows, columns(pos)]

    def g_along(d, row):
        window = g_window(position(0, row))
        return remote(window, window, "gz", d, along(d))

    def g_beside(line, row):
        window = g_window(position(line, row))
        return remote(window, window, "gy", row, beside)

    def g_partner(line, row):
        window = g_window(position(line, row))
        return remote(window, window, "gp", line * n_z + row, partner)

    def cross_copy(group):
        window = model_window(group, p)
        return remote(window, window, "cross", group, across)

    def model_along(group, d, row):
        window = model_window(group, position(0, row))
        return remote(window, window, "mz", group * n_z + d, along(d))

    def model_beside(group, line, row):
        window = model_window(group, position(line, row))
        return remote(window, window, "my", group * n_z + row, beside)

    def model_partner(group, line, row):
        window = model_window(group, position(line, row))
        return remote(window, window, "mp", group * n_pos + line * n_z + row, partner)

    def corr_copy(part):
        return remote(corr.at[part], role_corr.at[part], "corr", part, swap)

    def term_copy(step, part):
        return remote(
            term_out.at[part], term_in.at[step, part], "term%d" % step, part, partner
        )

    def current_copy(part):
        window = current.at[part, own_rows, :]
        return remote(window, window, "cur", part, partner)

    def sub_rows(s):
        return pl.ds(pl.multiple_of(s * sub, sub), sub)

    def return_copy(part, s):
        return remote(
            role_corr.at[part, sub_rows(s), :], g_rows.at[part, sub_rows(s), :],
            "ret", part * n_sub + s, swap,
        )

    def share_copy(part, s):
        return remote(
            term_out.at[part, sub_rows(s), :], share_in.at[part, sub_rows(s), :],
            "share", part * n_sub + s, partner,
        )

    def y_copy(k):
        return remote(y_out.at[k], y_in.at[k], "ry", k, beside)

    def z_copy(k, d):
        return remote(
            kept.at[k, lax.rem(z + d, n_z)], z_in.at[k, d], "rz", k * n_z + d, along(d)
        )

    def final_copy():
        return remote(
            final.at[:, pl.ds(pl.multiple_of((1 - b) * owner_span, owner_span), owner_span), :],
            final_in, "final", 0, partner,
        )

    def grad_store(part, s):
        return pltpu.make_async_copy(
            term_in.at[0, part, sub_rows(s), :], grad_out.at[part, sub_rows(s), :],
            local_sem.at[3 + part * n_sub + s],
        )

    barrier = pltpu.get_barrier_semaphore()
    for peer in [partner, across, swap, beside]:
        pl.semaphore_signal(barrier, inc=1, device_id=peer, device_id_type=MESH)
    for d in range(1, n_z):
        pl.semaphore_signal(barrier, inc=1, device_id=along(d), device_id_type=MESH)
    pl.semaphore_wait(barrier, 3 + n_z)

    own_load = pltpu.make_async_copy(own_ref, c_rows, local_sem.at[0])
    emb_load = pltpu.make_async_copy(
        emb_ref.at[pl.ds(0, rows), :],
        emb.at[:, pl.ds(pl.multiple_of(x * half, half), half)],
        local_sem.at[1],
    )
    target_load = pltpu.make_async_copy(target_ref, target, local_sem.at[2])

    packed[0, :, pl.ds(owner_at, owner_span), :] = model_ref[...].astype(BF)
    packed[1, :, pl.ds(owner_at, owner_span), :] = control_ref[...].astype(BF)

    pack_copy().start()
    own_load.start()
    emb_load.start()
    pl.when(home)(target_load.start)
    pack_copy().wait_recv()

    @pl.when(home)
    def _():
        for part in range(parts):
            model[part, own_rows, columns(p)] = packed[0, part].T
        for group in range(2):
            cross_copy(group).start()
        for part in range(parts):
            g_rows[part, :quarter, columns(p)] = packed[1, part].T[:quarter]

    @pl.when(away)
    def _():
        for part in range(parts):
            g_rows[part, quarter:, columns(p)] = packed[1, part].T[quarter:]

    for d in range(1, n_z):
        g_along(d, z).start()
    g_beside(0, z).start()
    g_partner(0, z).start()
    pl.when(home)(emb_copy().start)
    for group in range(2):
        pl.when(away)(cross_copy(group).wait_recv)
        for d in range(1, n_z):
            model_along(group, d, z).start()
        model_beside(group, 0, z).start()
        model_partner(group, 0, z).start()

    @pl.when(away)
    def _():
        emb_copy().start()
        target_copy().start()

    for d in range(1, n_z):
        row = behind(d)
        g_along(d, row).wait_recv()
        g_beside(0, row).start()
        g_partner(0, row).start()
    for row in range(n_z):
        g_beside(1, row).wait_recv()
        g_partner(1, row).start()
    for line in range(2):
        for row in range(n_z):
            g_partner(line, row).wait_recv()
    for d in range(1, n_z):
        g_along(d, z).wait_send()
    for row in range(n_z):
        g_beside(0, row).wait_send()
        for line in range(2):
            g_partner(line, row).wait_send()
    own_load.wait()

    chunk = half // 6
    for part in range(parts):

        def correct(i, carry):
            at = pl.ds(pl.multiple_of(i * chunk, chunk), chunk)
            value = (g_rows[part, at, :].astype(F32) - c_rows[part, at, :]).astype(BF)
            corr[part, at, :] = value

            @pl.when(home)
            def _():
                role_corr[part, at, :] = value

            return carry

        lax.fori_loop(0, 6, correct, 0)

        @pl.when(away)
        def _():
            corr_copy(part).start()

    emb_load.wait()
    emb_copy().wait_recv()
    block = rows // 5

    def normalise(i, carry):
        at = pl.ds(pl.multiple_of(i * block, block), block)
        widened = emb[at, :].astype(F32)
        inv_norm = lax.rsqrt(jnp.mean(widened * widened, axis=1, keepdims=True) + norm_eps)
        value = (widened * inv_norm * gain_ref[...]).astype(BF)
        normed[at, :] = value
        normed_t[:, at] = value.T
        return carry

    lax.fori_loop(0, 5, normalise, 0)

    def relay(group):
        for d in range(1, n_z):
            row = behind(d)
            model_along(group, d, row).wait_recv()
            model_beside(group, 0, row).start()
            model_partner(group, 0, row).start()

    def settle(group):
        for row in range(n_z):
            model_beside(group, 1, row).wait_recv()
            model_partner(group, 1, row).start()

    def arrive(group):
        for line in range(2):
            for row in range(n_z):
                model_partner(group, line, row).wait_recv()

    relay(0)
    settle(0)
    relay(1)
    arrive(0)

    loss_scale = 1.0 / math.sqrt(2 * rows)
    n_tiles = width // TILE

    def tile_at(j):
        return pl.ds(pl.multiple_of(j * TILE, TILE), TILE)

    def half_product(left, left_rows, right, store):
        def product(j, carry):
            store(j, dot(left[left_rows, :], right[:, tile_at(j)]).astype(BF))
            return carry

        lax.fori_loop(0, n_tiles, product, 0)

    def local_step(step, weights, finish, between):
        def forward(j, carry):
            cols = tile_at(j)
            gate_act, slope = gelu_parts(dot(normed[...], weights[0, :, cols]))
            up_pre = dot(normed[...], weights[1, :, cols])
            act[:, cols] = gate_act
            slope_up[:, cols] = slope * up_pre
            hidden[:, cols] = (gate_act * up_pre).astype(BF)
            return carry

        lax.fori_loop(0, n_tiles, forward, 0)
        if step == 0:
            settle(1)
            arrive(1)

            @pl.when(away)
            def _():
                target_copy().wait_recv()

            @pl.when(home)
            def _():
                target_load.wait()

        def project(j, carry):
            cols = tile_at(j)
            projected = dot(hidden[...], weights[2, cols, :], 1, 1)
            value = (
                (emb[:, cols].astype(F32) + projected - target[:, cols].astype(F32)) * loss_scale
            ).astype(BF)
            out_grad[:, cols] = value
            out_grad_t[cols, :] = value.T
            return carry

        lax.fori_loop(0, depth // TILE, project, 0)

        def term(part, left, right):
            def store_out(j, value):
                term_out[part, :, tile_at(j)] = value

            def store_own(j, value):
                term_own[part, :, tile_at(j)] = value

            if step > 0:
                term_copy(step - 1, part).wait_send()
            half_product(left, other_rows, right, store_out)
            term_copy(step, part).start()
            half_product(left, own_rows, right, store_own)

        term(2, out_grad_t, hidden)

        def backward(j, carry):
            cols = tile_at(j)
            hidden_grad = dot(out_grad[...], weights[2, :, cols])
            gate_grad[:, cols] = (hidden_grad * slope_up[:, cols]).astype(BF)
            up_grad[:, cols] = (hidden_grad * act[:, cols]).astype(BF)
            return carry

        lax.fori_loop(0, n_tiles, backward, 0)
        finish(2)
        term(0, normed_t, gate_grad)
        between()
        term(1, normed_t, up_grad)
        finish(0)
        finish(1)

    def update(part):
        term_copy(0, part).wait_recv()

        @pl.when(away)
        def _():
            corr_copy(part).wait_recv()

        def apply(i, carry):
            at = pl.ds(pl.multiple_of(i * chunk, chunk), chunk)
            model_at = pl.ds(pl.multiple_of(half_at + i * chunk, chunk), chunk)
            grads = term_own[part, at, :].astype(F32) + term_in[0, part, at, :].astype(F32)
            c_rows[part, at, :] = grads
            pseudo = grads + role_corr[part, at, :].astype(F32)
            current[part, model_at, :] = (
                model[part, model_at, :].astype(F32) - learning_rate * pseudo
            ).astype(BF)
            return carry

        lax.fori_loop(0, 6, apply, 0)
        current_copy(part).start()

    second = (steps_ref[role_client] > 1).astype(F32)

    def collect(part):
        term_copy(1, part).wait_recv()
        for s in range(n_sub):
            at = sub_rows(s)
            grads = term_own[part, at, :].astype(F32) + term_in[1, part, at, :].astype(F32)
            role_corr[part, at, :] = (c_rows[part, at, :] + second * grads).astype(BF)

            @pl.when(away)
            def _():
                return_copy(part, s).start()

    local_step(0, model, update, lambda: None)
    for part in range(parts):
        current_copy(part).wait_recv()
    weight = weights_ref[client].astype(F32)
    taken = steps_ref[client].astype(F32)
    inverse = 1.0 / taken

    def place(k):
        return lax.rem(k // n_sub + parts - 1, parts), lax.rem(k, n_sub)

    def share(k):
        part, s = place(k)
        at = sub_rows(s)

        @pl.when(s == 0)
        def _():
            term_copy(1, part).wait_send()

        def spread(source):
            value = source[part, at, :].astype(F32)
            averaged = inverse * value
            summed = value + taken * corr[part, at, :].astype(F32)
            term_in[0, part, at, :] = averaged.astype(BF)
            mine = jnp.where(b == 0, summed, averaged)
            theirs = jnp.where(b == 0, averaged, summed)
            term_own[part, at, :] = (weight * mine).astype(BF)
            term_out[part, at, :] = (weight * theirs).astype(BF)

        @pl.when(home)
        def _():
            spread(role_corr)

        @pl.when(away)
        def _():
            return_copy(part, s).wait_recv()
            spread(g_rows)

        share_copy(part, s).start()
        grad_store(part, s).start()

    def split(k):
        part, s = place(k)
        at = sub_rows(s)
        share_copy(part, s).wait_recv()
        for row in range(n_z):
            for line in range(2):
                cols = columns(position(line, row))
                value = (
                    term_own[part, at, cols].astype(F32) + share_in[part, at, cols].astype(F32)
                ).astype(BF)
                if line == 0:
                    kept[k, row] = value
                else:
                    y_out[k, row] = value
        y_copy(k).start()

    def spread_z(k):
        y_copy(k).wait_recv()
        kept[k] = (kept[k].astype(F32) + y_in[k].astype(F32)).astype(BF)
        for d in range(1, n_z):
            z_copy(k, d).start()

    def gather_z(k):
        part, s = place(k)
        value = kept[k, z].astype(F32)
        for d in range(1, n_z):
            z_copy(k, d).wait_recv()
            value += z_in[k, d].astype(F32)
        summed[part, sub_rows(s), :] = value

    split_lag, y_lag, z_lag = 1, 3, 6

    def advance(k):
        @pl.when(k < n_chunks)
        def _():
            share(k)

        @pl.when((k >= split_lag) & (k - split_lag < n_chunks))
        def _():
            split(k - split_lag)

        @pl.when((k >= y_lag) & (k - y_lag < n_chunks))
        def _():
            spread_z(k - y_lag)

        @pl.when(k >= z_lag)
        def _():
            gather_z(k - z_lag)

    def early():
        share(0)

    local_step(1, current, collect, early)

    def loop(k, carry):
        advance(k)
        return carry

    lax.fori_loop(1, n_chunks + z_lag, loop, 0)
    for part in range(parts):
        final[part] = summed[part].T
    final_copy().start()

    weight_total = weights_ref[0]
    step_total = weights_ref[0] * steps_ref[0]
    for i in range(1, 2 * n_pos):
        weight_total += weights_ref[i]
        step_total += weights_ref[i] * steps_ref[i]
    weight_total = weight_total.astype(F32)
    step_total = step_total.astype(F32)
    control = control_ref[...]
    lost = step_total * (control - control.astype(BF).astype(F32))
    final_copy().wait_recv()
    mine = final[:, pl.ds(owner_at, owner_span), :]
    theirs = final_in[...]
    step_out[...] = (jnp.where(b == 0, mine, theirs) + lost) / weight_total
    control_out[...] = jnp.where(b == 0, theirs, mine) / weight_total

    @pl.when(away)
    def _():
        target_copy().wait_send()
        for part in range(parts):
            corr_copy(part).wait_send()
            for s in range(n_sub):
                return_copy(part, s).wait_send()

    @pl.when(home)
    def _():
        for group in range(2):
            cross_copy(group).wait_send()

    pack_copy().wait_send()
    emb_copy().wait_send()
    for group in range(2):
        for d in range(1, n_z):
            model_along(group, d, z).wait_send()
        for row in range(n_z):
            model_beside(group, 0, row).wait_send()
            for line in range(2):
                model_partner(group, line, row).wait_send()
    for part in range(parts):
        current_copy(part).wait_send()
        for s in range(n_sub):
            share_copy(part, s).wait_send()
            grad_store(part, s).wait()
    for k in range(n_chunks):
        y_copy(k).wait_send()
        for d in range(1, n_z):
            z_copy(k, d).wait_send()
    final_copy().wait_send()


def paired_body(
    token_ids,
    target,
    embedding,
    norm_gain,
    global_model,
    global_control,
    client_control,
    local_steps,
    client_weight,
):
    n_clients = lax.axis_size("clients")
    n_pos = n_clients // 2
    n_z = n_pos // 2
    parts, half, owner_span = global_model.shape
    width = owner_span * n_clients
    span = 2 * owner_span
    rows = token_ids.shape[1]
    depth = 2 * half
    sub = 64
    n_chunks = parts * (half // sub)
    pairs = [(c, f) for c in range(n_clients) for f in range(2)]
    to_role = [(c * 2 + f, (c - c % 2 + f) * 2 + c % 2) for c, f in pairs]
    to_across = [(c * 2 + f, (c - c % 2 + f) * 2 + 1 - c % 2) for c, f in pairs]
    ids = jnp.concatenate(
        [
            lax.ppermute(token_ids[0], ("clients", "fsdp"), to_role),
            lax.ppermute(token_ids[0], ("clients", "fsdp"), to_across),
        ]
    )
    emb_columns = embedding.at[ids].get(mode="promise_in_bounds")

    n_sem = 6 + 6 * n_z + 3 * n_pos + 4 * parts + n_chunks * (3 + n_z)
    vmem = pltpu.VMEM
    scratch = [
        vmem((2, parts, span, half), BF),
        vmem((parts, depth, width), BF),
        vmem((parts, depth, width), BF),
        vmem((parts, half, width), BF),
        vmem((parts, half, width), F32),
        vmem((parts, half, width), BF),
        vmem((parts, half, width), BF),
        vmem((rows, depth), BF),
        vmem((rows, depth), BF),
        vmem((rows, depth), BF),
        vmem((depth, rows), BF),
        vmem((rows, width), F32),
        vmem((rows, width), F32),
        vmem((rows, width), BF),
        vmem((rows, depth), BF),
        vmem((depth, rows), BF),
        vmem((rows, width), BF),
        vmem((rows, width), BF),
        vmem((parts, half, width), BF),
        vmem((parts, half, width), BF),
        vmem((2, parts, half, width), BF),
        vmem((parts, half, width), BF),
        vmem((n_chunks, n_z, sub, span), BF),
        vmem((n_chunks, n_z, sub, span), BF),
        vmem((n_chunks, n_z, sub, span), BF),
        vmem((n_chunks, n_z, sub, span), BF),
        vmem((parts, half, span), F32),
        vmem((parts, span, half), F32),
        vmem((parts, owner_span, half), F32),
        pltpu.SemaphoreType.DMA((3 + n_chunks,)),
        pltpu.SemaphoreType.DMA((n_sem,)),
        pltpu.SemaphoreType.DMA((n_sem,)),
    ]
    smem = pl.BlockSpec(memory_space=pltpu.SMEM)
    anywhere = pl.BlockSpec(memory_space=pl.ANY)
    inside = pl.BlockSpec(memory_space=pltpu.VMEM)
    step_sum, control_sum, grad_rows = pl.pallas_call(
        functools.partial(round_kernel, n_z),
        out_shape=(
            jax.ShapeDtypeStruct((parts, owner_span, half), F32),
            jax.ShapeDtypeStruct((parts, owner_span, half), F32),
            jax.ShapeDtypeStruct((parts, half, width), BF),
        ),
        in_specs=[smem, smem, anywhere, anywhere, inside, inside, inside, anywhere],
        out_specs=(inside, inside, anywhere),
        scratch_shapes=scratch,
        compiler_params=pltpu.CompilerParams(
            collective_id=0, has_side_effects=True, vmem_limit_bytes=67043328
        ),
    )(
        local_steps,
        client_weight,
        emb_columns,
        target[0],
        norm_gain[None, :],
        jnp.swapaxes(global_model, 1, 2),
        jnp.swapaxes(global_control, 1, 2),
        client_control[0],
    )
    return (
        jnp.swapaxes(step_sum, 1, 2),
        jnp.swapaxes(control_sum, 1, 2),
        grad_rows.astype(F32)[None],
    )


def solution(mesh):
    placed = (
        P("clients", "fsdp"),
        P("clients", "fsdp", None),
        P(None, "fsdp"),
        P(),
        P(None, "fsdp", "clients"),
        P(None, "fsdp", "clients"),
        P("clients", None, "fsdp", None),
        P(),
        P(),
    )
    paired = mesh.shape["fsdp"] == 2 and mesh.shape["clients"] % 4 == 0
    return jax.shard_map(
        paired_body if paired else general_body,
        mesh=mesh,
        in_specs=placed,
        out_specs=(
            P(None, "fsdp", "clients"),
            P(None, "fsdp", "clients"),
            P("clients", None, "fsdp", None),
        ),
        check_vma=False,
    )
```

```python
import functools
import math

import jax
import jax.numpy as jnp
from jax import lax
from jax.experimental import pallas as pl
from jax.experimental.pallas import tpu as pltpu
from jax.sharding import PartitionSpec as P

LOCAL = 2


learning_rate = 0.005
norm_eps = 1e-06


def gelu_pair(pre_act):
    return jax.vjp(lambda inputs: jax.nn.gelu(inputs, approximate=True), pre_act)


def contract_rows(left, right):
    return lax.dot_general(
        left, right, (((0,), (0,)), ((), ())), preferred_element_type=jnp.float32
    )


def pack_owners(array, owners):
    parts, rows, columns = array.shape
    width = columns // owners
    split = array.reshape(parts, 2, rows // 2, owners, width)
    return split.transpose(3, 0, 2, 1, 4).reshape(owners, parts, rows // 2, 2 * width)


def unpack_owner(array):
    parts, half, width = array.shape
    split = array.reshape(parts, half, 2, width // 2)
    return split.transpose(0, 2, 1, 3).reshape(parts, 2 * half, width // 2)


def general_body(
    token_ids,
    target,
    embedding,
    norm_gain,
    global_model,
    global_control,
    client_control,
    local_steps,
    client_weight,
):
    n_clients = lax.axis_size("clients")
    n_fsdp = lax.axis_size("fsdp")
    client_index = lax.axis_index("clients")
    fsdp_index = lax.axis_index("fsdp")
    paired = n_fsdp == 2 and n_clients % 2 == 0
    if paired:
        core = client_index % 2
        role_client = client_index - core + fsdp_index
        block = core
        swap_pairs = [
            (c * 2 + f, ((c - c % 2) + f) * 2 + c % 2) for c in range(n_clients) for f in range(2)
        ]
        core_pairs = [(c, c ^ 1) for c in range(n_clients)]
    else:
        role_client = client_index
        block = fsdp_index

    def swap_roles(array):
        if not paired:
            return array
        return lax.ppermute(array, ("clients", "fsdp"), swap_pairs)

    def gather_rows(array):
        if not paired:
            return lax.all_gather(array, "fsdp", axis=0, tiled=True)
        other = lax.ppermute(array, "clients", core_pairs)
        return jnp.concatenate(
            [jnp.where(core == 0, array, other), jnp.where(core == 0, other, array)], axis=0
        )

    def reduce_rows(term):
        if not paired:
            return lax.psum_scatter(term, "fsdp", scatter_dimension=0, tiled=True).astype(
                jnp.float32
            )
        rows = term.shape[0] // 2
        own = lax.dynamic_slice_in_dim(term, core * rows, rows, axis=0)
        sent = lax.dynamic_slice_in_dim(term, (1 - core) * rows, rows, axis=0)
        received = lax.ppermute(sent, "clients", core_pairs)
        return own.astype(jnp.float32) + received.astype(jnp.float32)

    tok_rows = target.shape[1]
    group_rows = tok_rows * n_fsdp
    loss_scale = 1.0 / math.sqrt(group_rows)
    all_ids = lax.all_gather(swap_roles(token_ids), "fsdp", axis=1, tiled=True)
    emb_columns = jnp.take(embedding, all_ids[0], axis=0)
    embedded = lax.all_to_all(emb_columns, "fsdp", split_axis=0, concat_axis=1, tiled=True)
    widened = embedded.astype(jnp.float32)
    inv_norm = lax.rsqrt(jnp.mean(widened * widened, axis=1, keepdims=True) + norm_eps)
    normed = (widened * inv_norm * norm_gain).astype(jnp.bfloat16)
    target_rows = swap_roles(target[0]).astype(jnp.float32)
    model_columns = lax.all_gather(
        global_model.astype(jnp.bfloat16), "fsdp", axis=1, tiled=True
    )
    model_full = lax.all_gather(model_columns, "clients", axis=2, tiled=True)
    control_rows = lax.all_gather(
        global_control.astype(jnp.bfloat16), "clients", axis=2, tiled=True
    ).astype(global_control.dtype)
    slots = jnp.arange(local_steps.shape[0])
    step_count = jnp.sum(jnp.where(slots == client_index, local_steps, 0))
    role_steps = jnp.sum(jnp.where(slots == role_client, local_steps, 0))
    own_weight = jnp.sum(jnp.where(slots == client_index, client_weight, 0)).astype(jnp.float32)
    weight_total = jnp.sum(client_weight).astype(jnp.float32)
    correction = control_rows - client_control[0]
    parts, rows = correction.shape[0], correction.shape[1]
    role_correction = [
        swap_roles(correction[part].astype(jnp.bfloat16)).astype(jnp.float32)
        for part in range(parts)
    ]
    role_model = lax.dynamic_slice_in_dim(model_full, block * rows, rows, axis=1).astype(
        jnp.float32
    )
    gathered = [model_full[part] for part in range(parts)]
    pseudo = [jnp.zeros_like(role_correction[part]) for part in range(parts)]
    summed = [jnp.zeros_like(role_correction[part]) for part in range(parts)]
    for local_step in range(LOCAL):
        if local_step > 0:
            gathered = [
                gather_rows(
                    (role_model[part] - learning_rate * pseudo[part]).astype(jnp.bfloat16)
                )
                for part in range(parts)
            ]
        gate_pre = jnp.dot(normed, gathered[0], preferred_element_type=jnp.float32)
        up_pre = jnp.dot(normed, gathered[1], preferred_element_type=jnp.float32)
        gate_act, gelu_back = gelu_pair(gate_pre)
        hidden = (gate_act * up_pre).astype(jnp.bfloat16)
        projected = lax.dot_general(
            hidden, gathered[2], (((1,), (1,)), ((), ())), preferred_element_type=jnp.float32
        )
        out_grad = ((widened + projected - target_rows) * loss_scale).astype(jnp.bfloat16)
        outer_term = contract_rows(out_grad, hidden).astype(jnp.bfloat16)
        hidden_grad = jnp.dot(out_grad, gathered[2], preferred_element_type=jnp.float32)
        gate_grad = gelu_back(hidden_grad * up_pre)[0].astype(jnp.bfloat16)
        up_grad = (hidden_grad * gate_act).astype(jnp.bfloat16)
        gate_term = contract_rows(normed, gate_grad).astype(jnp.bfloat16)
        up_term = contract_rows(normed, up_grad).astype(jnp.bfloat16)
        grads = [reduce_rows(term) for term in (gate_term, up_term, outer_term)]
        step_mask = (local_step < role_steps).astype(jnp.float32)
        for part in range(parts):
            pseudo[part] = pseudo[part] + step_mask * (grads[part] + role_correction[part])
            summed[part] = summed[part] + step_mask * grads[part]
    own_grads = jnp.stack(
        [swap_roles(summed[part].astype(jnp.bfloat16)).astype(jnp.float32) for part in range(parts)]
    )
    taken = jnp.sum((jnp.arange(LOCAL) < step_count).astype(jnp.float32))
    own_pseudo = own_grads + taken * correction
    update = client_control[0] - control_rows + own_pseudo / step_count.astype(jnp.float32)
    packed = jnp.concatenate(
        [
            pack_owners((own_weight * own_pseudo).astype(jnp.bfloat16), n_clients),
            pack_owners((own_weight * update).astype(jnp.bfloat16), n_clients),
        ],
        axis=1,
    )
    sums = lax.psum_scatter(packed, "clients", scatter_dimension=0, tiled=True)[0]
    sums = unpack_owner(sums).astype(jnp.float32) / weight_total
    return (sums[:parts], sums[parts:], update[None])


MESH = pl.DeviceIdType.MESH
TILE = 256
BF = jnp.bfloat16
F32 = jnp.float32


def gelu_parts(x):
    cubic = 0.044715
    scale = math.sqrt(2.0 / math.pi)
    square = x * x
    t = jnp.tanh(scale * x * (1.0 + cubic * square))
    half = 0.5 * (1.0 + t)
    slope = half + (0.5 * scale) * x * (1.0 - t * t) * (1.0 + (3.0 * cubic) * square)
    return x * half, slope


def dot(left, right, left_dim=1, right_dim=0):
    return lax.dot_general(
        left, right, (((left_dim,), (right_dim,)), ((), ())), preferred_element_type=F32
    )


def round_kernel(
    n_z,
    steps_ref,
    weights_ref,
    emb_ref,
    target_ref,
    gain_ref,
    model_ref,
    control_ref,
    own_ref,
    step_out,
    control_out,
    grad_out,
    packed,
    model,
    current,
    g_rows,
    c_rows,
    corr,
    role_corr,
    emb,
    target,
    normed,
    normed_t,
    act,
    slope_up,
    hidden,
    out_grad,
    out_grad_t,
    gate_grad,
    up_grad,
    term_out,
    term_own,
    term_in,
    kept,
    y_out,
    y_in,
    z_in,
    summed,
    final,
    final_in,
    local_sem,
    send_sem,
    recv_sem,
):
    parts, half, width = own_ref.shape
    rows = emb.shape[0]
    depth = 2 * half
    n_pos = 2 * n_z
    span = width // n_pos
    owner_span = span // 2
    sub = kept.shape[2]
    n_sub = half // sub
    client = lax.axis_index("clients")
    x = lax.axis_index("fsdp")
    b = lax.rem(client, 2)
    p = client // 2
    y = lax.rem(p, 2)
    z = p // 2
    home = b == x
    away = b != x
    role_client = 2 * p + x
    half_at = pl.multiple_of(b * half, half)
    other_at = pl.multiple_of((1 - b) * half, half)
    own_rows = pl.ds(half_at, half)
    other_rows = pl.ds(other_at, half)
    owner_at = pl.multiple_of(b * owner_span, owner_span)

    partner = {"clients": 2 * p + 1 - b, "fsdp": x}
    across = {"clients": client, "fsdp": 1 - x}
    swap = {"clients": 2 * p + 1 - b, "fsdp": 1 - x}
    beside = {"clients": 2 * (2 * z + 1 - y) + b, "fsdp": x}

    def along(d):
        return {"clients": 2 * (2 * lax.rem(z + d, n_z) + y) + b, "fsdp": x}

    def behind(d):
        return lax.rem(z + n_z - d, n_z)

    def position(line, row):
        return 2 * row + (y if line == 0 else 1 - y)

    def columns(pos):
        return pl.ds(pl.multiple_of(pos * span, span), span)

    n_chunks = parts * n_sub
    groups = ((0, parts - 1), (parts - 1, 1))
    counts = dict(
        pack=1, emb=1, target=1, cross=2, gz=n_z, gy=n_z, gp=n_pos, mz=2 * n_z, my=2 * n_z,
        mp=2 * n_pos, corr=parts, term0=parts, term1=parts, cur=parts, ret=n_chunks,
        share=n_chunks, ry=n_chunks, rz=n_chunks * n_z, final=parts,
    )
    base = {}
    total = 0
    for name, count in counts.items():
        base[name] = total
        total += count

    def remote(src, dst, name, index, device):
        k = base[name] + index
        return pltpu.make_async_remote_copy(
            src_ref=src, dst_ref=dst, send_sem=send_sem.at[k], recv_sem=recv_sem.at[k],
            device_id=device, device_id_type=MESH,
        )

    def pack_copy():
        window = packed.at[:, :, pl.ds(owner_at, owner_span), :]
        return remote(window, window, "pack", 0, partner)

    def emb_copy():
        return remote(
            emb_ref.at[pl.ds(rows, rows), :],
            emb.at[:, pl.ds(pl.multiple_of(x * half, half), half)],
            "emb", 0, across,
        )

    def target_copy():
        return remote(target_ref, target, "target", 0, swap)

    quarter = half // 2
    g_own = pl.ds(pl.multiple_of(jnp.where(home, 0, quarter), quarter), quarter)

    def g_window(pos):
        return g_rows.at[:, g_own, columns(pos)]

    def model_window(group, pos):
        first, count = groups[group]
        return model.at[pl.ds(first, count), own_rows, columns(pos)]

    def g_along(d, row):
        window = g_window(position(0, row))
        return remote(window, window, "gz", d, along(d))

    def g_beside(line, row):
        window = g_window(position(line, row))
        return remote(window, window, "gy", row, beside)

    def g_partner(line, row):
        window = g_window(position(line, row))
        return remote(window, window, "gp", line * n_z + row, partner)

    def cross_copy(group):
        window = model_window(group, p)
        return remote(window, window, "cross", group, across)

    def model_along(group, d, row):
        window = model_window(group, position(0, row))
        return remote(window, window, "mz", group * n_z + d, along(d))

    def model_beside(group, line, row):
        window = model_window(group, position(line, row))
        return remote(window, window, "my", group * n_z + row, beside)

    def model_partner(group, line, row):
        window = model_window(group, position(line, row))
        return remote(window, window, "mp", group * n_pos + line * n_z + row, partner)

    def corr_copy(part):
        return remote(corr.at[part], role_corr.at[part], "corr", part, swap)

    def term_copy(step, part):
        return remote(
            term_out.at[part], term_in.at[part], "term%d" % step, part, partner
        )

    def current_copy(part):
        window = current.at[part, own_rows, :]
        return remote(window, window, "cur", part, partner)

    def sub_rows(s):
        return pl.ds(pl.multiple_of(s * sub, sub), sub)

    def return_copy(part, s):
        return remote(
            role_corr.at[part, sub_rows(s), :], g_rows.at[part, sub_rows(s), :],
            "ret", part * n_sub + s, swap,
        )

    def share_copy(part, s):
        return remote(
            term_out.at[part, sub_rows(s), :], model.at[part, sub_rows(s), :],
            "share", part * n_sub + s, partner,
        )

    def y_copy(k):
        return remote(y_out.at[k], y_in.at[k], "ry", k, beside)

    def z_copy(k, d):
        return remote(
            kept.at[k, lax.rem(z + d, n_z)], z_in.at[k, d], "rz", k * n_z + d, along(d)
        )

    def final_copy(part):
        at = pl.ds(pl.multiple_of((1 - b) * owner_span, owner_span), owner_span)
        return remote(final.at[part, at, :], final_in.at[part], "final", part, partner)

    def grad_store(part, s):
        return pltpu.make_async_copy(
            term_in.at[part, sub_rows(s), :], grad_out.at[part, sub_rows(s), :],
            local_sem.at[3 + part * n_sub + s],
        )

    barrier = pltpu.get_barrier_semaphore()
    for peer in [partner, across, swap, beside]:
        pl.semaphore_signal(barrier, inc=1, device_id=peer, device_id_type=MESH)
    for d in range(1, n_z):
        pl.semaphore_signal(barrier, inc=1, device_id=along(d), device_id_type=MESH)
    pl.semaphore_wait(barrier, 3 + n_z)

    own_load = pltpu.make_async_copy(own_ref, c_rows, local_sem.at[0])
    emb_load = pltpu.make_async_copy(
        emb_ref.at[pl.ds(0, rows), :],
        emb.at[:, pl.ds(pl.multiple_of(x * half, half), half)],
        local_sem.at[1],
    )
    target_load = pltpu.make_async_copy(target_ref, target, local_sem.at[2])

    packed[0, :, pl.ds(owner_at, owner_span), :] = model_ref[...].astype(BF)
    packed[1, :, pl.ds(owner_at, owner_span), :] = control_ref[...].astype(BF)

    pack_copy().start()
    own_load.start()
    emb_load.start()
    pl.when(home)(target_load.start)
    pack_copy().wait_recv()

    @pl.when(home)
    def _():
        for part in range(parts):
            model[part, own_rows, columns(p)] = packed[0, part].T
        for group in range(2):
            cross_copy(group).start()
        for part in range(parts):
            g_rows[part, :quarter, columns(p)] = packed[1, part].T[:quarter]

    @pl.when(away)
    def _():
        for part in range(parts):
            g_rows[part, quarter:, columns(p)] = packed[1, part].T[quarter:]

    for d in range(1, n_z):
        g_along(d, z).start()
    g_beside(0, z).start()
    g_partner(0, z).start()
    pl.when(home)(emb_copy().start)
    for group in range(2):
        pl.when(away)(cross_copy(group).wait_recv)
        for d in range(1, n_z):
            model_along(group, d, z).start()
        model_beside(group, 0, z).start()
        model_partner(group, 0, z).start()

    @pl.when(away)
    def _():
        emb_copy().start()
        target_copy().start()

    for d in range(1, n_z):
        row = behind(d)
        g_along(d, row).wait_recv()
        g_beside(0, row).start()
        g_partner(0, row).start()
    for row in range(n_z):
        g_beside(1, row).wait_recv()
        g_partner(1, row).start()
    for line in range(2):
        for row in range(n_z):
            g_partner(line, row).wait_recv()
    for d in range(1, n_z):
        g_along(d, z).wait_send()
    for row in range(n_z):
        g_beside(0, row).wait_send()
        for line in range(2):
            g_partner(line, row).wait_send()
    own_load.wait()

    chunk = half // 6
    for part in (2, 0, 1):

        def correct(i, carry):
            at = pl.ds(pl.multiple_of(i * chunk, chunk), chunk)
            value = (g_rows[part, at, :].astype(F32) - c_rows[part, at, :]).astype(BF)
            corr[part, at, :] = value

            @pl.when(home)
            def _():
                role_corr[part, at, :] = value

            return carry

        lax.fori_loop(0, 6, correct, 0)

        @pl.when(away)
        def _():
            corr_copy(part).start()

    emb_load.wait()
    emb_copy().wait_recv()
    block = rows // 5

    def normalise(i, carry):
        at = pl.ds(pl.multiple_of(i * block, block), block)
        widened = emb[at, :].astype(F32)
        inv_norm = lax.rsqrt(jnp.mean(widened * widened, axis=1, keepdims=True) + norm_eps)
        value = (widened * inv_norm * gain_ref[...][None, :]).astype(BF)
        normed[at, :] = value
        normed_t[:, at] = value.T
        return carry

    lax.fori_loop(0, 5, normalise, 0)

    def relay(group):
        for d in range(1, n_z):
            row = behind(d)
            model_along(group, d, row).wait_recv()
            model_beside(group, 0, row).start()
            model_partner(group, 0, row).start()

    def settle(group):
        for row in range(n_z):
            model_beside(group, 1, row).wait_recv()
            model_partner(group, 1, row).start()

    def arrive(group):
        for line in range(2):
            for row in range(n_z):
                model_partner(group, line, row).wait_recv()

    relay(0)
    settle(0)
    relay(1)
    arrive(0)

    loss_scale = 1.0 / math.sqrt(2 * rows)
    n_tiles = width // TILE

    def tile_at(j):
        return pl.ds(pl.multiple_of(j * TILE, TILE), TILE)

    def half_product(left, left_rows, right, store):
        def product(j, carry):
            store(j, dot(left[left_rows, :], right[:, tile_at(j)]).astype(BF))
            return carry

        lax.fori_loop(0, n_tiles, product, 0, unroll=True)

    def local_step(step, weights, finish, between):
        def forward(j, carry):
            cols = tile_at(j)
            gate_act, slope = gelu_parts(dot(normed[...], weights[0, :, cols]))
            up_pre = dot(normed[...], weights[1, :, cols])
            act[:, cols] = gate_act.astype(BF)
            slope_up[:, cols] = (slope * up_pre).astype(BF)
            hidden[:, cols] = (gate_act * up_pre).astype(BF)
            return carry

        lax.fori_loop(0, n_tiles, forward, 0, unroll=True)
        if step == 0:
            settle(1)
            arrive(1)

            @pl.when(away)
            def _():
                target_copy().wait_recv()

            @pl.when(home)
            def _():
                target_load.wait()

        def project(j, carry):
            cols = tile_at(j)
            projected = dot(hidden[...], weights[2, cols, :], 1, 1)
            value = (
                (emb[:, cols].astype(F32) + projected - target[:, cols].astype(F32)) * loss_scale
            ).astype(BF)
            out_grad[:, cols] = value
            out_grad_t[cols, :] = value.T
            return carry

        lax.fori_loop(0, depth // TILE, project, 0, unroll=True)

        def term_other(part, left, right):
            def store(j, value):
                term_out[part, :, tile_at(j)] = value

            if step > 0:
                term_copy(step - 1, part).wait_send()
            half_product(left, other_rows, right, store)
            term_copy(step, part).start()

        def term_mine(part, left, right):
            def store(j, value):
                term_own[part, :, tile_at(j)] = value

            half_product(left, own_rows, right, store)

        term_other(2, out_grad_t, hidden)
        term_mine(2, out_grad_t, hidden)
        if step > 0:
            finish(2)

        def backward(j, carry):
            cols = tile_at(j)
            hidden_grad = dot(out_grad[...], weights[2, :, cols])
            gate_grad[:, cols] = (hidden_grad * slope_up[:, cols]).astype(BF)
            up_grad[:, cols] = (hidden_grad * act[:, cols]).astype(BF)
            return carry

        lax.fori_loop(0, n_tiles, backward, 0, unroll=True)
        if step == 0:
            finish(2)
        term_other(0, normed_t, gate_grad)
        term_other(1, normed_t, up_grad)
        between(0)
        term_mine(0, normed_t, gate_grad)
        between(1)
        term_mine(1, normed_t, up_grad)
        between(2)
        finish(0)
        finish(1)

    def update(part):
        term_copy(0, part).wait_recv()

        @pl.when(away)
        def _():
            corr_copy(part).wait_recv()

        def apply(i, carry):
            at = pl.ds(pl.multiple_of(i * chunk, chunk), chunk)
            model_at = pl.ds(pl.multiple_of(half_at + i * chunk, chunk), chunk)
            grads = term_own[part, at, :].astype(F32) + term_in[part, at, :].astype(F32)
            c_rows[part, at, :] = grads
            pseudo = grads + role_corr[part, at, :].astype(F32)
            current[part, model_at, :] = (
                model[part, model_at, :].astype(F32) - learning_rate * pseudo
            ).astype(BF)
            return carry

        lax.fori_loop(0, 6, apply, 0)
        current_copy(part).start()

    second = (steps_ref[role_client] > 1).astype(F32)

    def collect(part):
        term_copy(1, part).wait_recv()
        for s in range(n_sub):
            at = sub_rows(s)
            grads = term_own[part, at, :].astype(F32) + term_in[part, at, :].astype(F32)
            role_corr[part, at, :] = (c_rows[part, at, :] + second * grads).astype(BF)

            @pl.when(away)
            def _():
                return_copy(part, s).start()

    local_step(0, model, update, lambda k: None)
    pack_copy().wait_send()
    emb_copy().wait_send()
    for group in range(2):
        pl.when(home)(cross_copy(group).wait_send)
        for d in range(1, n_z):
            model_along(group, d, z).wait_send()
        for row in range(n_z):
            model_beside(group, 0, row).wait_send()
            for line in range(2):
                model_partner(group, line, row).wait_send()

    @pl.when(away)
    def _():
        target_copy().wait_send()
        for part in range(parts):
            corr_copy(part).wait_send()

    for part in range(parts):
        current_copy(part).wait_recv()
    weight = weights_ref[client].astype(F32)
    taken = steps_ref[client].astype(F32)
    inverse = 1.0 / taken

    def place(k):
        return lax.rem(k // n_sub + parts - 1, parts), lax.rem(k, n_sub)

    def share(k):
        part, s = place(k)
        at = sub_rows(s)

        @pl.when(s == 0)
        def _():
            term_copy(1, part).wait_send()

        def spread(source):
            value = source[part, at, :].astype(F32)
            averaged = inverse * value
            summed = value + taken * corr[part, at, :].astype(F32)
            term_in[part, at, :] = averaged.astype(BF)
            mine = jnp.where(b == 0, summed, averaged)
            theirs = jnp.where(b == 0, averaged, summed)
            term_own[part, at, :] = (weight * mine).astype(BF)
            term_out[part, at, :] = (weight * theirs).astype(BF)

        @pl.when(home)
        def _():
            spread(role_corr)

        @pl.when(away)
        def _():
            return_copy(part, s).wait_recv()
            spread(g_rows)

        share_copy(part, s).start()
        grad_store(part, s).start()

    def split(k):
        part, s = place(k)
        at = sub_rows(s)
        share_copy(part, s).wait_recv()
        for row in range(n_z):
            for line in range(2):
                cols = columns(position(line, row))
                value = (
                    term_own[part, at, cols].astype(F32) + model[part, at, cols].astype(F32)
                ).astype(BF)
                if line == 0:
                    kept[k, row] = value
                else:
                    y_out[k, row] = value
        y_copy(k).start()

    def spread_z(k):
        y_copy(k).wait_recv()
        kept[k] = (kept[k].astype(F32) + y_in[k].astype(F32)).astype(BF)
        for d in range(1, n_z):
            z_copy(k, d).start()

    def gather_z(k):
        part, s = place(k)
        value = kept[k, z].astype(F32)
        for d in range(1, n_z):
            z_copy(k, d).wait_recv()
            value += z_in[k, d].astype(F32)
        summed[part, sub_rows(s), :] = value
        y_copy(k).wait_send()
        for d in range(1, n_z):
            z_copy(k, d).wait_send()
        share_copy(part, s).wait_send()
        grad_store(part, s).wait()
        pl.when(away)(return_copy(part, s).wait_send)

        @pl.when(s == n_sub - 1)
        def _():
            final[part] = summed[part].T
            final_copy(part).start()

    split_lag, y_lag, z_lag = 1, 3, 6

    def advance(k):
        @pl.when(k < n_chunks)
        def _():
            share(k)

        @pl.when((k >= split_lag) & (k - split_lag < n_chunks))
        def _():
            split(k - split_lag)

        @pl.when((k >= y_lag) & (k - y_lag < n_chunks))
        def _():
            spread_z(k - y_lag)

        @pl.when(k >= z_lag)
        def _():
            gather_z(k - z_lag)

    local_step(1, current, collect, advance)
    for part in range(parts):
        current_copy(part).wait_send()

    def loop(k, carry):
        advance(k)
        return carry

    lax.fori_loop(3, n_chunks + z_lag, loop, 0)

    weight_total = weights_ref[0]
    step_total = weights_ref[0] * steps_ref[0]
    for i in range(1, 2 * n_pos):
        weight_total += weights_ref[i]
        step_total += weights_ref[i] * steps_ref[i]
    weight_total = weight_total.astype(F32)
    step_total = step_total.astype(F32)
    control = control_ref[...]
    lost = step_total * (control - control.astype(BF).astype(F32))
    for part in range(parts):
        final_copy(part).wait_recv()
    mine = final[:, pl.ds(owner_at, owner_span), :]
    theirs = final_in[...]
    step_out[...] = (jnp.where(b == 0, mine, theirs) + lost) / weight_total
    control_out[...] = jnp.where(b == 0, theirs, mine) / weight_total

    for part in range(parts):
        final_copy(part).wait_send()


def widen_kernel(step_ref, control_ref, grad_ref, step_out, control_out, grad_out):
    @pl.when(pl.program_id(0) == 0)
    def _():
        step_out[...] = step_ref[...]
        control_out[...] = control_ref[...]

    grad_out[...] = grad_ref[...].astype(F32)


def paired_body(
    token_ids,
    target,
    embedding,
    norm_gain,
    global_model,
    global_control,
    client_control,
    local_steps,
    client_weight,
):
    n_clients = lax.axis_size("clients")
    n_pos = n_clients // 2
    n_z = n_pos // 2
    parts, half, owner_span = global_model.shape
    width = owner_span * n_clients
    span = 2 * owner_span
    rows = token_ids.shape[1]
    depth = 2 * half
    sub = 64
    n_chunks = parts * (half // sub)
    pairs = [(c, f) for c in range(n_clients) for f in range(2)]
    to_role = [(c * 2 + f, (c - c % 2 + f) * 2 + c % 2) for c, f in pairs]
    to_across = [(c * 2 + f, (c - c % 2 + f) * 2 + 1 - c % 2) for c, f in pairs]
    ids = jnp.concatenate(
        [
            lax.ppermute(token_ids[0], ("clients", "fsdp"), to_role),
            lax.ppermute(token_ids[0], ("clients", "fsdp"), to_across),
        ]
    )
    emb_columns = embedding.at[ids].get(mode="promise_in_bounds")

    n_sem = 5 + 6 * n_z + 3 * n_pos + 5 * parts + n_chunks * (3 + n_z)
    vmem = pltpu.VMEM
    scratch = [
        vmem((2, parts, span, half), BF),
        vmem((parts, depth, width), BF),
        vmem((parts, depth, width), BF),
        vmem((parts, half, width), BF),
        vmem((parts, half, width), F32),
        vmem((parts, half, width), BF),
        vmem((parts, half, width), BF),
        vmem((rows, depth), BF),
        vmem((rows, depth), BF),
        vmem((rows, depth), BF),
        vmem((depth, rows), BF),
        vmem((rows, width), BF),
        vmem((rows, width), BF),
        vmem((rows, width), BF),
        vmem((rows, depth), BF),
        vmem((depth, rows), BF),
        vmem((rows, width), BF),
        vmem((rows, width), BF),
        vmem((parts, half, width), BF),
        vmem((parts, half, width), BF),
        vmem((parts, half, width), BF),
        vmem((n_chunks, n_z, sub, span), BF),
        vmem((n_chunks, n_z, sub, span), BF),
        vmem((n_chunks, n_z, sub, span), BF),
        vmem((n_chunks, n_z, sub, span), BF),
        vmem((parts, half, span), F32),
        vmem((parts, span, half), F32),
        vmem((parts, owner_span, half), F32),
        pltpu.SemaphoreType.DMA((3 + n_chunks,)),
        pltpu.SemaphoreType.DMA((n_sem,)),
        pltpu.SemaphoreType.DMA((n_sem,)),
    ]
    smem = pl.BlockSpec(memory_space=pltpu.SMEM)
    anywhere = pl.BlockSpec(memory_space=pl.ANY)
    inside = pl.BlockSpec(memory_space=pltpu.VMEM)
    step_sum, control_sum, grad_rows = pl.pallas_call(
        functools.partial(round_kernel, n_z),
        out_shape=(
            jax.ShapeDtypeStruct((parts, owner_span, half), F32),
            jax.ShapeDtypeStruct((parts, owner_span, half), F32),
            jax.ShapeDtypeStruct((parts, half, width), BF),
        ),
        in_specs=[smem, smem, anywhere, anywhere, inside, inside, inside, anywhere],
        out_specs=(inside, inside, anywhere),
        scratch_shapes=scratch,
        compiler_params=pltpu.CompilerParams(
            collective_id=0, has_side_effects=True, vmem_limit_bytes=67043328
        ),
    )(
        local_steps,
        client_weight,
        emb_columns,
        target[0],
        norm_gain,
        jnp.swapaxes(global_model, 1, 2),
        jnp.swapaxes(global_control, 1, 2),
        client_control[0],
    )
    block = half // 2
    small = pl.BlockSpec((parts, owner_span, half), lambda i: (0, 0, 0))
    large = pl.BlockSpec((block, width), lambda i: (i, 0))
    step_sum, control_sum, update = pl.pallas_call(
        widen_kernel,
        out_shape=(
            jax.ShapeDtypeStruct((parts, owner_span, half), F32),
            jax.ShapeDtypeStruct((parts, owner_span, half), F32),
            jax.ShapeDtypeStruct((parts * half, width), F32),
        ),
        grid=(parts * half // block,),
        in_specs=[small, small, large],
        out_specs=(small, small, large),
    )(step_sum, control_sum, grad_rows.reshape(parts * half, width))
    return (
        jnp.swapaxes(step_sum, 1, 2),
        jnp.swapaxes(control_sum, 1, 2),
        update.reshape(1, parts, half, width),
    )


def solution(mesh):
    placed = (
        P("clients", "fsdp"),
        P("clients", "fsdp", None),
        P(None, "fsdp"),
        P(),
        P(None, "fsdp", "clients"),
        P(None, "fsdp", "clients"),
        P("clients", None, "fsdp", None),
        P(),
        P(),
    )
    paired = mesh.shape["fsdp"] == 2 and mesh.shape["clients"] % 4 == 0
    return jax.shard_map(
        paired_body if paired else general_body,
        mesh=mesh,
        in_specs=placed,
        out_specs=(
            P(None, "fsdp", "clients"),
            P(None, "fsdp", "clients"),
            P("clients", None, "fsdp", None),
        ),
        check_vma=False,
    )
```

```python
import functools
import math

import jax
import jax.numpy as jnp
from jax import lax
from jax.experimental import pallas as pl
from jax.experimental.pallas import tpu as pltpu
from jax.sharding import PartitionSpec as P

LOCAL = 2


learning_rate = 0.005
norm_eps = 1e-06


def gelu_pair(pre_act):
    return jax.vjp(lambda inputs: jax.nn.gelu(inputs, approximate=True), pre_act)


def contract_rows(left, right):
    return lax.dot_general(
        left, right, (((0,), (0,)), ((), ())), preferred_element_type=jnp.float32
    )


def pack_owners(array, owners):
    parts, rows, columns = array.shape
    width = columns // owners
    split = array.reshape(parts, 2, rows // 2, owners, width)
    return split.transpose(3, 0, 2, 1, 4).reshape(owners, parts, rows // 2, 2 * width)


def unpack_owner(array):
    parts, half, width = array.shape
    split = array.reshape(parts, half, 2, width // 2)
    return split.transpose(0, 2, 1, 3).reshape(parts, 2 * half, width // 2)


def general_body(
    token_ids,
    target,
    embedding,
    norm_gain,
    global_model,
    global_control,
    client_control,
    local_steps,
    client_weight,
):
    n_clients = lax.axis_size("clients")
    n_fsdp = lax.axis_size("fsdp")
    client_index = lax.axis_index("clients")
    fsdp_index = lax.axis_index("fsdp")
    paired = n_fsdp == 2 and n_clients % 2 == 0
    if paired:
        core = client_index % 2
        role_client = client_index - core + fsdp_index
        block = core
        swap_pairs = [
            (c * 2 + f, ((c - c % 2) + f) * 2 + c % 2) for c in range(n_clients) for f in range(2)
        ]
        core_pairs = [(c, c ^ 1) for c in range(n_clients)]
    else:
        role_client = client_index
        block = fsdp_index

    def swap_roles(array):
        if not paired:
            return array
        return lax.ppermute(array, ("clients", "fsdp"), swap_pairs)

    def gather_rows(array):
        if not paired:
            return lax.all_gather(array, "fsdp", axis=0, tiled=True)
        other = lax.ppermute(array, "clients", core_pairs)
        return jnp.concatenate(
            [jnp.where(core == 0, array, other), jnp.where(core == 0, other, array)], axis=0
        )

    def reduce_rows(term):
        if not paired:
            return lax.psum_scatter(term, "fsdp", scatter_dimension=0, tiled=True).astype(
                jnp.float32
            )
        rows = term.shape[0] // 2
        own = lax.dynamic_slice_in_dim(term, core * rows, rows, axis=0)
        sent = lax.dynamic_slice_in_dim(term, (1 - core) * rows, rows, axis=0)
        received = lax.ppermute(sent, "clients", core_pairs)
        return own.astype(jnp.float32) + received.astype(jnp.float32)

    tok_rows = target.shape[1]
    group_rows = tok_rows * n_fsdp
    loss_scale = 1.0 / math.sqrt(group_rows)
    all_ids = lax.all_gather(swap_roles(token_ids), "fsdp", axis=1, tiled=True)
    emb_columns = jnp.take(embedding, all_ids[0], axis=0)
    embedded = lax.all_to_all(emb_columns, "fsdp", split_axis=0, concat_axis=1, tiled=True)
    widened = embedded.astype(jnp.float32)
    inv_norm = lax.rsqrt(jnp.mean(widened * widened, axis=1, keepdims=True) + norm_eps)
    normed = (widened * inv_norm * norm_gain).astype(jnp.bfloat16)
    target_rows = swap_roles(target[0]).astype(jnp.float32)
    model_columns = lax.all_gather(
        global_model.astype(jnp.bfloat16), "fsdp", axis=1, tiled=True
    )
    model_full = lax.all_gather(model_columns, "clients", axis=2, tiled=True)
    control_rows = lax.all_gather(
        global_control.astype(jnp.bfloat16), "clients", axis=2, tiled=True
    ).astype(global_control.dtype)
    slots = jnp.arange(local_steps.shape[0])
    step_count = jnp.sum(jnp.where(slots == client_index, local_steps, 0))
    role_steps = jnp.sum(jnp.where(slots == role_client, local_steps, 0))
    own_weight = jnp.sum(jnp.where(slots == client_index, client_weight, 0)).astype(jnp.float32)
    weight_total = jnp.sum(client_weight).astype(jnp.float32)
    correction = control_rows - client_control[0]
    parts, rows = correction.shape[0], correction.shape[1]
    role_correction = [
        swap_roles(correction[part].astype(jnp.bfloat16)).astype(jnp.float32)
        for part in range(parts)
    ]
    role_model = lax.dynamic_slice_in_dim(model_full, block * rows, rows, axis=1).astype(
        jnp.float32
    )
    gathered = [model_full[part] for part in range(parts)]
    pseudo = [jnp.zeros_like(role_correction[part]) for part in range(parts)]
    summed = [jnp.zeros_like(role_correction[part]) for part in range(parts)]
    for local_step in range(LOCAL):
        if local_step > 0:
            gathered = [
                gather_rows(
                    (role_model[part] - learning_rate * pseudo[part]).astype(jnp.bfloat16)
                )
                for part in range(parts)
            ]
        gate_pre = jnp.dot(normed, gathered[0], preferred_element_type=jnp.float32)
        up_pre = jnp.dot(normed, gathered[1], preferred_element_type=jnp.float32)
        gate_act, gelu_back = gelu_pair(gate_pre)
        hidden = (gate_act * up_pre).astype(jnp.bfloat16)
        projected = lax.dot_general(
            hidden, gathered[2], (((1,), (1,)), ((), ())), preferred_element_type=jnp.float32
        )
        out_grad = ((widened + projected - target_rows) * loss_scale).astype(jnp.bfloat16)
        outer_term = contract_rows(out_grad, hidden).astype(jnp.bfloat16)
        hidden_grad = jnp.dot(out_grad, gathered[2], preferred_element_type=jnp.float32)
        gate_grad = gelu_back(hidden_grad * up_pre)[0].astype(jnp.bfloat16)
        up_grad = (hidden_grad * gate_act).astype(jnp.bfloat16)
        gate_term = contract_rows(normed, gate_grad).astype(jnp.bfloat16)
        up_term = contract_rows(normed, up_grad).astype(jnp.bfloat16)
        grads = [reduce_rows(term) for term in (gate_term, up_term, outer_term)]
        step_mask = (local_step < role_steps).astype(jnp.float32)
        for part in range(parts):
            pseudo[part] = pseudo[part] + step_mask * (grads[part] + role_correction[part])
            summed[part] = summed[part] + step_mask * grads[part]
    own_grads = jnp.stack(
        [swap_roles(summed[part].astype(jnp.bfloat16)).astype(jnp.float32) for part in range(parts)]
    )
    taken = jnp.sum((jnp.arange(LOCAL) < step_count).astype(jnp.float32))
    own_pseudo = own_grads + taken * correction
    update = client_control[0] - control_rows + own_pseudo / step_count.astype(jnp.float32)
    packed = jnp.concatenate(
        [
            pack_owners((own_weight * own_pseudo).astype(jnp.bfloat16), n_clients),
            pack_owners((own_weight * update).astype(jnp.bfloat16), n_clients),
        ],
        axis=1,
    )
    sums = lax.psum_scatter(packed, "clients", scatter_dimension=0, tiled=True)[0]
    sums = unpack_owner(sums).astype(jnp.float32) / weight_total
    return (sums[:parts], sums[parts:], update[None])


MESH = pl.DeviceIdType.MESH
TILE = 256
BF = jnp.bfloat16
F32 = jnp.float32


def gelu_parts(x):
    cubic = 0.044715
    scale = math.sqrt(2.0 / math.pi)
    square = x * x
    t = jnp.tanh(scale * x * (1.0 + cubic * square))
    half = 0.5 * (1.0 + t)
    slope = half + (0.5 * scale) * x * (1.0 - t * t) * (1.0 + (3.0 * cubic) * square)
    return x * half, slope


def dot(left, right, left_dim=1, right_dim=0):
    return lax.dot_general(
        left, right, (((left_dim,), (right_dim,)), ((), ())), preferred_element_type=F32
    )


def semaphore_counts(parts, n_z, n_chunks):
    arrivals = dict(
        ids=2, pack=1, emb=1, target=1, cross=2, gz=n_z, gy=n_z, gp=1, mz=2 * n_z, my=2 * n_z,
        mp=2, corr=parts, term0=parts, term1=parts, cur=1, ret=n_chunks, share=n_chunks,
        ry=n_chunks, rz=n_chunks, final=1,
    )
    return arrivals, len(arrivals) + 2 * parts + 2


def round_kernel(
    n_z,
    steps_ref,
    weights_ref,
    ids_ref,
    table_ref,
    target_ref,
    gain_ref,
    model_ref,
    control_ref,
    own_ref,
    step_out,
    control_out,
    grad_out,
    table,
    ids_in,
    ids,
    emb_out,
    packed,
    model,
    current,
    g_rows,
    c_rows,
    corr,
    role_corr,
    emb,
    target,
    normed,
    normed_t,
    act,
    slope_up,
    hidden,
    out_grad,
    out_grad_t,
    gate_grad,
    up_grad,
    term_out,
    term_own,
    term_in,
    kept,
    y_out,
    y_in,
    z_in,
    summed,
    final,
    final_in,
    local_sem,
    send_sem,
    recv_sem,
):
    parts, half, width = own_ref.shape
    rows = emb.shape[0]
    depth = 2 * half
    n_pos = 2 * n_z
    span = width // n_pos
    owner_span = span // 2
    sub = kept.shape[2]
    n_sub = half // sub
    client = lax.axis_index("clients")
    x = lax.axis_index("fsdp")
    b = lax.rem(client, 2)
    p = client // 2
    y = lax.rem(p, 2)
    z = p // 2
    home = b == x
    away = b != x
    role_client = 2 * p + x
    half_at = pl.multiple_of(b * half, half)
    other_at = pl.multiple_of((1 - b) * half, half)
    own_rows = pl.ds(half_at, half)
    other_rows = pl.ds(other_at, half)
    owner_at = pl.multiple_of(b * owner_span, owner_span)

    partner = {"clients": 2 * p + 1 - b, "fsdp": x}
    across = {"clients": client, "fsdp": 1 - x}
    swap = {"clients": 2 * p + 1 - b, "fsdp": 1 - x}
    beside = {"clients": 2 * (2 * z + 1 - y) + b, "fsdp": x}

    def along(d):
        return {"clients": 2 * (2 * lax.rem(z + d, n_z) + y) + b, "fsdp": x}

    def behind(d):
        return lax.rem(z + n_z - d, n_z)

    def position(line, row):
        return 2 * row + (y if line == 0 else 1 - y)

    def columns(pos):
        return pl.ds(pl.multiple_of(pos * span, span), span)

    n_chunks = parts * n_sub
    groups = ((0, parts - 1), (parts - 1, 1))
    arrivals, _ = semaphore_counts(parts, n_z, n_chunks)
    base = {}
    total = 0
    for name, count in arrivals.items():
        base[name] = total
        total += count
    kinds = list(arrivals)

    def remote(src, dst, name, index, device, leave=None):
        if leave is None:
            leave = kinds.index(name)
        return pltpu.make_async_remote_copy(
            src_ref=src, dst_ref=dst, send_sem=send_sem.at[leave],
            recv_sem=recv_sem.at[base[name] + index],
            device_id=device, device_id_type=MESH,
        )

    def all_sent(window, name):
        remote(window, window, name, 0, partner).wait_send()

    def pack_copy():
        window = packed.at[:, :, pl.ds(owner_at, owner_span), :]
        return remote(window, window, "pack", 0, partner)

    emb_columns = pl.ds(pl.multiple_of(x * half, half), half)

    def ids_copy(slot, device):
        return remote(
            ids_ref, ids_in.at[slot], "ids", slot, device, len(kinds) + 2 * parts + slot
        )

    def emb_copy():
        return remote(
            emb_out, emb.at[:, emb_columns], "emb", 0, across,
        )

    def target_copy():
        return remote(target_ref, target, "target", 0, swap)

    quarter = half // 2
    g_own = pl.ds(pl.multiple_of(jnp.where(home, 0, quarter), quarter), quarter)

    def g_window(pos):
        return g_rows.at[:, g_own, columns(pos)]

    def model_window(group, pos):
        first, count = groups[group]
        return model.at[pl.ds(first, count), own_rows, columns(pos)]

    def g_along(d, row):
        window = g_window(position(0, row))
        return remote(window, window, "gz", d, along(d))

    def g_beside(line, row):
        window = g_window(position(line, row))
        return remote(window, window, "gy", row, beside)

    def g_partner(line, row):
        window = g_window(position(line, row))
        return remote(window, window, "gp", 0, partner)

    def cross_copy(group):
        window = model_window(group, p)
        return remote(window, window, "cross", group, across)

    def model_along(group, d, row):
        window = model_window(group, position(0, row))
        return remote(window, window, "mz", group * n_z + d, along(d))

    def model_beside(group, line, row):
        window = model_window(group, position(line, row))
        return remote(window, window, "my", group * n_z + row, beside)

    def model_partner(group, line, row):
        window = model_window(group, position(line, row))
        return remote(window, window, "mp", group, partner)

    def corr_copy(part):
        return remote(corr.at[part], role_corr.at[part], "corr", part, swap)

    def term_copy(step, part):
        return remote(
            term_out.at[part], term_in.at[part], "term%d" % step, part, partner,
            len(kinds) + step * parts + part,
        )

    def current_copy(part):
        window = current.at[part, own_rows, :]
        return remote(window, window, "cur", 0, partner)

    def sub_rows(s):
        return pl.ds(pl.multiple_of(s * sub, sub), sub)

    def return_copy(part, s):
        return remote(
            role_corr.at[part, sub_rows(s), :], g_rows.at[part, sub_rows(s), :],
            "ret", part * n_sub + s, swap,
        )

    def share_copy(part, s):
        return remote(
            term_out.at[part, sub_rows(s), :], model.at[part, sub_rows(s), :],
            "share", part * n_sub + s, partner,
        )

    def y_copy(k):
        return remote(y_out.at[k], y_in.at[k], "ry", k, beside)

    def z_copy(k, d):
        return remote(
            kept.at[k, lax.rem(z + d, n_z)], z_in.at[k, d], "rz", k, along(d)
        )

    def final_copy(part):
        at = pl.ds(pl.multiple_of((1 - b) * owner_span, owner_span), owner_span)
        return remote(final.at[part, at, :], final_in.at[part], "final", 0, partner)

    def grad_store(part, s):
        return pltpu.make_async_copy(
            term_in.at[part, sub_rows(s), :], grad_out.at[part, sub_rows(s), :],
            local_sem.at[4],
        )

    barrier = pltpu.get_barrier_semaphore()
    for peer in [partner, across, swap, beside]:
        pl.semaphore_signal(barrier, inc=1, device_id=peer, device_id_type=MESH)
    for d in range(1, n_z):
        pl.semaphore_signal(barrier, inc=1, device_id=along(d), device_id_type=MESH)
    pl.semaphore_wait(barrier, 3 + n_z)

    own_load = pltpu.make_async_copy(own_ref, c_rows, local_sem.at[0])
    table_load = pltpu.make_async_copy(table_ref, table, local_sem.at[1])
    table_load.start()

    @pl.when(home)
    def _():
        ids_copy(1, across).start()
        ids_in[0] = ids_ref[...]

    @pl.when(away)
    def _():
        ids_copy(0, swap).start()
        ids_copy(1, partner).start()

    target_load = pltpu.make_async_copy(target_ref, target, local_sem.at[2])

    packed[0, :, pl.ds(owner_at, owner_span), :] = model_ref[...].astype(BF)
    packed[1, :, pl.ds(owner_at, owner_span), :] = control_ref[...].astype(BF)

    pack_copy().start()
    own_load.start()
    pl.when(home)(target_load.start)
    pack_copy().wait_recv()

    @pl.when(home)
    def _():
        for part in range(parts):
            model[part, own_rows, columns(p)] = packed[0, part].T
        for group in range(2):
            cross_copy(group).start()
        for part in range(parts):
            g_rows[part, :quarter, columns(p)] = packed[1, part].T[:quarter]

    @pl.when(away)
    def _():
        for part in range(parts):
            g_rows[part, quarter:, columns(p)] = packed[1, part].T[quarter:]

    for d in range(1, n_z):
        g_along(d, z).start()
    g_beside(0, z).start()
    g_partner(0, z).start()
    for group in range(2):
        pl.when(away)(cross_copy(group).wait_recv)
        for d in range(1, n_z):
            model_along(group, d, z).start()
        model_beside(group, 0, z).start()
        model_partner(group, 0, z).start()
    pl.when(away)(target_copy().start)

    ids_copy(1, across).wait_recv()
    pl.when(away)(ids_copy(0, swap).wait_recv)
    ids_load = pltpu.make_async_copy(ids_in, ids, local_sem.at[3])
    ids_load.start()
    ids_load.wait()
    table_load.wait()
    sublane = lax.broadcasted_iota(jnp.int32, (8, half), 0)

    def pick(slot, first, count, target_rows):
        def block(i, carry):
            at = (first + i) * 16
            eights = []
            for group in range(2):
                value = jnp.zeros((8, half), F32)
                for r in range(8):
                    token = ids[slot, 0, at + group * 8 + r]
                    aligned = token // 8
                    tile = table[aligned].astype(F32)
                    found = jnp.where(sublane == token - 8 * aligned, tile, 0.0)
                    line = jnp.sum(found, axis=0, keepdims=True)
                    value = jnp.where(sublane == r, line, value)
                eights.append(value)
            target_rows(
                pl.ds(pl.multiple_of(at, 16), 16), jnp.concatenate(eights, axis=0).astype(BF)
            )
            return carry

        lax.fori_loop(0, count, block, 0)

    def to_across(at, value):
        emb_out[at, :] = value

    def to_own(at, value):
        emb[at, emb_columns] = value

    n_blocks = rows // 16
    piece = n_blocks // 4

    def g_relay(d):
        row = behind(d)
        g_along(d, row).wait_recv()
        g_beside(0, row).start()
        g_partner(0, row).start()

    pick(1, 0, piece, to_across)
    pick(1, piece, piece, to_across)
    g_relay(1)
    pick(1, 2 * piece, piece, to_across)
    for d in range(2, n_z):
        g_relay(d)
    pick(1, 3 * piece, n_blocks - 3 * piece, to_across)
    emb_copy().start()
    for row in range(n_z):
        pick(0, row * piece, piece if row < 3 else n_blocks - 3 * piece, to_own)
        g_beside(1, row).wait_recv()
        g_partner(1, row).start()
    g_arrived = g_rows.at[:, pl.ds(pl.multiple_of(jnp.where(home, quarter, 0), quarter), quarter), :]
    remote(g_arrived, g_arrived, "gp", 0, partner).wait_recv()
    all_sent(g_rows.at[:, g_own, pl.ds(0, (n_z - 1) * span)], "gz")
    all_sent(g_rows.at[:, g_own, pl.ds(0, n_z * span)], "gy")
    all_sent(g_rows.at[:, g_own, :], "gp")
    own_load.wait()

    chunk = half // 6
    for part in (2, 0, 1):

        def correct(i, carry):
            at = pl.ds(pl.multiple_of(i * chunk, chunk), chunk)
            value = (g_rows[part, at, :].astype(F32) - c_rows[part, at, :]).astype(BF)
            corr[part, at, :] = value

            @pl.when(home)
            def _():
                role_corr[part, at, :] = value

            return carry

        lax.fori_loop(0, 6, correct, 0)

        @pl.when(away)
        def _():
            corr_copy(part).start()

    emb_copy().wait_recv()
    block = rows // 5

    def normalise(i, carry):
        at = pl.ds(pl.multiple_of(i * block, block), block)
        widened = emb[at, :].astype(F32)
        inv_norm = lax.rsqrt(jnp.mean(widened * widened, axis=1, keepdims=True) + norm_eps)
        value = (widened * inv_norm * gain_ref[...][None, :]).astype(BF)
        normed[at, :] = value
        normed_t[:, at] = value.T
        return carry

    lax.fori_loop(0, 5, normalise, 0)

    def relay(group):
        for d in range(1, n_z):
            row = behind(d)
            model_along(group, d, row).wait_recv()
            model_beside(group, 0, row).start()
            model_partner(group, 0, row).start()

    def settle(group):
        for row in range(n_z):
            model_beside(group, 1, row).wait_recv()
            model_partner(group, 1, row).start()

    def arrive(group):
        first, count = groups[group]
        window = model.at[pl.ds(first, count), other_rows, :]
        remote(window, window, "mp", group, partner).wait_recv()

    relay(0)
    settle(0)
    relay(1)
    arrive(0)

    loss_scale = 1.0 / math.sqrt(2 * rows)
    n_tiles = width // TILE

    def tile_at(j):
        return pl.ds(pl.multiple_of(j * TILE, TILE), TILE)

    def half_product(left, left_rows, right, store):
        def product(j, carry):
            store(j, dot(left[left_rows, :], right[:, tile_at(j)]).astype(BF))
            return carry

        lax.fori_loop(0, n_tiles, product, 0, unroll=True)

    def local_step(step, weights, finish, between):
        def forward(j, carry):
            cols = tile_at(j)
            gate_act, slope = gelu_parts(dot(normed[...], weights[0, :, cols]))
            up_pre = dot(normed[...], weights[1, :, cols])
            act[:, cols] = gate_act.astype(BF)
            slope_up[:, cols] = (slope * up_pre).astype(BF)
            hidden[:, cols] = (gate_act * up_pre).astype(BF)
            return carry

        lax.fori_loop(0, n_tiles, forward, 0, unroll=True)
        if step == 0:
            settle(1)
            arrive(1)

            @pl.when(away)
            def _():
                target_copy().wait_recv()

            @pl.when(home)
            def _():
                target_load.wait()

        def project(j, carry):
            cols = tile_at(j)
            projected = dot(hidden[...], weights[2, cols, :], 1, 1)
            value = (
                (emb[:, cols].astype(F32) + projected - target[:, cols].astype(F32)) * loss_scale
            ).astype(BF)
            out_grad[:, cols] = value
            out_grad_t[cols, :] = value.T
            return carry

        lax.fori_loop(0, depth // TILE, project, 0, unroll=True)

        def term_other(part, left, right):
            def store(j, value):
                term_out[part, :, tile_at(j)] = value

            if step > 0:
                term_copy(step - 1, part).wait_send()
            half_product(left, other_rows, right, store)
            term_copy(step, part).start()

        def term_mine(part, left, right):
            def store(j, value):
                term_own[part, :, tile_at(j)] = value

            half_product(left, own_rows, right, store)

        term_other(2, out_grad_t, hidden)
        term_mine(2, out_grad_t, hidden)
        if step > 0:
            finish(2)

        def backward(j, carry):
            cols = tile_at(j)
            hidden_grad = dot(out_grad[...], weights[2, :, cols])
            gate_grad[:, cols] = (hidden_grad * slope_up[:, cols]).astype(BF)
            up_grad[:, cols] = (hidden_grad * act[:, cols]).astype(BF)
            return carry

        lax.fori_loop(0, n_tiles, backward, 0, unroll=True)
        if step == 0:
            finish(2)
        term_other(0, normed_t, gate_grad)
        term_other(1, normed_t, up_grad)
        between(0)
        term_mine(0, normed_t, gate_grad)
        between(1)
        term_mine(1, normed_t, up_grad)
        between(2)
        finish(0)
        finish(1)

    def update(part):
        term_copy(0, part).wait_recv()

        @pl.when(away)
        def _():
            corr_copy(part).wait_recv()

        def apply(i, carry):
            at = pl.ds(pl.multiple_of(i * chunk, chunk), chunk)
            model_at = pl.ds(pl.multiple_of(half_at + i * chunk, chunk), chunk)
            grads = term_own[part, at, :].astype(F32) + term_in[part, at, :].astype(F32)
            c_rows[part, at, :] = grads
            pseudo = grads + role_corr[part, at, :].astype(F32)
            current[part, model_at, :] = (
                model[part, model_at, :].astype(F32) - learning_rate * pseudo
            ).astype(BF)
            return carry

        lax.fori_loop(0, 6, apply, 0)
        current_copy(part).start()

    second = (steps_ref[role_client] > 1).astype(F32)

    def collect(part):
        term_copy(1, part).wait_recv()
        for s in range(n_sub):
            at = sub_rows(s)
            grads = term_own[part, at, :].astype(F32) + term_in[part, at, :].astype(F32)
            role_corr[part, at, :] = (c_rows[part, at, :] + second * grads).astype(BF)

            @pl.when(away)
            def _():
                return_copy(part, s).start()

    local_step(0, model, update, lambda k: None)
    pack_copy().wait_send()
    emb_copy().wait_send()
    ids_copy(1, across).wait_send()
    all_sent(model.at[:, own_rows, pl.ds(0, (n_z - 1) * span)], "mz")
    all_sent(model.at[:, own_rows, pl.ds(0, n_z * span)], "my")
    all_sent(model.at[:, own_rows, :], "mp")

    @pl.when(home)
    def _():
        all_sent(model.at[:, own_rows, columns(p)], "cross")

    @pl.when(away)
    def _():
        ids_copy(0, swap).wait_send()
        target_copy().wait_send()
        all_sent(corr, "corr")

    arrived = current.at[:, other_rows, :]
    remote(arrived, arrived, "cur", 0, partner).wait_recv()
    weight = weights_ref[client].astype(F32)
    taken = steps_ref[client].astype(F32)
    inverse = 1.0 / taken

    def place(k):
        return lax.rem(k // n_sub + parts - 1, parts), lax.rem(k, n_sub)

    def share(k):
        part, s = place(k)
        at = sub_rows(s)

        @pl.when(s == 0)
        def _():
            term_copy(1, part).wait_send()

        def spread(source):
            value = source[part, at, :].astype(F32)
            averaged = inverse * value
            summed = value + taken * corr[part, at, :].astype(F32)
            term_in[part, at, :] = averaged.astype(BF)
            mine = jnp.where(b == 0, summed, averaged)
            theirs = jnp.where(b == 0, averaged, summed)
            term_own[part, at, :] = (weight * mine).astype(BF)
            term_out[part, at, :] = (weight * theirs).astype(BF)

        @pl.when(home)
        def _():
            spread(role_corr)

        @pl.when(away)
        def _():
            return_copy(part, s).wait_recv()
            spread(g_rows)

        share_copy(part, s).start()
        grad_store(part, s).start()

    def split(k):
        part, s = place(k)
        at = sub_rows(s)
        share_copy(part, s).wait_recv()
        for row in range(n_z):
            for line in range(2):
                cols = columns(position(line, row))
                value = (
                    term_own[part, at, cols].astype(F32) + model[part, at, cols].astype(F32)
                ).astype(BF)
                if line == 0:
                    kept[k, row] = value
                else:
                    y_out[k, row] = value
        y_copy(k).start()

    def spread_z(k):
        y_copy(k).wait_recv()
        kept[k] = (kept[k].astype(F32) + y_in[k].astype(F32)).astype(BF)
        for d in range(1, n_z):
            z_copy(k, d).start()

    def gather_z(k):
        part, s = place(k)
        arrived = z_in.at[k, pl.ds(1, n_z - 1)]
        remote(arrived, arrived, "rz", k, partner).wait_recv()
        value = kept[k, z].astype(F32)
        for d in range(1, n_z):
            value += z_in[k, d].astype(F32)
        summed[part, sub_rows(s), :] = value
        @pl.when(s == n_sub - 1)
        def _():
            final[part] = summed[part].T
            final_copy(part).start()

    split_lag, y_lag, z_lag = 1, 3, 6

    def advance(k):
        @pl.when(k < n_chunks)
        def _():
            share(k)

        @pl.when((k >= split_lag) & (k - split_lag < n_chunks))
        def _():
            split(k - split_lag)

        @pl.when((k >= y_lag) & (k - y_lag < n_chunks))
        def _():
            spread_z(k - y_lag)

        @pl.when(k >= z_lag)
        def _():
            gather_z(k - z_lag)

    local_step(1, current, collect, advance)
    all_sent(current.at[:, own_rows, :], "cur")

    def loop(k, carry):
        advance(k)
        return carry

    lax.fori_loop(3, n_chunks + z_lag, loop, 0)

    weight_total = weights_ref[0]
    step_total = weights_ref[0] * steps_ref[0]
    for i in range(1, 2 * n_pos):
        weight_total += weights_ref[i]
        step_total += weights_ref[i] * steps_ref[i]
    weight_total = weight_total.astype(F32)
    step_total = step_total.astype(F32)
    control = control_ref[...]
    lost = step_total * (control - control.astype(BF).astype(F32))
    remote(final_in, final_in, "final", 0, partner).wait_recv()
    mine = final[:, pl.ds(owner_at, owner_span), :]
    theirs = final_in[...]
    step_out[...] = (jnp.where(b == 0, mine, theirs) + lost) / weight_total
    control_out[...] = jnp.where(b == 0, theirs, mine) / weight_total

    all_sent(final_in, "final")
    all_sent(y_out, "ry")
    all_sent(z_in.at[:, pl.ds(1, n_z - 1)], "rz")
    all_sent(term_out, "share")

    @pl.when(away)
    def _():
        all_sent(role_corr, "ret")

    pltpu.make_async_copy(term_in, grad_out, local_sem.at[4]).wait()


def widen_kernel(step_ref, control_ref, grad_ref, step_out, control_out, grad_out, narrow, wide, sem):
    pieces = grad_ref.shape[0]
    loads = [
        pltpu.make_async_copy(grad_ref.at[i], narrow.at[i], sem.at[0, i]) for i in range(pieces)
    ]
    stores = [
        pltpu.make_async_copy(wide.at[i], grad_out.at[i], sem.at[1, i]) for i in range(pieces)
    ]
    for load in loads:
        load.start()
    step_out[...] = step_ref[...]
    control_out[...] = control_ref[...]
    for i in range(pieces):
        loads[i].wait()
        wide[i] = narrow[i].astype(F32)
        stores[i].start()
    for store in stores:
        store.wait()


def paired_body(
    token_ids,
    target,
    embedding,
    norm_gain,
    global_model,
    global_control,
    client_control,
    local_steps,
    client_weight,
):
    n_clients = lax.axis_size("clients")
    n_pos = n_clients // 2
    n_z = n_pos // 2
    parts, half, owner_span = global_model.shape
    width = owner_span * n_clients
    span = 2 * owner_span
    rows = token_ids.shape[1]
    depth = 2 * half
    sub = 64
    n_chunks = parts * (half // sub)
    arrivals, n_send = semaphore_counts(parts, n_z, n_chunks)
    vmem = pltpu.VMEM
    scratch = [
        vmem((embedding.shape[0] // 8, 8, half), BF),
        vmem((2, 1, rows), jnp.int32),
        pltpu.SMEM((2, 1, rows), jnp.int32),
        vmem((rows, half), BF),
        vmem((2, parts, span, half), BF),
        vmem((parts, depth, width), BF),
        vmem((parts, depth, width), BF),
        vmem((parts, half, width), BF),
        vmem((parts, half, width), F32),
        vmem((parts, half, width), BF),
        vmem((parts, half, width), BF),
        vmem((rows, depth), BF),
        vmem((rows, depth), BF),
        vmem((rows, depth), BF),
        vmem((depth, rows), BF),
        vmem((rows, width), BF),
        vmem((rows, width), BF),
        vmem((rows, width), BF),
        vmem((rows, depth), BF),
        vmem((depth, rows), BF),
        vmem((rows, width), BF),
        vmem((rows, width), BF),
        vmem((parts, half, width), BF),
        vmem((parts, half, width), BF),
        vmem((parts, half, width), BF),
        vmem((n_chunks, n_z, sub, span), BF),
        vmem((n_chunks, n_z, sub, span), BF),
        vmem((n_chunks, n_z, sub, span), BF),
        vmem((n_chunks, n_z, sub, span), BF),
        vmem((parts, half, span), F32),
        vmem((parts, span, half), F32),
        vmem((parts, owner_span, half), F32),
        pltpu.SemaphoreType.DMA((5,)),
        pltpu.SemaphoreType.DMA((n_send,)),
        pltpu.SemaphoreType.DMA((sum(arrivals.values()),)),
    ]
    smem = pl.BlockSpec(memory_space=pltpu.SMEM)
    anywhere = pl.BlockSpec(memory_space=pl.ANY)
    inside = pl.BlockSpec(memory_space=pltpu.VMEM)
    step_sum, control_sum, grad_rows = pl.pallas_call(
        functools.partial(round_kernel, n_z),
        out_shape=(
            jax.ShapeDtypeStruct((parts, owner_span, half), F32),
            jax.ShapeDtypeStruct((parts, owner_span, half), F32),
            jax.ShapeDtypeStruct((parts, half, width), BF),
        ),
        in_specs=[smem, smem, inside, anywhere, anywhere, inside, inside, inside, anywhere],
        out_specs=(inside, inside, anywhere),
        scratch_shapes=scratch,
        compiler_params=pltpu.CompilerParams(
            collective_id=0, has_side_effects=True, vmem_limit_bytes=67043328
        ),
    )(
        local_steps,
        client_weight,
        token_ids,
        embedding.reshape(-1, 8, half),
        target[0],
        norm_gain,
        jnp.swapaxes(global_model, 1, 2),
        jnp.swapaxes(global_control, 1, 2),
        client_control[0],
    )
    pieces = 2 * parts
    block = parts * half // pieces
    step_sum, control_sum, update = pl.pallas_call(
        widen_kernel,
        out_shape=(
            jax.ShapeDtypeStruct((parts, owner_span, half), F32),
            jax.ShapeDtypeStruct((parts, owner_span, half), F32),
            jax.ShapeDtypeStruct((pieces, block, width), F32),
        ),
        in_specs=[inside, inside, anywhere],
        out_specs=(inside, inside, anywhere),
        scratch_shapes=[
            vmem((pieces, block, width), BF),
            vmem((pieces, block, width), F32),
            pltpu.SemaphoreType.DMA((2, pieces)),
        ],
    )(step_sum, control_sum, grad_rows.reshape(pieces, block, width))
    return (
        jnp.swapaxes(step_sum, 1, 2),
        jnp.swapaxes(control_sum, 1, 2),
        update.reshape(1, parts, half, width),
    )


def solution(mesh):
    placed = (
        P("clients", "fsdp"),
        P("clients", "fsdp", None),
        P(None, "fsdp"),
        P(),
        P(None, "fsdp", "clients"),
        P(None, "fsdp", "clients"),
        P("clients", None, "fsdp", None),
        P(),
        P(),
    )
    paired = mesh.shape["fsdp"] == 2 and mesh.shape["clients"] % 4 == 0
    return jax.shard_map(
        paired_body if paired else general_body,
        mesh=mesh,
        in_specs=placed,
        out_specs=(
            P(None, "fsdp", "clients"),
            P(None, "fsdp", "clients"),
            P("clients", None, "fsdp", None),
        ),
        check_vma=False,
    )
```

```python
import functools
import math

import jax
import jax.numpy as jnp
from jax import lax
from jax.experimental import pallas as pl
from jax.experimental.pallas import tpu as pltpu
from jax.sharding import PartitionSpec as P

LOCAL = 2


learning_rate = 0.005
norm_eps = 1e-06


def gelu_pair(pre_act):
    return jax.vjp(lambda inputs: jax.nn.gelu(inputs, approximate=True), pre_act)


def contract_rows(left, right):
    return lax.dot_general(
        left, right, (((0,), (0,)), ((), ())), preferred_element_type=jnp.float32
    )


def pack_owners(array, owners):
    parts, rows, columns = array.shape
    width = columns // owners
    split = array.reshape(parts, 2, rows // 2, owners, width)
    return split.transpose(3, 0, 2, 1, 4).reshape(owners, parts, rows // 2, 2 * width)


def unpack_owner(array):
    parts, half, width = array.shape
    split = array.reshape(parts, half, 2, width // 2)
    return split.transpose(0, 2, 1, 3).reshape(parts, 2 * half, width // 2)


def general_body(
    token_ids,
    target,
    embedding,
    norm_gain,
    global_model,
    global_control,
    client_control,
    local_steps,
    client_weight,
):
    n_clients = lax.axis_size("clients")
    n_fsdp = lax.axis_size("fsdp")
    client_index = lax.axis_index("clients")
    fsdp_index = lax.axis_index("fsdp")
    paired = n_fsdp == 2 and n_clients % 2 == 0
    if paired:
        core = client_index % 2
        role_client = client_index - core + fsdp_index
        block = core
        swap_pairs = [
            (c * 2 + f, ((c - c % 2) + f) * 2 + c % 2) for c in range(n_clients) for f in range(2)
        ]
        core_pairs = [(c, c ^ 1) for c in range(n_clients)]
    else:
        role_client = client_index
        block = fsdp_index

    def swap_roles(array):
        if not paired:
            return array
        return lax.ppermute(array, ("clients", "fsdp"), swap_pairs)

    def gather_rows(array):
        if not paired:
            return lax.all_gather(array, "fsdp", axis=0, tiled=True)
        other = lax.ppermute(array, "clients", core_pairs)
        return jnp.concatenate(
            [jnp.where(core == 0, array, other), jnp.where(core == 0, other, array)], axis=0
        )

    def reduce_rows(term):
        if not paired:
            return lax.psum_scatter(term, "fsdp", scatter_dimension=0, tiled=True).astype(
                jnp.float32
            )
        rows = term.shape[0] // 2
        own = lax.dynamic_slice_in_dim(term, core * rows, rows, axis=0)
        sent = lax.dynamic_slice_in_dim(term, (1 - core) * rows, rows, axis=0)
        received = lax.ppermute(sent, "clients", core_pairs)
        return own.astype(jnp.float32) + received.astype(jnp.float32)

    tok_rows = target.shape[1]
    group_rows = tok_rows * n_fsdp
    loss_scale = 1.0 / math.sqrt(group_rows)
    all_ids = lax.all_gather(swap_roles(token_ids), "fsdp", axis=1, tiled=True)
    emb_columns = jnp.take(embedding, all_ids[0], axis=0)
    embedded = lax.all_to_all(emb_columns, "fsdp", split_axis=0, concat_axis=1, tiled=True)
    widened = embedded.astype(jnp.float32)
    inv_norm = lax.rsqrt(jnp.mean(widened * widened, axis=1, keepdims=True) + norm_eps)
    normed = (widened * inv_norm * norm_gain).astype(jnp.bfloat16)
    target_rows = swap_roles(target[0]).astype(jnp.float32)
    model_columns = lax.all_gather(
        global_model.astype(jnp.bfloat16), "fsdp", axis=1, tiled=True
    )
    model_full = lax.all_gather(model_columns, "clients", axis=2, tiled=True)
    control_rows = lax.all_gather(
        global_control.astype(jnp.bfloat16), "clients", axis=2, tiled=True
    ).astype(global_control.dtype)
    slots = jnp.arange(local_steps.shape[0])
    step_count = jnp.sum(jnp.where(slots == client_index, local_steps, 0))
    role_steps = jnp.sum(jnp.where(slots == role_client, local_steps, 0))
    own_weight = jnp.sum(jnp.where(slots == client_index, client_weight, 0)).astype(jnp.float32)
    weight_total = jnp.sum(client_weight).astype(jnp.float32)
    correction = control_rows - client_control[0]
    parts, rows = correction.shape[0], correction.shape[1]
    role_correction = [
        swap_roles(correction[part].astype(jnp.bfloat16)).astype(jnp.float32)
        for part in range(parts)
    ]
    role_model = lax.dynamic_slice_in_dim(model_full, block * rows, rows, axis=1).astype(
        jnp.float32
    )
    gathered = [model_full[part] for part in range(parts)]
    pseudo = [jnp.zeros_like(role_correction[part]) for part in range(parts)]
    summed = [jnp.zeros_like(role_correction[part]) for part in range(parts)]
    for local_step in range(LOCAL):
        if local_step > 0:
            gathered = [
                gather_rows(
                    (role_model[part] - learning_rate * pseudo[part]).astype(jnp.bfloat16)
                )
                for part in range(parts)
            ]
        gate_pre = jnp.dot(normed, gathered[0], preferred_element_type=jnp.float32)
        up_pre = jnp.dot(normed, gathered[1], preferred_element_type=jnp.float32)
        gate_act, gelu_back = gelu_pair(gate_pre)
        hidden = (gate_act * up_pre).astype(jnp.bfloat16)
        projected = lax.dot_general(
            hidden, gathered[2], (((1,), (1,)), ((), ())), preferred_element_type=jnp.float32
        )
        out_grad = ((widened + projected - target_rows) * loss_scale).astype(jnp.bfloat16)
        outer_term = contract_rows(out_grad, hidden).astype(jnp.bfloat16)
        hidden_grad = jnp.dot(out_grad, gathered[2], preferred_element_type=jnp.float32)
        gate_grad = gelu_back(hidden_grad * up_pre)[0].astype(jnp.bfloat16)
        up_grad = (hidden_grad * gate_act).astype(jnp.bfloat16)
        gate_term = contract_rows(normed, gate_grad).astype(jnp.bfloat16)
        up_term = contract_rows(normed, up_grad).astype(jnp.bfloat16)
        grads = [reduce_rows(term) for term in (gate_term, up_term, outer_term)]
        step_mask = (local_step < role_steps).astype(jnp.float32)
        for part in range(parts):
            pseudo[part] = pseudo[part] + step_mask * (grads[part] + role_correction[part])
            summed[part] = summed[part] + step_mask * grads[part]
    own_grads = jnp.stack(
        [swap_roles(summed[part].astype(jnp.bfloat16)).astype(jnp.float32) for part in range(parts)]
    )
    taken = jnp.sum((jnp.arange(LOCAL) < step_count).astype(jnp.float32))
    own_pseudo = own_grads + taken * correction
    update = client_control[0] - control_rows + own_pseudo / step_count.astype(jnp.float32)
    packed = jnp.concatenate(
        [
            pack_owners((own_weight * own_pseudo).astype(jnp.bfloat16), n_clients),
            pack_owners((own_weight * update).astype(jnp.bfloat16), n_clients),
        ],
        axis=1,
    )
    sums = lax.psum_scatter(packed, "clients", scatter_dimension=0, tiled=True)[0]
    sums = unpack_owner(sums).astype(jnp.float32) / weight_total
    return (sums[:parts], sums[parts:], update[None])


MESH = pl.DeviceIdType.MESH
TILE = 256
BF = jnp.bfloat16
F32 = jnp.float32


def gelu_parts(x):
    cubic = 0.044715
    scale = math.sqrt(2.0 / math.pi)
    square = x * x
    t = jnp.tanh(scale * x * (1.0 + cubic * square))
    half = 0.5 * (1.0 + t)
    slope = half + (0.5 * scale) * x * (1.0 - t * t) * (1.0 + (3.0 * cubic) * square)
    return x * half, slope


def dot(left, right, left_dim=1, right_dim=0):
    return lax.dot_general(
        left, right, (((left_dim,), (right_dim,)), ((), ())), preferred_element_type=F32
    )


def semaphore_counts(parts, n_z, n_chunks):
    arrivals = dict(
        ids=2, pack=1, emb=1, target=1, cross=2, gz=n_z, gy=n_z, gp=1, mz=2 * n_z, my=2 * n_z,
        mp=2, corr=parts, term0=parts, term1=parts, cur=1, ret=n_chunks, share=n_chunks,
        ry=n_chunks, rz=n_chunks, final=1,
    )
    return arrivals, len(arrivals) + 2 * parts + 2


def round_kernel(
    n_z,
    steps_ref,
    weights_ref,
    ids_ref,
    table_ref,
    target_ref,
    gain_ref,
    model_ref,
    control_ref,
    own_ref,
    step_out,
    control_out,
    grad_out,
    table,
    ids_in,
    ids,
    emb_out,
    packed,
    model,
    current,
    g_rows,
    c_rows,
    corr,
    role_corr,
    emb,
    target,
    normed,
    normed_t,
    act,
    slope_up,
    hidden,
    out_grad,
    out_grad_t,
    gate_grad,
    up_grad,
    term_out,
    term_own,
    term_in,
    kept,
    y_out,
    y_in,
    z_in,
    summed,
    final,
    final_in,
    local_sem,
    send_sem,
    recv_sem,
):
    parts, half, width = own_ref.shape
    rows = emb.shape[0]
    depth = 2 * half
    n_pos = 2 * n_z
    span = width // n_pos
    owner_span = span // 2
    sub = kept.shape[2]
    n_sub = half // sub
    client = lax.axis_index("clients")
    x = lax.axis_index("fsdp")
    b = lax.rem(client, 2)
    p = client // 2
    y = lax.rem(p, 2)
    z = p // 2
    home = b == x
    away = b != x
    role_client = 2 * p + x
    half_at = pl.multiple_of(b * half, half)
    other_at = pl.multiple_of((1 - b) * half, half)
    own_rows = pl.ds(half_at, half)
    other_rows = pl.ds(other_at, half)
    owner_at = pl.multiple_of(b * owner_span, owner_span)

    partner = {"clients": 2 * p + 1 - b, "fsdp": x}
    across = {"clients": client, "fsdp": 1 - x}
    swap = {"clients": 2 * p + 1 - b, "fsdp": 1 - x}
    beside = {"clients": 2 * (2 * z + 1 - y) + b, "fsdp": x}

    def along(d):
        return {"clients": 2 * (2 * lax.rem(z + d, n_z) + y) + b, "fsdp": x}

    def behind(d):
        return lax.rem(z + n_z - d, n_z)

    def position(line, row):
        return 2 * row + (y if line == 0 else 1 - y)

    def columns(pos):
        return pl.ds(pl.multiple_of(pos * span, span), span)

    n_chunks = parts * n_sub
    groups = ((0, parts - 1), (parts - 1, 1))
    arrivals, _ = semaphore_counts(parts, n_z, n_chunks)
    base = {}
    total = 0
    for name, count in arrivals.items():
        base[name] = total
        total += count
    kinds = list(arrivals)

    def remote(src, dst, name, index, device, leave=None):
        if leave is None:
            leave = kinds.index(name)
        return pltpu.make_async_remote_copy(
            src_ref=src, dst_ref=dst, send_sem=send_sem.at[leave],
            recv_sem=recv_sem.at[base[name] + index],
            device_id=device, device_id_type=MESH,
        )

    def all_sent(window, name):
        remote(window, window, name, 0, partner).wait_send()

    def pack_copy():
        window = packed.at[:, :, pl.ds(owner_at, owner_span), :]
        return remote(window, window, "pack", 0, partner)

    emb_columns = pl.ds(pl.multiple_of(x * half, half), half)

    def ids_copy(slot, device):
        return remote(
            ids_ref, ids_in.at[slot], "ids", slot, device, len(kinds) + 2 * parts + slot
        )

    def emb_copy():
        return remote(
            emb_out, emb.at[:, emb_columns], "emb", 0, across,
        )

    def target_copy():
        return remote(target_ref, target, "target", 0, swap)

    quarter = half // 2
    g_own = pl.ds(pl.multiple_of(jnp.where(home, 0, quarter), quarter), quarter)

    def g_window(pos):
        return g_rows.at[:, g_own, columns(pos)]

    def model_window(group, pos):
        first, count = groups[group]
        return model.at[pl.ds(first, count), own_rows, columns(pos)]

    def g_along(d, row):
        window = g_window(position(0, row))
        return remote(window, window, "gz", d, along(d))

    def g_beside(line, row):
        window = g_window(position(line, row))
        return remote(window, window, "gy", row, beside)

    def g_partner(line, row):
        window = g_window(position(line, row))
        return remote(window, window, "gp", 0, partner)

    def cross_copy(group):
        window = model_window(group, p)
        return remote(window, window, "cross", group, across)

    def model_along(group, d, row):
        window = model_window(group, position(0, row))
        return remote(window, window, "mz", group * n_z + d, along(d))

    def model_beside(group, line, row):
        window = model_window(group, position(line, row))
        return remote(window, window, "my", group * n_z + row, beside)

    def model_partner(group, line, row):
        window = model_window(group, position(line, row))
        return remote(window, window, "mp", group, partner)

    def corr_copy(part):
        return remote(corr.at[part], role_corr.at[part], "corr", part, swap)

    def term_copy(step, part):
        return remote(
            term_out.at[part], term_in.at[part], "term%d" % step, part, partner,
            len(kinds) + step * parts + part,
        )

    def current_copy(part):
        window = current.at[part, own_rows, :]
        return remote(window, window, "cur", 0, partner)

    def sub_rows(s):
        return pl.ds(pl.multiple_of(s * sub, sub), sub)

    def return_copy(part, s):
        return remote(
            role_corr.at[part, sub_rows(s), :], g_rows.at[part, sub_rows(s), :],
            "ret", part * n_sub + s, swap,
        )

    def share_copy(part, s):
        return remote(
            term_out.at[part, sub_rows(s), :], model.at[part, sub_rows(s), :],
            "share", part * n_sub + s, partner,
        )

    def y_copy(k):
        return remote(y_out.at[k], y_in.at[k], "ry", k, beside)

    def z_copy(k, d):
        return remote(
            kept.at[k, lax.rem(z + d, n_z)], z_in.at[k, d], "rz", k, along(d)
        )

    def final_copy(part):
        at = pl.ds(pl.multiple_of((1 - b) * owner_span, owner_span), owner_span)
        return remote(final.at[part, at, :], final_in.at[part], "final", 0, partner)

    def grad_store(part, s):
        return pltpu.make_async_copy(
            term_in.at[part, sub_rows(s), :], grad_out.at[part, sub_rows(s), :],
            local_sem.at[4],
        )

    barrier = pltpu.get_barrier_semaphore()
    for peer in [partner, across, swap, beside]:
        pl.semaphore_signal(barrier, inc=1, device_id=peer, device_id_type=MESH)
    for d in range(1, n_z):
        pl.semaphore_signal(barrier, inc=1, device_id=along(d), device_id_type=MESH)
    pl.semaphore_wait(barrier, 3 + n_z)

    own_load = pltpu.make_async_copy(own_ref, c_rows, local_sem.at[0])
    table_load = pltpu.make_async_copy(table_ref, table, local_sem.at[1])
    table_load.start()

    @pl.when(home)
    def _():
        ids_copy(1, across).start()
        ids_in[0] = ids_ref[...]

    @pl.when(away)
    def _():
        ids_copy(0, swap).start()
        ids_copy(1, partner).start()

    target_load = pltpu.make_async_copy(target_ref, target, local_sem.at[2])

    packed[0, :, pl.ds(owner_at, owner_span), :] = model_ref[...].astype(BF)
    packed[1, :, pl.ds(owner_at, owner_span), :] = control_ref[...].astype(BF)

    pack_copy().start()
    own_load.start()
    pl.when(home)(target_load.start)
    pack_copy().wait_recv()

    @pl.when(home)
    def _():
        for part in range(parts):
            model[part, own_rows, columns(p)] = packed[0, part].T
        for group in range(2):
            cross_copy(group).start()
        for part in range(parts):
            g_rows[part, :quarter, columns(p)] = packed[1, part].T[:quarter]

    @pl.when(away)
    def _():
        for part in range(parts):
            g_rows[part, quarter:, columns(p)] = packed[1, part].T[quarter:]

    for d in range(1, n_z):
        g_along(d, z).start()
    g_beside(0, z).start()
    g_partner(0, z).start()
    for group in range(2):
        pl.when(away)(cross_copy(group).wait_recv)
        model_beside(group, 0, z).start()
        model_partner(group, 0, z).start()
    pl.when(away)(target_copy().start)

    ids_copy(1, across).wait_recv()
    pl.when(away)(ids_copy(0, swap).wait_recv)
    ids_load = pltpu.make_async_copy(ids_in, ids, local_sem.at[3])
    ids_load.start()
    ids_load.wait()
    table_load.wait()
    sublane = lax.broadcasted_iota(jnp.int32, (8, half), 0)

    def pick(slot, first, count, target_rows):
        def block(i, carry):
            at = (first + i) * 16
            eights = []
            for group in range(2):
                value = jnp.zeros((8, half), F32)
                for r in range(8):
                    token = ids[slot, 0, at + group * 8 + r]
                    aligned = token // 8
                    tile = table[aligned].astype(F32)
                    found = jnp.where(sublane == token - 8 * aligned, tile, 0.0)
                    line = jnp.sum(found, axis=0, keepdims=True)
                    value = jnp.where(sublane == r, line, value)
                eights.append(value)
            target_rows(
                pl.ds(pl.multiple_of(at, 16), 16), jnp.concatenate(eights, axis=0).astype(BF)
            )
            return carry

        lax.fori_loop(0, count, block, 0)

    def to_across(at, value):
        emb_out[at, :] = value

    def to_own(at, value):
        emb[at, emb_columns] = value

    n_blocks = rows // 16
    piece = n_blocks // 4

    def g_relay(d):
        row = behind(d)
        g_along(d, row).wait_recv()
        g_beside(0, row).start()
        g_partner(0, row).start()

    def relay(group, d):
        row = behind(d)
        model_along(group, d, row).wait_recv()
        model_beside(group, 0, row).start()
        model_partner(group, 0, row).start()

    def launch(group):
        for d in range(1, n_z):
            model_along(group, d, z).start()

    pick(1, 0, 2 * piece, to_across)
    g_relay(1)
    launch(0)
    pick(1, 2 * piece, n_blocks - 2 * piece, to_across)
    emb_copy().start()
    for d in range(2, n_z):
        g_relay(d)
    launch(1)
    for row in range(n_z):
        if row < 2:
            pick(0, row * piece, piece, to_own)
        g_beside(1, row).wait_recv()
        g_partner(1, row).start()
    g_arrived = g_rows.at[:, pl.ds(pl.multiple_of(jnp.where(home, quarter, 0), quarter), quarter), :]
    remote(g_arrived, g_arrived, "gp", 0, partner).wait_recv()
    all_sent(g_rows.at[:, g_own, pl.ds(0, (n_z - 1) * span)], "gz")
    all_sent(g_rows.at[:, g_own, pl.ds(0, n_z * span)], "gy")
    all_sent(g_rows.at[:, g_own, :], "gp")
    own_load.wait()

    chunk = half // 6
    for part in (2, 0, 1):

        def correct(i, carry):
            at = pl.ds(pl.multiple_of(i * chunk, chunk), chunk)
            value = (g_rows[part, at, :].astype(F32) - c_rows[part, at, :]).astype(BF)
            corr[part, at, :] = value

            @pl.when(home)
            def _():
                role_corr[part, at, :] = value

            return carry

        lax.fori_loop(0, 6, correct, 0)

        @pl.when(away)
        def _():
            corr_copy(part).start()

    for d in range(1, n_z):
        relay(0, d)
    pick(0, 2 * piece, n_blocks - 2 * piece, to_own)
    emb_copy().wait_recv()
    block = rows // 5

    def normalise(i, carry):
        at = pl.ds(pl.multiple_of(i * block, block), block)
        widened = emb[at, :].astype(F32)
        inv_norm = lax.rsqrt(jnp.mean(widened * widened, axis=1, keepdims=True) + norm_eps)
        value = (widened * inv_norm * gain_ref[...][None, :]).astype(BF)
        normed[at, :] = value
        normed_t[:, at] = value.T
        return carry

    lax.fori_loop(0, 5, normalise, 0)

    def settle(group):
        for row in range(n_z):
            model_beside(group, 1, row).wait_recv()
            model_partner(group, 1, row).start()

    def arrive(group):
        first, count = groups[group]
        window = model.at[pl.ds(first, count), other_rows, :]
        remote(window, window, "mp", group, partner).wait_recv()

    settle(0)
    for d in range(1, n_z):
        relay(1, d)
    arrive(0)

    loss_scale = 1.0 / math.sqrt(2 * rows)
    n_tiles = width // TILE

    def tile_at(j):
        return pl.ds(pl.multiple_of(j * TILE, TILE), TILE)

    def half_product(left, left_rows, right, store):
        def product(j, carry):
            store(j, dot(left[left_rows, :], right[:, tile_at(j)]).astype(BF))
            return carry

        lax.fori_loop(0, n_tiles, product, 0, unroll=True)

    def local_step(step, weights, finish, between):
        def forward(j, carry):
            cols = tile_at(j)
            gate_act, slope = gelu_parts(dot(normed[...], weights[0, :, cols]))
            up_pre = dot(normed[...], weights[1, :, cols])
            act[:, cols] = gate_act.astype(BF)
            slope_up[:, cols] = (slope * up_pre).astype(BF)
            hidden[:, cols] = (gate_act * up_pre).astype(BF)
            return carry

        lax.fori_loop(0, n_tiles, forward, 0, unroll=True)
        if step == 0:
            settle(1)
            arrive(1)

            @pl.when(away)
            def _():
                target_copy().wait_recv()

            @pl.when(home)
            def _():
                target_load.wait()

        def project(j, carry):
            cols = tile_at(j)
            projected = dot(hidden[...], weights[2, cols, :], 1, 1)
            value = (
                (emb[:, cols].astype(F32) + projected - target[:, cols].astype(F32)) * loss_scale
            ).astype(BF)
            out_grad[:, cols] = value
            out_grad_t[cols, :] = value.T
            return carry

        lax.fori_loop(0, depth // TILE, project, 0, unroll=True)

        def term_other(part, left, right):
            def store(j, value):
                term_out[part, :, tile_at(j)] = value

            if step > 0:
                term_copy(step - 1, part).wait_send()
            half_product(left, other_rows, right, store)
            term_copy(step, part).start()

        def term_mine(part, left, right):
            def store(j, value):
                term_own[part, :, tile_at(j)] = value

            half_product(left, own_rows, right, store)

        term_other(2, out_grad_t, hidden)
        term_mine(2, out_grad_t, hidden)
        if step > 0:
            finish(2)

        def backward(j, carry):
            cols = tile_at(j)
            hidden_grad = dot(out_grad[...], weights[2, :, cols])
            gate_grad[:, cols] = (hidden_grad * slope_up[:, cols]).astype(BF)
            up_grad[:, cols] = (hidden_grad * act[:, cols]).astype(BF)
            return carry

        lax.fori_loop(0, n_tiles, backward, 0, unroll=True)
        if step == 0:
            finish(2)
        term_other(0, normed_t, gate_grad)
        term_other(1, normed_t, up_grad)
        between(0)
        term_mine(0, normed_t, gate_grad)
        between(1)
        term_mine(1, normed_t, up_grad)
        between(2)
        finish(0)
        finish(1)

    def update(part):
        term_copy(0, part).wait_recv()

        @pl.when(away)
        def _():
            corr_copy(part).wait_recv()

        def apply(i, carry):
            at = pl.ds(pl.multiple_of(i * chunk, chunk), chunk)
            model_at = pl.ds(pl.multiple_of(half_at + i * chunk, chunk), chunk)
            grads = term_own[part, at, :].astype(F32) + term_in[part, at, :].astype(F32)
            c_rows[part, at, :] = grads
            pseudo = grads + role_corr[part, at, :].astype(F32)
            current[part, model_at, :] = (
                model[part, model_at, :].astype(F32) - learning_rate * pseudo
            ).astype(BF)
            return carry

        lax.fori_loop(0, 6, apply, 0)
        current_copy(part).start()

    second = (steps_ref[role_client] > 1).astype(F32)

    def collect(part):
        term_copy(1, part).wait_recv()
        for s in range(n_sub):
            at = sub_rows(s)
            grads = term_own[part, at, :].astype(F32) + term_in[part, at, :].astype(F32)
            role_corr[part, at, :] = (c_rows[part, at, :] + second * grads).astype(BF)

            @pl.when(away)
            def _():
                return_copy(part, s).start()

    local_step(0, model, update, lambda k: None)
    pack_copy().wait_send()
    emb_copy().wait_send()
    ids_copy(1, across).wait_send()
    all_sent(model.at[:, own_rows, pl.ds(0, (n_z - 1) * span)], "mz")
    all_sent(model.at[:, own_rows, pl.ds(0, n_z * span)], "my")
    all_sent(model.at[:, own_rows, :], "mp")

    @pl.when(home)
    def _():
        all_sent(model.at[:, own_rows, columns(p)], "cross")

    @pl.when(away)
    def _():
        ids_copy(0, swap).wait_send()
        target_copy().wait_send()
        all_sent(corr, "corr")

    arrived = current.at[:, other_rows, :]
    remote(arrived, arrived, "cur", 0, partner).wait_recv()
    weight = weights_ref[client].astype(F32)
    taken = steps_ref[client].astype(F32)
    inverse = 1.0 / taken

    def place(k):
        return lax.rem(k // n_sub + parts - 1, parts), lax.rem(k, n_sub)

    def share(k):
        part, s = place(k)
        at = sub_rows(s)

        @pl.when(s == 0)
        def _():
            term_copy(1, part).wait_send()

        def spread(source):
            value = source[part, at, :].astype(F32)
            averaged = inverse * value
            summed = value + taken * corr[part, at, :].astype(F32)
            term_in[part, at, :] = averaged.astype(BF)
            mine = jnp.where(b == 0, summed, averaged)
            theirs = jnp.where(b == 0, averaged, summed)
            term_own[part, at, :] = (weight * mine).astype(BF)
            term_out[part, at, :] = (weight * theirs).astype(BF)

        @pl.when(home)
        def _():
            spread(role_corr)

        @pl.when(away)
        def _():
            return_copy(part, s).wait_recv()
            spread(g_rows)

        share_copy(part, s).start()
        grad_store(part, s).start()

    def split(k):
        part, s = place(k)
        at = sub_rows(s)
        share_copy(part, s).wait_recv()
        for row in range(n_z):
            for line in range(2):
                cols = columns(position(line, row))
                value = (
                    term_own[part, at, cols].astype(F32) + model[part, at, cols].astype(F32)
                ).astype(BF)
                if line == 0:
                    kept[k, row] = value
                else:
                    y_out[k, row] = value
        y_copy(k).start()

    def spread_z(k):
        y_copy(k).wait_recv()
        kept[k] = (kept[k].astype(F32) + y_in[k].astype(F32)).astype(BF)
        for d in range(1, n_z):
            z_copy(k, d).start()

    def gather_z(k):
        part, s = place(k)
        arrived = z_in.at[k, pl.ds(1, n_z - 1)]
        remote(arrived, arrived, "rz", k, partner).wait_recv()
        value = kept[k, z].astype(F32)
        for d in range(1, n_z):
            value += z_in[k, d].astype(F32)
        summed[part, sub_rows(s), :] = value
        @pl.when(s == n_sub - 1)
        def _():
            final[part] = summed[part].T
            final_copy(part).start()

    split_lag, y_lag, z_lag = 1, 3, 6

    def advance(k):
        @pl.when(k < n_chunks)
        def _():
            share(k)

        @pl.when((k >= split_lag) & (k - split_lag < n_chunks))
        def _():
            split(k - split_lag)

        @pl.when((k >= y_lag) & (k - y_lag < n_chunks))
        def _():
            spread_z(k - y_lag)

        @pl.when(k >= z_lag)
        def _():
            gather_z(k - z_lag)

    local_step(1, current, collect, advance)
    all_sent(current.at[:, own_rows, :], "cur")

    def loop(k, carry):
        advance(k)
        return carry

    lax.fori_loop(3, n_chunks + z_lag, loop, 0)

    weight_total = weights_ref[0]
    step_total = weights_ref[0] * steps_ref[0]
    for i in range(1, 2 * n_pos):
        weight_total += weights_ref[i]
        step_total += weights_ref[i] * steps_ref[i]
    weight_total = weight_total.astype(F32)
    step_total = step_total.astype(F32)
    control = control_ref[...]
    lost = step_total * (control - control.astype(BF).astype(F32))
    remote(final_in, final_in, "final", 0, partner).wait_recv()
    mine = final[:, pl.ds(owner_at, owner_span), :]
    theirs = final_in[...]
    step_out[...] = (jnp.where(b == 0, mine, theirs) + lost) / weight_total
    control_out[...] = jnp.where(b == 0, theirs, mine) / weight_total

    all_sent(final_in, "final")
    all_sent(y_out, "ry")
    all_sent(z_in.at[:, pl.ds(1, n_z - 1)], "rz")
    all_sent(term_out, "share")

    @pl.when(away)
    def _():
        all_sent(role_corr, "ret")

    pltpu.make_async_copy(term_in, grad_out, local_sem.at[4]).wait()


def widen_kernel(
    step_ref, control_ref, grad_ref, step_out, control_out, grad_out, narrow, wide, small, sem
):
    pieces = grad_ref.shape[0]
    pairs = [(step_ref, small.at[0]), (control_ref, small.at[1])]
    pairs += [(grad_ref.at[i], narrow.at[i]) for i in range(pieces)]
    loads = [pltpu.make_async_copy(src, dst, sem.at[0, i]) for i, (src, dst) in enumerate(pairs)]
    pairs = [(small.at[0], step_out), (small.at[1], control_out)]
    pairs += [(wide.at[i], grad_out.at[i]) for i in range(pieces)]
    stores = [pltpu.make_async_copy(src, dst, sem.at[1, i]) for i, (src, dst) in enumerate(pairs)]
    for load in loads:
        load.start()
    for i, (load, store) in enumerate(zip(loads, stores)):
        load.wait()
        if i >= 2:
            wide[i - 2] = narrow[i - 2].astype(F32)
        store.start()
    for store in stores:
        store.wait()


def paired_body(
    token_ids,
    target,
    embedding,
    norm_gain,
    global_model,
    global_control,
    client_control,
    local_steps,
    client_weight,
):
    n_clients = lax.axis_size("clients")
    n_pos = n_clients // 2
    n_z = n_pos // 2
    parts, half, owner_span = global_model.shape
    width = owner_span * n_clients
    span = 2 * owner_span
    rows = token_ids.shape[1]
    depth = 2 * half
    sub = 64
    n_chunks = parts * (half // sub)
    arrivals, n_send = semaphore_counts(parts, n_z, n_chunks)
    vmem = pltpu.VMEM
    scratch = [
        vmem((embedding.shape[0] // 8, 8, half), BF),
        vmem((2, 1, rows), jnp.int32),
        pltpu.SMEM((2, 1, rows), jnp.int32),
        vmem((rows, half), BF),
        vmem((2, parts, span, half), BF),
        vmem((parts, depth, width), BF),
        vmem((parts, depth, width), BF),
        vmem((parts, half, width), BF),
        vmem((parts, half, width), F32),
        vmem((parts, half, width), BF),
        vmem((parts, half, width), BF),
        vmem((rows, depth), BF),
        vmem((rows, depth), BF),
        vmem((rows, depth), BF),
        vmem((depth, rows), BF),
        vmem((rows, width), BF),
        vmem((rows, width), BF),
        vmem((rows, width), BF),
        vmem((rows, depth), BF),
        vmem((depth, rows), BF),
        vmem((rows, width), BF),
        vmem((rows, width), BF),
        vmem((parts, half, width), BF),
        vmem((parts, half, width), BF),
        vmem((parts, half, width), BF),
        vmem((n_chunks, n_z, sub, span), BF),
        vmem((n_chunks, n_z, sub, span), BF),
        vmem((n_chunks, n_z, sub, span), BF),
        vmem((n_chunks, n_z, sub, span), BF),
        vmem((parts, half, span), F32),
        vmem((parts, span, half), F32),
        vmem((parts, owner_span, half), F32),
        pltpu.SemaphoreType.DMA((5,)),
        pltpu.SemaphoreType.DMA((n_send,)),
        pltpu.SemaphoreType.DMA((sum(arrivals.values()),)),
    ]
    smem = pl.BlockSpec(memory_space=pltpu.SMEM)
    anywhere = pl.BlockSpec(memory_space=pl.ANY)
    inside = pl.BlockSpec(memory_space=pltpu.VMEM)
    step_sum, control_sum, grad_rows = pl.pallas_call(
        functools.partial(round_kernel, n_z),
        out_shape=(
            jax.ShapeDtypeStruct((parts, owner_span, half), F32),
            jax.ShapeDtypeStruct((parts, owner_span, half), F32),
            jax.ShapeDtypeStruct((parts, half, width), BF),
        ),
        in_specs=[smem, smem, inside, anywhere, anywhere, inside, inside, inside, anywhere],
        out_specs=(inside, inside, anywhere),
        scratch_shapes=scratch,
        compiler_params=pltpu.CompilerParams(
            collective_id=0, has_side_effects=True, vmem_limit_bytes=67043328
        ),
    )(
        local_steps,
        client_weight,
        token_ids,
        embedding.reshape(-1, 8, half),
        target[0],
        norm_gain,
        jnp.swapaxes(global_model, 1, 2),
        jnp.swapaxes(global_control, 1, 2),
        client_control[0],
    )
    pieces = 2 * parts
    block = parts * half // pieces
    step_sum, control_sum, update = pl.pallas_call(
        widen_kernel,
        out_shape=(
            jax.ShapeDtypeStruct((parts, owner_span, half), F32),
            jax.ShapeDtypeStruct((parts, owner_span, half), F32),
            jax.ShapeDtypeStruct((pieces, block, width), F32),
        ),
        in_specs=[anywhere, anywhere, anywhere],
        out_specs=(anywhere, anywhere, anywhere),
        scratch_shapes=[
            vmem((pieces, block, width), BF),
            vmem((pieces, block, width), F32),
            vmem((2, parts, owner_span, half), F32),
            pltpu.SemaphoreType.DMA((2, pieces + 2)),
        ],
    )(step_sum, control_sum, grad_rows.reshape(pieces, block, width))
    return (
        jnp.swapaxes(step_sum, 1, 2),
        jnp.swapaxes(control_sum, 1, 2),
        update.reshape(1, parts, half, width),
    )


def solution(mesh):
    placed = (
        P("clients", "fsdp"),
        P("clients", "fsdp", None),
        P(None, "fsdp"),
        P(),
        P(None, "fsdp", "clients"),
        P(None, "fsdp", "clients"),
        P("clients", None, "fsdp", None),
        P(),
        P(),
    )
    paired = mesh.shape["fsdp"] == 2 and mesh.shape["clients"] % 4 == 0
    return jax.shard_map(
        paired_body if paired else general_body,
        mesh=mesh,
        in_specs=placed,
        out_specs=(
            P(None, "fsdp", "clients"),
            P(None, "fsdp", "clients"),
            P("clients", None, "fsdp", None),
        ),
        check_vma=False,
    )
```

```python
import functools
import math

import jax
import jax.numpy as jnp
from jax import lax
from jax.experimental import pallas as pl
from jax.experimental.pallas import tpu as pltpu
from jax.sharding import PartitionSpec as P

LOCAL = 2


learning_rate = 0.005
norm_eps = 1e-06


def gelu_pair(pre_act):
    return jax.vjp(lambda inputs: jax.nn.gelu(inputs, approximate=True), pre_act)


def contract_rows(left, right):
    return lax.dot_general(
        left, right, (((0,), (0,)), ((), ())), preferred_element_type=jnp.float32
    )


def pack_owners(array, owners):
    parts, rows, columns = array.shape
    width = columns // owners
    split = array.reshape(parts, 2, rows // 2, owners, width)
    return split.transpose(3, 0, 2, 1, 4).reshape(owners, parts, rows // 2, 2 * width)


def unpack_owner(array):
    parts, half, width = array.shape
    split = array.reshape(parts, half, 2, width // 2)
    return split.transpose(0, 2, 1, 3).reshape(parts, 2 * half, width // 2)


def general_body(
    token_ids,
    target,
    embedding,
    norm_gain,
    global_model,
    global_control,
    client_control,
    local_steps,
    client_weight,
):
    n_clients = lax.axis_size("clients")
    n_fsdp = lax.axis_size("fsdp")
    client_index = lax.axis_index("clients")
    fsdp_index = lax.axis_index("fsdp")
    paired = n_fsdp == 2 and n_clients % 2 == 0
    if paired:
        core = client_index % 2
        role_client = client_index - core + fsdp_index
        block = core
        swap_pairs = [
            (c * 2 + f, ((c - c % 2) + f) * 2 + c % 2) for c in range(n_clients) for f in range(2)
        ]
        core_pairs = [(c, c ^ 1) for c in range(n_clients)]
    else:
        role_client = client_index
        block = fsdp_index

    def swap_roles(array):
        if not paired:
            return array
        return lax.ppermute(array, ("clients", "fsdp"), swap_pairs)

    def gather_rows(array):
        if not paired:
            return lax.all_gather(array, "fsdp", axis=0, tiled=True)
        other = lax.ppermute(array, "clients", core_pairs)
        return jnp.concatenate(
            [jnp.where(core == 0, array, other), jnp.where(core == 0, other, array)], axis=0
        )

    def reduce_rows(term):
        if not paired:
            return lax.psum_scatter(term, "fsdp", scatter_dimension=0, tiled=True).astype(
                jnp.float32
            )
        rows = term.shape[0] // 2
        own = lax.dynamic_slice_in_dim(term, core * rows, rows, axis=0)
        sent = lax.dynamic_slice_in_dim(term, (1 - core) * rows, rows, axis=0)
        received = lax.ppermute(sent, "clients", core_pairs)
        return own.astype(jnp.float32) + received.astype(jnp.float32)

    tok_rows = target.shape[1]
    group_rows = tok_rows * n_fsdp
    loss_scale = 1.0 / math.sqrt(group_rows)
    all_ids = lax.all_gather(swap_roles(token_ids), "fsdp", axis=1, tiled=True)
    emb_columns = jnp.take(embedding, all_ids[0], axis=0)
    embedded = lax.all_to_all(emb_columns, "fsdp", split_axis=0, concat_axis=1, tiled=True)
    widened = embedded.astype(jnp.float32)
    inv_norm = lax.rsqrt(jnp.mean(widened * widened, axis=1, keepdims=True) + norm_eps)
    normed = (widened * inv_norm * norm_gain).astype(jnp.bfloat16)
    target_rows = swap_roles(target[0]).astype(jnp.float32)
    model_columns = lax.all_gather(
        global_model.astype(jnp.bfloat16), "fsdp", axis=1, tiled=True
    )
    model_full = lax.all_gather(model_columns, "clients", axis=2, tiled=True)
    control_rows = lax.all_gather(
        global_control.astype(jnp.bfloat16), "clients", axis=2, tiled=True
    ).astype(global_control.dtype)
    slots = jnp.arange(local_steps.shape[0])
    step_count = jnp.sum(jnp.where(slots == client_index, local_steps, 0))
    role_steps = jnp.sum(jnp.where(slots == role_client, local_steps, 0))
    own_weight = jnp.sum(jnp.where(slots == client_index, client_weight, 0)).astype(jnp.float32)
    weight_total = jnp.sum(client_weight).astype(jnp.float32)
    correction = control_rows - client_control[0]
    parts, rows = correction.shape[0], correction.shape[1]
    role_correction = [
        swap_roles(correction[part].astype(jnp.bfloat16)).astype(jnp.float32)
        for part in range(parts)
    ]
    role_model = lax.dynamic_slice_in_dim(model_full, block * rows, rows, axis=1).astype(
        jnp.float32
    )
    gathered = [model_full[part] for part in range(parts)]
    pseudo = [jnp.zeros_like(role_correction[part]) for part in range(parts)]
    summed = [jnp.zeros_like(role_correction[part]) for part in range(parts)]
    for local_step in range(LOCAL):
        if local_step > 0:
            gathered = [
                gather_rows(
                    (role_model[part] - learning_rate * pseudo[part]).astype(jnp.bfloat16)
                )
                for part in range(parts)
            ]
        gate_pre = jnp.dot(normed, gathered[0], preferred_element_type=jnp.float32)
        up_pre = jnp.dot(normed, gathered[1], preferred_element_type=jnp.float32)
        gate_act, gelu_back = gelu_pair(gate_pre)
        hidden = (gate_act * up_pre).astype(jnp.bfloat16)
        projected = lax.dot_general(
            hidden, gathered[2], (((1,), (1,)), ((), ())), preferred_element_type=jnp.float32
        )
        out_grad = ((widened + projected - target_rows) * loss_scale).astype(jnp.bfloat16)
        outer_term = contract_rows(out_grad, hidden).astype(jnp.bfloat16)
        hidden_grad = jnp.dot(out_grad, gathered[2], preferred_element_type=jnp.float32)
        gate_grad = gelu_back(hidden_grad * up_pre)[0].astype(jnp.bfloat16)
        up_grad = (hidden_grad * gate_act).astype(jnp.bfloat16)
        gate_term = contract_rows(normed, gate_grad).astype(jnp.bfloat16)
        up_term = contract_rows(normed, up_grad).astype(jnp.bfloat16)
        grads = [reduce_rows(term) for term in (gate_term, up_term, outer_term)]
        step_mask = (local_step < role_steps).astype(jnp.float32)
        for part in range(parts):
            pseudo[part] = pseudo[part] + step_mask * (grads[part] + role_correction[part])
            summed[part] = summed[part] + step_mask * grads[part]
    own_grads = jnp.stack(
        [swap_roles(summed[part].astype(jnp.bfloat16)).astype(jnp.float32) for part in range(parts)]
    )
    taken = jnp.sum((jnp.arange(LOCAL) < step_count).astype(jnp.float32))
    own_pseudo = own_grads + taken * correction
    update = client_control[0] - control_rows + own_pseudo / step_count.astype(jnp.float32)
    packed = jnp.concatenate(
        [
            pack_owners((own_weight * own_pseudo).astype(jnp.bfloat16), n_clients),
            pack_owners((own_weight * update).astype(jnp.bfloat16), n_clients),
        ],
        axis=1,
    )
    sums = lax.psum_scatter(packed, "clients", scatter_dimension=0, tiled=True)[0]
    sums = unpack_owner(sums).astype(jnp.float32) / weight_total
    return (sums[:parts], sums[parts:], update[None])


MESH = pl.DeviceIdType.MESH
TILE = 256
BF = jnp.bfloat16
F32 = jnp.float32


def gelu_parts(x):
    cubic = 0.044715
    scale = math.sqrt(2.0 / math.pi)
    square = x * x
    t = jnp.tanh(scale * x * (1.0 + cubic * square))
    half = 0.5 * (1.0 + t)
    slope = half + (0.5 * scale) * x * (1.0 - t * t) * (1.0 + (3.0 * cubic) * square)
    return x * half, slope


def dot(left, right, left_dim=1, right_dim=0):
    return lax.dot_general(
        left, right, (((left_dim,), (right_dim,)), ((), ())), preferred_element_type=F32
    )


def semaphore_counts(parts, n_z, n_chunks):
    arrivals = dict(
        ids=2, pack=1, emb=1, target=1, cross=2, gz=n_z, gy=n_z, gp=1, mz=2 * n_z, my=2 * n_z,
        mp=2, corr=parts, term0=parts, term1=parts, cur=1, ret=n_chunks, share=n_chunks,
        ry=n_chunks, rz=n_chunks, final=1,
    )
    return arrivals, len(arrivals) + 2 * parts + 2


def round_kernel(
    n_z,
    steps_ref,
    weights_ref,
    ids_ref,
    table_ref,
    target_ref,
    gain_ref,
    model_ref,
    control_ref,
    own_ref,
    step_out,
    control_out,
    grad_out,
    table,
    ids_in,
    ids,
    emb_out,
    packed,
    model,
    current,
    g_rows,
    c_rows,
    corr,
    role_corr,
    emb,
    target,
    normed,
    normed_t,
    act,
    slope_up,
    hidden,
    out_grad,
    out_grad_t,
    gate_grad,
    up_grad,
    term_out,
    term_own,
    term_in,
    kept,
    y_out,
    y_in,
    z_in,
    summed,
    final,
    final_in,
    local_sem,
    send_sem,
    recv_sem,
):
    parts, half, width = own_ref.shape
    rows = emb.shape[0]
    depth = 2 * half
    n_pos = 2 * n_z
    span = width // n_pos
    owner_span = span // 2
    sub = kept.shape[2]
    n_sub = half // sub
    client = lax.axis_index("clients")
    x = lax.axis_index("fsdp")
    b = lax.rem(client, 2)
    p = client // 2
    y = lax.rem(p, 2)
    z = p // 2
    home = b == x
    away = b != x
    role_client = 2 * p + x
    half_at = pl.multiple_of(b * half, half)
    other_at = pl.multiple_of((1 - b) * half, half)
    own_rows = pl.ds(half_at, half)
    other_rows = pl.ds(other_at, half)
    owner_at = pl.multiple_of(b * owner_span, owner_span)

    partner = {"clients": 2 * p + 1 - b, "fsdp": x}
    across = {"clients": client, "fsdp": 1 - x}
    swap = {"clients": 2 * p + 1 - b, "fsdp": 1 - x}
    beside = {"clients": 2 * (2 * z + 1 - y) + b, "fsdp": x}

    def along(d):
        return {"clients": 2 * (2 * lax.rem(z + d, n_z) + y) + b, "fsdp": x}

    def behind(d):
        return lax.rem(z + n_z - d, n_z)

    hop = n_z == 4

    def turn(i):
        return jnp.where(z == 0, n_z - i, i) if hop else i

    def send_tiles(copy):
        for d in range(1, n_z):
            if not hop or d == 2:
                copy(d, z).start()
            else:
                pl.when(z != (n_z - 1 if d == 1 else 0))(copy(d, z).start)

    def hop_tile(copy, d, row):
        if hop:
            pl.when((d == 2) & (z == 1))(copy(1, row, -1).start)
            pl.when((d == 2) & (z == 2))(copy(3, row, 1).start)

    def along_sent(window, name):
        if hop:
            ends = (z == 0) | (z == n_z - 1)

            @pl.when(ends)
            def _():
                all_sent(window(n_z - 2), name)

            @pl.when(jnp.logical_not(ends))
            def _():
                all_sent(window(n_z), name)

        else:
            all_sent(window(n_z - 1), name)

    def position(line, row):
        return 2 * row + (y if line == 0 else 1 - y)

    def columns(pos):
        return pl.ds(pl.multiple_of(pos * span, span), span)

    n_chunks = parts * n_sub
    groups = ((0, parts - 1), (parts - 1, 1))
    arrivals, _ = semaphore_counts(parts, n_z, n_chunks)
    base = {}
    total = 0
    for name, count in arrivals.items():
        base[name] = total
        total += count
    kinds = list(arrivals)

    def remote(src, dst, name, index, device, leave=None):
        if leave is None:
            leave = kinds.index(name)
        return pltpu.make_async_remote_copy(
            src_ref=src, dst_ref=dst, send_sem=send_sem.at[leave],
            recv_sem=recv_sem.at[base[name] + index],
            device_id=device, device_id_type=MESH,
        )

    def all_sent(window, name):
        remote(window, window, name, 0, partner).wait_send()

    def pack_copy():
        window = packed.at[:, :, pl.ds(owner_at, owner_span), :]
        return remote(window, window, "pack", 0, partner)

    emb_columns = pl.ds(pl.multiple_of(x * half, half), half)

    def ids_copy(slot, device):
        return remote(
            ids_ref, ids_in.at[slot], "ids", slot, device, len(kinds) + 2 * parts + slot
        )

    def emb_copy():
        return remote(
            emb_out, emb.at[:, emb_columns], "emb", 0, across,
        )

    def target_copy():
        return remote(target_ref, target, "target", 0, swap)

    quarter = half // 2
    g_own = pl.ds(pl.multiple_of(jnp.where(home, 0, quarter), quarter), quarter)

    def g_window(pos):
        return g_rows.at[:, g_own, columns(pos)]

    def model_window(group, pos):
        first, count = groups[group]
        return model.at[pl.ds(first, count), own_rows, columns(pos)]

    def g_along(d, row, step=None):
        window = g_window(position(0, row))
        return remote(window, window, "gz", d, along(d) if step is None else along(step + n_z))

    def g_beside(line, row):
        window = g_window(position(line, row))
        return remote(window, window, "gy", row, beside)

    def g_partner(line, row):
        window = g_window(position(line, row))
        return remote(window, window, "gp", 0, partner)

    def cross_copy(group):
        window = model_window(group, p)
        return remote(window, window, "cross", group, across)

    def model_along(group, d, row, step=None):
        window = model_window(group, position(0, row))
        return remote(
            window, window, "mz", group * n_z + d,
            along(d) if step is None else along(step + n_z),
        )

    def model_beside(group, line, row):
        window = model_window(group, position(line, row))
        return remote(window, window, "my", group * n_z + row, beside)

    def model_partner(group, line, row):
        window = model_window(group, position(line, row))
        return remote(window, window, "mp", group, partner)

    def corr_copy(part):
        return remote(corr.at[part], role_corr.at[part], "corr", part, swap)

    def term_copy(step, part):
        return remote(
            term_out.at[part], term_in.at[part], "term%d" % step, part, partner,
            len(kinds) + step * parts + part,
        )

    def current_copy(part):
        window = current.at[part, own_rows, :]
        return remote(window, window, "cur", 0, partner)

    def sub_rows(s):
        return pl.ds(pl.multiple_of(s * sub, sub), sub)

    def return_copy(part, s):
        return remote(
            role_corr.at[part, sub_rows(s), :], g_rows.at[part, sub_rows(s), :],
            "ret", part * n_sub + s, swap,
        )

    def share_copy(part, s):
        return remote(
            term_out.at[part, sub_rows(s), :], model.at[part, sub_rows(s), :],
            "share", part * n_sub + s, partner,
        )

    def y_copy(k):
        return remote(y_out.at[k], y_in.at[k], "ry", k, beside)

    def z_copy(k, d):
        return remote(
            kept.at[k, lax.rem(z + d, n_z)], z_in.at[k, d], "rz", k, along(d)
        )

    def final_copy(part):
        at = pl.ds(pl.multiple_of((1 - b) * owner_span, owner_span), owner_span)
        return remote(final.at[part, at, :], final_in.at[part], "final", 0, partner)

    def grad_store(part, s):
        return pltpu.make_async_copy(
            term_in.at[part, sub_rows(s), :], grad_out.at[part, sub_rows(s), :],
            local_sem.at[4],
        )

    barrier = pltpu.get_barrier_semaphore()
    for peer in [partner, across, swap, beside]:
        pl.semaphore_signal(barrier, inc=1, device_id=peer, device_id_type=MESH)
    for d in range(1, n_z):
        pl.semaphore_signal(barrier, inc=1, device_id=along(d), device_id_type=MESH)
    pl.semaphore_wait(barrier, 3 + n_z)

    own_load = pltpu.make_async_copy(own_ref, c_rows, local_sem.at[0])
    table_load = pltpu.make_async_copy(table_ref, table, local_sem.at[1])
    table_load.start()

    @pl.when(home)
    def _():
        ids_copy(1, across).start()
        ids_in[0] = ids_ref[...]

    @pl.when(away)
    def _():
        ids_copy(0, swap).start()
        ids_copy(1, partner).start()

    target_load = pltpu.make_async_copy(target_ref, target, local_sem.at[2])

    packed[0, :, pl.ds(owner_at, owner_span), :] = model_ref[...].astype(BF)
    packed[1, :, pl.ds(owner_at, owner_span), :] = control_ref[...].astype(BF)

    pack_copy().start()
    own_load.start()
    pl.when(home)(target_load.start)
    pack_copy().wait_recv()

    @pl.when(home)
    def _():
        for part in range(parts):
            model[part, own_rows, columns(p)] = packed[0, part].T
        for group in range(2):
            cross_copy(group).start()
        for part in range(parts):
            g_rows[part, :quarter, columns(p)] = packed[1, part].T[:quarter]

    @pl.when(away)
    def _():
        for part in range(parts):
            g_rows[part, quarter:, columns(p)] = packed[1, part].T[quarter:]

    send_tiles(g_along)
    g_beside(0, z).start()
    g_partner(0, z).start()
    for group in range(2):
        pl.when(away)(cross_copy(group).wait_recv)
        model_beside(group, 0, z).start()
        model_partner(group, 0, z).start()
    pl.when(away)(target_copy().start)

    ids_copy(1, across).wait_recv()
    pl.when(away)(ids_copy(0, swap).wait_recv)
    ids_load = pltpu.make_async_copy(ids_in, ids, local_sem.at[3])
    ids_load.start()
    ids_load.wait()
    table_load.wait()
    sublane = lax.broadcasted_iota(jnp.int32, (8, half), 0)

    def pick(slot, first, count, target_rows):
        def block(i, carry):
            at = (first + i) * 16
            eights = []
            for group in range(2):
                value = jnp.zeros((8, half), F32)
                for r in range(8):
                    token = ids[slot, 0, at + group * 8 + r]
                    aligned = token // 8
                    tile = table[aligned].astype(F32)
                    found = jnp.where(sublane == token - 8 * aligned, tile, 0.0)
                    line = jnp.sum(found, axis=0, keepdims=True)
                    value = jnp.where(sublane == r, line, value)
                eights.append(value)
            target_rows(
                pl.ds(pl.multiple_of(at, 16), 16), jnp.concatenate(eights, axis=0).astype(BF)
            )
            return carry

        lax.fori_loop(0, count, block, 0)

    def to_across(at, value):
        emb_out[at, :] = value

    def to_own(at, value):
        emb[at, emb_columns] = value

    n_blocks = rows // 16
    piece = n_blocks // 4

    def g_relay(i):
        d = turn(i)
        row = behind(d)
        g_along(d, row).wait_recv()
        hop_tile(g_along, d, row)
        g_beside(0, row).start()
        g_partner(0, row).start()

    def relay(group, i):
        d = turn(i)
        row = behind(d)
        model_along(group, d, row).wait_recv()
        hop_tile(functools.partial(model_along, group), d, row)
        model_beside(group, 0, row).start()
        model_partner(group, 0, row).start()

    def launch(group):
        send_tiles(functools.partial(model_along, group))

    pick(1, 0, 2 * piece, to_across)
    g_relay(1)
    launch(0)
    pick(1, 2 * piece, n_blocks - 2 * piece, to_across)
    emb_copy().start()
    for d in range(2, n_z):
        g_relay(d)
    launch(1)
    for row in range(n_z):
        if row < 2:
            pick(0, row * piece, piece, to_own)
        g_beside(1, row).wait_recv()
        g_partner(1, row).start()
    g_arrived = g_rows.at[:, pl.ds(pl.multiple_of(jnp.where(home, quarter, 0), quarter), quarter), :]
    remote(g_arrived, g_arrived, "gp", 0, partner).wait_recv()
    along_sent(lambda count: g_rows.at[:, g_own, pl.ds(0, count * span)], "gz")
    all_sent(g_rows.at[:, g_own, pl.ds(0, n_z * span)], "gy")
    all_sent(g_rows.at[:, g_own, :], "gp")
    own_load.wait()

    chunk = half // 6
    for part in (2, 0, 1):

        def correct(i, carry):
            at = pl.ds(pl.multiple_of(i * chunk, chunk), chunk)
            value = (g_rows[part, at, :].astype(F32) - c_rows[part, at, :]).astype(BF)
            corr[part, at, :] = value

            @pl.when(home)
            def _():
                role_corr[part, at, :] = value

            return carry

        lax.fori_loop(0, 6, correct, 0)

        @pl.when(away)
        def _():
            corr_copy(part).start()

    for d in range(1, n_z):
        relay(0, d)
    pick(0, 2 * piece, n_blocks - 2 * piece, to_own)
    emb_copy().wait_recv()
    block = rows // 5

    def normalise(i, carry):
        at = pl.ds(pl.multiple_of(i * block, block), block)
        widened = emb[at, :].astype(F32)
        inv_norm = lax.rsqrt(jnp.mean(widened * widened, axis=1, keepdims=True) + norm_eps)
        value = (widened * inv_norm * gain_ref[...][None, :]).astype(BF)
        normed[at, :] = value
        normed_t[:, at] = value.T
        return carry

    lax.fori_loop(0, 5, normalise, 0)

    def settle(group):
        for row in range(n_z):
            model_beside(group, 1, row).wait_recv()
            model_partner(group, 1, row).start()

    def arrive(group):
        first, count = groups[group]
        window = model.at[pl.ds(first, count), other_rows, :]
        remote(window, window, "mp", group, partner).wait_recv()

    settle(0)
    for d in range(1, n_z):
        relay(1, d)
    arrive(0)

    loss_scale = 1.0 / math.sqrt(2 * rows)
    n_tiles = width // TILE

    def tile_at(j):
        return pl.ds(pl.multiple_of(j * TILE, TILE), TILE)

    def half_product(left, left_rows, right, store):
        def product(j, carry):
            store(j, dot(left[left_rows, :], right[:, tile_at(j)]).astype(BF))
            return carry

        lax.fori_loop(0, n_tiles, product, 0, unroll=True)

    def local_step(step, weights, finish, between):
        def forward(j, carry):
            cols = tile_at(j)
            gate_act, slope = gelu_parts(dot(normed[...], weights[0, :, cols]))
            up_pre = dot(normed[...], weights[1, :, cols])
            act[:, cols] = gate_act.astype(BF)
            slope_up[:, cols] = (slope * up_pre).astype(BF)
            hidden[:, cols] = (gate_act * up_pre).astype(BF)
            return carry

        lax.fori_loop(0, n_tiles, forward, 0, unroll=True)
        if step == 0:
            settle(1)
            arrive(1)

            @pl.when(away)
            def _():
                target_copy().wait_recv()

            @pl.when(home)
            def _():
                target_load.wait()

        def project(j, carry):
            cols = tile_at(j)
            projected = dot(hidden[...], weights[2, cols, :], 1, 1)
            value = (
                (emb[:, cols].astype(F32) + projected - target[:, cols].astype(F32)) * loss_scale
            ).astype(BF)
            out_grad[:, cols] = value
            out_grad_t[cols, :] = value.T
            return carry

        lax.fori_loop(0, depth // TILE, project, 0, unroll=True)

        def term_other(part, left, right):
            def store(j, value):
                term_out[part, :, tile_at(j)] = value

            if step > 0:
                term_copy(step - 1, part).wait_send()
            half_product(left, other_rows, right, store)
            term_copy(step, part).start()

        def term_mine(part, left, right):
            def store(j, value):
                term_own[part, :, tile_at(j)] = value

            half_product(left, own_rows, right, store)

        term_other(2, out_grad_t, hidden)
        term_mine(2, out_grad_t, hidden)
        if step > 0:
            finish(2)

        def backward(j, carry):
            cols = tile_at(j)
            hidden_grad = dot(out_grad[...], weights[2, :, cols])
            gate_grad[:, cols] = (hidden_grad * slope_up[:, cols]).astype(BF)
            up_grad[:, cols] = (hidden_grad * act[:, cols]).astype(BF)
            return carry

        lax.fori_loop(0, n_tiles, backward, 0, unroll=True)
        if step == 0:
            finish(2)
        term_other(0, normed_t, gate_grad)
        term_other(1, normed_t, up_grad)
        between(0)
        term_mine(0, normed_t, gate_grad)
        between(1)
        term_mine(1, normed_t, up_grad)
        between(2)
        finish(0)
        finish(1)

    def update(part):
        term_copy(0, part).wait_recv()

        @pl.when(away)
        def _():
            corr_copy(part).wait_recv()

        def apply(i, carry):
            at = pl.ds(pl.multiple_of(i * chunk, chunk), chunk)
            model_at = pl.ds(pl.multiple_of(half_at + i * chunk, chunk), chunk)
            grads = term_own[part, at, :].astype(F32) + term_in[part, at, :].astype(F32)
            c_rows[part, at, :] = grads
            pseudo = grads + role_corr[part, at, :].astype(F32)
            current[part, model_at, :] = (
                model[part, model_at, :].astype(F32) - learning_rate * pseudo
            ).astype(BF)
            return carry

        lax.fori_loop(0, 6, apply, 0)
        current_copy(part).start()

    second = (steps_ref[role_client] > 1).astype(F32)

    def collect(part):
        term_copy(1, part).wait_recv()
        for s in range(n_sub):
            at = sub_rows(s)
            grads = term_own[part, at, :].astype(F32) + term_in[part, at, :].astype(F32)
            role_corr[part, at, :] = (c_rows[part, at, :] + second * grads).astype(BF)

            @pl.when(away)
            def _():
                return_copy(part, s).start()

    local_step(0, model, update, lambda k: None)
    pack_copy().wait_send()
    emb_copy().wait_send()
    ids_copy(1, across).wait_send()
    along_sent(lambda count: model.at[:, own_rows, pl.ds(0, count * span)], "mz")
    all_sent(model.at[:, own_rows, pl.ds(0, n_z * span)], "my")
    all_sent(model.at[:, own_rows, :], "mp")

    @pl.when(home)
    def _():
        all_sent(model.at[:, own_rows, columns(p)], "cross")

    @pl.when(away)
    def _():
        ids_copy(0, swap).wait_send()
        target_copy().wait_send()
        all_sent(corr, "corr")

    arrived = current.at[:, other_rows, :]
    remote(arrived, arrived, "cur", 0, partner).wait_recv()
    weight = weights_ref[client].astype(F32)
    taken = steps_ref[client].astype(F32)
    inverse = 1.0 / taken

    def place(k):
        return lax.rem(k // n_sub + parts - 1, parts), lax.rem(k, n_sub)

    def share(k):
        part, s = place(k)
        at = sub_rows(s)

        @pl.when(s == 0)
        def _():
            term_copy(1, part).wait_send()

        def spread(source):
            value = source[part, at, :].astype(F32)
            averaged = inverse * value
            summed = value + taken * corr[part, at, :].astype(F32)
            term_in[part, at, :] = averaged.astype(BF)
            mine = jnp.where(b == 0, summed, averaged)
            theirs = jnp.where(b == 0, averaged, summed)
            term_own[part, at, :] = (weight * mine).astype(BF)
            term_out[part, at, :] = (weight * theirs).astype(BF)

        @pl.when(home)
        def _():
            spread(role_corr)

        @pl.when(away)
        def _():
            return_copy(part, s).wait_recv()
            spread(g_rows)

        share_copy(part, s).start()
        grad_store(part, s).start()

    def split(k):
        part, s = place(k)
        at = sub_rows(s)
        share_copy(part, s).wait_recv()
        for row in range(n_z):
            for line in range(2):
                cols = columns(position(line, row))
                value = (
                    term_own[part, at, cols].astype(F32) + model[part, at, cols].astype(F32)
                ).astype(BF)
                if line == 0:
                    kept[k, row] = value
                else:
                    y_out[k, row] = value
        y_copy(k).start()

    def spread_z(k):
        y_copy(k).wait_recv()
        kept[k] = (kept[k].astype(F32) + y_in[k].astype(F32)).astype(BF)
        for d in range(1, n_z):
            z_copy(k, d).start()

    def gather_z(k):
        part, s = place(k)
        arrived = z_in.at[k, pl.ds(1, n_z - 1)]
        remote(arrived, arrived, "rz", k, partner).wait_recv()
        value = kept[k, z].astype(F32)
        for d in range(1, n_z):
            value += z_in[k, d].astype(F32)
        summed[part, sub_rows(s), :] = value
        @pl.when(s == n_sub - 1)
        def _():
            final[part] = summed[part].T
            final_copy(part).start()

    split_lag, y_lag, z_lag = 1, 3, 6

    def advance(k):
        @pl.when(k < n_chunks)
        def _():
            share(k)

        @pl.when((k >= split_lag) & (k - split_lag < n_chunks))
        def _():
            split(k - split_lag)

        @pl.when((k >= y_lag) & (k - y_lag < n_chunks))
        def _():
            spread_z(k - y_lag)

        @pl.when(k >= z_lag)
        def _():
            gather_z(k - z_lag)

    local_step(1, current, collect, advance)
    all_sent(current.at[:, own_rows, :], "cur")

    def loop(k, carry):
        advance(k)
        return carry

    lax.fori_loop(3, n_chunks + z_lag, loop, 0)

    weight_total = weights_ref[0]
    step_total = weights_ref[0] * steps_ref[0]
    for i in range(1, 2 * n_pos):
        weight_total += weights_ref[i]
        step_total += weights_ref[i] * steps_ref[i]
    weight_total = weight_total.astype(F32)
    step_total = step_total.astype(F32)
    control = control_ref[...]
    lost = step_total * (control - control.astype(BF).astype(F32))
    remote(final_in, final_in, "final", 0, partner).wait_recv()
    mine = final[:, pl.ds(owner_at, owner_span), :]
    theirs = final_in[...]
    step_out[...] = (jnp.where(b == 0, mine, theirs) + lost) / weight_total
    control_out[...] = jnp.where(b == 0, theirs, mine) / weight_total

    all_sent(final_in, "final")
    all_sent(y_out, "ry")
    all_sent(z_in.at[:, pl.ds(1, n_z - 1)], "rz")
    all_sent(term_out, "share")

    @pl.when(away)
    def _():
        all_sent(role_corr, "ret")

    pltpu.make_async_copy(term_in, grad_out, local_sem.at[4]).wait()


def widen_kernel(
    step_ref, control_ref, grad_ref, step_out, control_out, grad_out, narrow, wide, small, sem
):
    pieces = grad_ref.shape[0]
    pairs = [(step_ref, small.at[0]), (control_ref, small.at[1])]
    pairs += [(grad_ref.at[i], narrow.at[i]) for i in range(pieces)]
    loads = [pltpu.make_async_copy(src, dst, sem.at[0, i]) for i, (src, dst) in enumerate(pairs)]
    pairs = [(small.at[0], step_out), (small.at[1], control_out)]
    pairs += [(wide.at[i], grad_out.at[i]) for i in range(pieces)]
    stores = [pltpu.make_async_copy(src, dst, sem.at[1, i]) for i, (src, dst) in enumerate(pairs)]
    for load in loads:
        load.start()
    for i, (load, store) in enumerate(zip(loads, stores)):
        load.wait()
        if i >= 2:
            wide[i - 2] = narrow[i - 2].astype(F32)
        store.start()
    for store in stores:
        store.wait()


def paired_body(
    token_ids,
    target,
    embedding,
    norm_gain,
    global_model,
    global_control,
    client_control,
    local_steps,
    client_weight,
):
    n_clients = lax.axis_size("clients")
    n_pos = n_clients // 2
    n_z = n_pos // 2
    parts, half, owner_span = global_model.shape
    width = owner_span * n_clients
    span = 2 * owner_span
    rows = token_ids.shape[1]
    depth = 2 * half
    sub = 64
    n_chunks = parts * (half // sub)
    arrivals, n_send = semaphore_counts(parts, n_z, n_chunks)
    vmem = pltpu.VMEM
    scratch = [
        vmem((embedding.shape[0] // 8, 8, half), BF),
        vmem((2, 1, rows), jnp.int32),
        pltpu.SMEM((2, 1, rows), jnp.int32),
        vmem((rows, half), BF),
        vmem((2, parts, span, half), BF),
        vmem((parts, depth, width), BF),
        vmem((parts, depth, width), BF),
        vmem((parts, half, width), BF),
        vmem((parts, half, width), F32),
        vmem((parts, half, width), BF),
        vmem((parts, half, width), BF),
        vmem((rows, depth), BF),
        vmem((rows, depth), BF),
        vmem((rows, depth), BF),
        vmem((depth, rows), BF),
        vmem((rows, width), BF),
        vmem((rows, width), BF),
        vmem((rows, width), BF),
        vmem((rows, depth), BF),
        vmem((depth, rows), BF),
        vmem((rows, width), BF),
        vmem((rows, width), BF),
        vmem((parts, half, width), BF),
        vmem((parts, half, width), BF),
        vmem((parts, half, width), BF),
        vmem((n_chunks, n_z, sub, span), BF),
        vmem((n_chunks, n_z, sub, span), BF),
        vmem((n_chunks, n_z, sub, span), BF),
        vmem((n_chunks, n_z, sub, span), BF),
        vmem((parts, half, span), F32),
        vmem((parts, span, half), F32),
        vmem((parts, owner_span, half), F32),
        pltpu.SemaphoreType.DMA((5,)),
        pltpu.SemaphoreType.DMA((n_send,)),
        pltpu.SemaphoreType.DMA((sum(arrivals.values()),)),
    ]
    smem = pl.BlockSpec(memory_space=pltpu.SMEM)
    anywhere = pl.BlockSpec(memory_space=pl.ANY)
    inside = pl.BlockSpec(memory_space=pltpu.VMEM)
    step_sum, control_sum, grad_rows = pl.pallas_call(
        functools.partial(round_kernel, n_z),
        out_shape=(
            jax.ShapeDtypeStruct((parts, owner_span, half), F32),
            jax.ShapeDtypeStruct((parts, owner_span, half), F32),
            jax.ShapeDtypeStruct((parts, half, width), BF),
        ),
        in_specs=[smem, smem, inside, anywhere, anywhere, inside, inside, inside, anywhere],
        out_specs=(inside, inside, anywhere),
        scratch_shapes=scratch,
        compiler_params=pltpu.CompilerParams(
            collective_id=0, has_side_effects=True, vmem_limit_bytes=67043328
        ),
    )(
        local_steps,
        client_weight,
        token_ids,
        embedding.reshape(-1, 8, half),
        target[0],
        norm_gain,
        jnp.swapaxes(global_model, 1, 2),
        jnp.swapaxes(global_control, 1, 2),
        client_control[0],
    )
    pieces = 2 * parts
    block = parts * half // pieces
    step_sum, control_sum, update = pl.pallas_call(
        widen_kernel,
        out_shape=(
            jax.ShapeDtypeStruct((parts, owner_span, half), F32),
            jax.ShapeDtypeStruct((parts, owner_span, half), F32),
            jax.ShapeDtypeStruct((pieces, block, width), F32),
        ),
        in_specs=[anywhere, anywhere, anywhere],
        out_specs=(anywhere, anywhere, anywhere),
        scratch_shapes=[
            vmem((pieces, block, width), BF),
            vmem((pieces, block, width), F32),
            vmem((2, parts, owner_span, half), F32),
            pltpu.SemaphoreType.DMA((2, pieces + 2)),
        ],
    )(step_sum, control_sum, grad_rows.reshape(pieces, block, width))
    return (
        jnp.swapaxes(step_sum, 1, 2),
        jnp.swapaxes(control_sum, 1, 2),
        update.reshape(1, parts, half, width),
    )


def solution(mesh):
    placed = (
        P("clients", "fsdp"),
        P("clients", "fsdp", None),
        P(None, "fsdp"),
        P(),
        P(None, "fsdp", "clients"),
        P(None, "fsdp", "clients"),
        P("clients", None, "fsdp", None),
        P(),
        P(),
    )
    paired = mesh.shape["fsdp"] == 2 and mesh.shape["clients"] % 4 == 0
    return jax.shard_map(
        paired_body if paired else general_body,
        mesh=mesh,
        in_specs=placed,
        out_specs=(
            P(None, "fsdp", "clients"),
            P(None, "fsdp", "clients"),
            P("clients", None, "fsdp", None),
        ),
        check_vma=False,
    )
```

```python
import functools
import math

import jax
import jax.numpy as jnp
from jax import lax
from jax.experimental import pallas as pl
from jax.experimental.pallas import tpu as pltpu
from jax.sharding import PartitionSpec as P

LOCAL = 2


learning_rate = 0.005
norm_eps = 1e-06


def gelu_pair(pre_act):
    return jax.vjp(lambda inputs: jax.nn.gelu(inputs, approximate=True), pre_act)


def contract_rows(left, right):
    return lax.dot_general(
        left, right, (((0,), (0,)), ((), ())), preferred_element_type=jnp.float32
    )


def pack_owners(array, owners):
    parts, rows, columns = array.shape
    width = columns // owners
    split = array.reshape(parts, 2, rows // 2, owners, width)
    return split.transpose(3, 0, 2, 1, 4).reshape(owners, parts, rows // 2, 2 * width)


def unpack_owner(array):
    parts, half, width = array.shape
    split = array.reshape(parts, half, 2, width // 2)
    return split.transpose(0, 2, 1, 3).reshape(parts, 2 * half, width // 2)


def general_body(
    token_ids,
    target,
    embedding,
    norm_gain,
    global_model,
    global_control,
    client_control,
    local_steps,
    client_weight,
):
    n_clients = lax.axis_size("clients")
    n_fsdp = lax.axis_size("fsdp")
    client_index = lax.axis_index("clients")
    fsdp_index = lax.axis_index("fsdp")
    paired = n_fsdp == 2 and n_clients % 2 == 0
    if paired:
        core = client_index % 2
        role_client = client_index - core + fsdp_index
        block = core
        swap_pairs = [
            (c * 2 + f, ((c - c % 2) + f) * 2 + c % 2) for c in range(n_clients) for f in range(2)
        ]
        core_pairs = [(c, c ^ 1) for c in range(n_clients)]
    else:
        role_client = client_index
        block = fsdp_index

    def swap_roles(array):
        if not paired:
            return array
        return lax.ppermute(array, ("clients", "fsdp"), swap_pairs)

    def gather_rows(array):
        if not paired:
            return lax.all_gather(array, "fsdp", axis=0, tiled=True)
        other = lax.ppermute(array, "clients", core_pairs)
        return jnp.concatenate(
            [jnp.where(core == 0, array, other), jnp.where(core == 0, other, array)], axis=0
        )

    def reduce_rows(term):
        if not paired:
            return lax.psum_scatter(term, "fsdp", scatter_dimension=0, tiled=True).astype(
                jnp.float32
            )
        rows = term.shape[0] // 2
        own = lax.dynamic_slice_in_dim(term, core * rows, rows, axis=0)
        sent = lax.dynamic_slice_in_dim(term, (1 - core) * rows, rows, axis=0)
        received = lax.ppermute(sent, "clients", core_pairs)
        return own.astype(jnp.float32) + received.astype(jnp.float32)

    tok_rows = target.shape[1]
    group_rows = tok_rows * n_fsdp
    loss_scale = 1.0 / math.sqrt(group_rows)
    all_ids = lax.all_gather(swap_roles(token_ids), "fsdp", axis=1, tiled=True)
    emb_columns = jnp.take(embedding, all_ids[0], axis=0)
    embedded = lax.all_to_all(emb_columns, "fsdp", split_axis=0, concat_axis=1, tiled=True)
    widened = embedded.astype(jnp.float32)
    inv_norm = lax.rsqrt(jnp.mean(widened * widened, axis=1, keepdims=True) + norm_eps)
    normed = (widened * inv_norm * norm_gain).astype(jnp.bfloat16)
    target_rows = swap_roles(target[0]).astype(jnp.float32)
    model_columns = lax.all_gather(
        global_model.astype(jnp.bfloat16), "fsdp", axis=1, tiled=True
    )
    model_full = lax.all_gather(model_columns, "clients", axis=2, tiled=True)
    control_rows = lax.all_gather(
        global_control.astype(jnp.bfloat16), "clients", axis=2, tiled=True
    ).astype(global_control.dtype)
    slots = jnp.arange(local_steps.shape[0])
    step_count = jnp.sum(jnp.where(slots == client_index, local_steps, 0))
    role_steps = jnp.sum(jnp.where(slots == role_client, local_steps, 0))
    own_weight = jnp.sum(jnp.where(slots == client_index, client_weight, 0)).astype(jnp.float32)
    weight_total = jnp.sum(client_weight).astype(jnp.float32)
    correction = control_rows - client_control[0]
    parts, rows = correction.shape[0], correction.shape[1]
    role_correction = [
        swap_roles(correction[part].astype(jnp.bfloat16)).astype(jnp.float32)
        for part in range(parts)
    ]
    role_model = lax.dynamic_slice_in_dim(model_full, block * rows, rows, axis=1).astype(
        jnp.float32
    )
    gathered = [model_full[part] for part in range(parts)]
    pseudo = [jnp.zeros_like(role_correction[part]) for part in range(parts)]
    summed = [jnp.zeros_like(role_correction[part]) for part in range(parts)]
    for local_step in range(LOCAL):
        if local_step > 0:
            gathered = [
                gather_rows(
                    (role_model[part] - learning_rate * pseudo[part]).astype(jnp.bfloat16)
                )
                for part in range(parts)
            ]
        gate_pre = jnp.dot(normed, gathered[0], preferred_element_type=jnp.float32)
        up_pre = jnp.dot(normed, gathered[1], preferred_element_type=jnp.float32)
        gate_act, gelu_back = gelu_pair(gate_pre)
        hidden = (gate_act * up_pre).astype(jnp.bfloat16)
        projected = lax.dot_general(
            hidden, gathered[2], (((1,), (1,)), ((), ())), preferred_element_type=jnp.float32
        )
        out_grad = ((widened + projected - target_rows) * loss_scale).astype(jnp.bfloat16)
        outer_term = contract_rows(out_grad, hidden).astype(jnp.bfloat16)
        hidden_grad = jnp.dot(out_grad, gathered[2], preferred_element_type=jnp.float32)
        gate_grad = gelu_back(hidden_grad * up_pre)[0].astype(jnp.bfloat16)
        up_grad = (hidden_grad * gate_act).astype(jnp.bfloat16)
        gate_term = contract_rows(normed, gate_grad).astype(jnp.bfloat16)
        up_term = contract_rows(normed, up_grad).astype(jnp.bfloat16)
        grads = [reduce_rows(term) for term in (gate_term, up_term, outer_term)]
        step_mask = (local_step < role_steps).astype(jnp.float32)
        for part in range(parts):
            pseudo[part] = pseudo[part] + step_mask * (grads[part] + role_correction[part])
            summed[part] = summed[part] + step_mask * grads[part]
    own_grads = jnp.stack(
        [swap_roles(summed[part].astype(jnp.bfloat16)).astype(jnp.float32) for part in range(parts)]
    )
    taken = jnp.sum((jnp.arange(LOCAL) < step_count).astype(jnp.float32))
    own_pseudo = own_grads + taken * correction
    update = client_control[0] - control_rows + own_pseudo / step_count.astype(jnp.float32)
    packed = jnp.concatenate(
        [
            pack_owners((own_weight * own_pseudo).astype(jnp.bfloat16), n_clients),
            pack_owners((own_weight * update).astype(jnp.bfloat16), n_clients),
        ],
        axis=1,
    )
    sums = lax.psum_scatter(packed, "clients", scatter_dimension=0, tiled=True)[0]
    sums = unpack_owner(sums).astype(jnp.float32) / weight_total
    return (sums[:parts], sums[parts:], update[None])


MESH = pl.DeviceIdType.MESH
TILE = 256
BF = jnp.bfloat16
F32 = jnp.float32


def gelu_parts(x):
    cubic = 0.044715
    scale = math.sqrt(2.0 / math.pi)
    square = x * x
    t = jnp.tanh(scale * x * (1.0 + cubic * square))
    half = 0.5 * (1.0 + t)
    slope = half + (0.5 * scale) * x * (1.0 - t * t) * (1.0 + (3.0 * cubic) * square)
    return x * half, slope


def dot(left, right, left_dim=1, right_dim=0):
    return lax.dot_general(
        left, right, (((left_dim,), (right_dim,)), ((), ())), preferred_element_type=F32
    )


def semaphore_counts(parts, n_z, n_chunks):
    arrivals = dict(
        ids=2, pack=1, emb=1, target=1, cross=2, gz=n_z, gy=n_z, gp=1, mz=2 * n_z, my=2 * n_z,
        mp=2, corr=parts, term0=parts, term1=parts, cur=1, ret=n_chunks, share=n_chunks,
        ry=n_chunks, rz=n_chunks, final=1,
    )
    return arrivals, len(arrivals) + 2 * parts + 2


def round_kernel(
    n_z,
    steps_ref,
    weights_ref,
    ids_ref,
    table_ref,
    target_ref,
    gain_ref,
    model_ref,
    control_ref,
    own_ref,
    step_out,
    control_out,
    grad_out,
    table,
    ids_in,
    ids,
    emb_out,
    packed,
    model,
    current,
    g_rows,
    c_rows,
    corr,
    role_corr,
    emb,
    target,
    normed,
    normed_t,
    act,
    slope_up,
    hidden,
    out_grad,
    out_grad_t,
    gate_grad,
    up_grad,
    term_out,
    term_own,
    term_in,
    kept,
    y_out,
    y_in,
    z_in,
    summed,
    final,
    final_in,
    local_sem,
    send_sem,
    recv_sem,
):
    parts, half, width = own_ref.shape
    rows = emb.shape[0]
    depth = 2 * half
    n_pos = 2 * n_z
    span = width // n_pos
    owner_span = span // 2
    sub = kept.shape[2]
    n_sub = half // sub
    client = lax.axis_index("clients")
    x = lax.axis_index("fsdp")
    b = lax.rem(client, 2)
    p = client // 2
    y = lax.rem(p, 2)
    z = p // 2
    home = b == x
    away = b != x
    role_client = 2 * p + x
    half_at = pl.multiple_of(b * half, half)
    other_at = pl.multiple_of((1 - b) * half, half)
    own_rows = pl.ds(half_at, half)
    other_rows = pl.ds(other_at, half)
    owner_at = pl.multiple_of(b * owner_span, owner_span)

    partner = {"clients": 2 * p + 1 - b, "fsdp": x}
    across = {"clients": client, "fsdp": 1 - x}
    swap = {"clients": 2 * p + 1 - b, "fsdp": 1 - x}
    beside = {"clients": 2 * (2 * z + 1 - y) + b, "fsdp": x}

    def along(d):
        return {"clients": 2 * (2 * lax.rem(z + d, n_z) + y) + b, "fsdp": x}

    def behind(d):
        return lax.rem(z + n_z - d, n_z)

    hop = n_z == 4

    def turn(i):
        return jnp.where(z == 0, n_z - i, i) if hop else i

    def send_tiles(copy):
        for d in range(1, n_z):
            if not hop or d == 2:
                copy(d, z).start()
            else:
                pl.when(z != (n_z - 1 if d == 1 else 0))(copy(d, z).start)

    def hop_tile(copy, d, row):
        if hop:
            pl.when((d == 2) & (z == 1))(copy(1, row, -1).start)
            pl.when((d == 2) & (z == 2))(copy(3, row, 1).start)

    def along_sent(window, name):
        if hop:
            ends = (z == 0) | (z == n_z - 1)

            @pl.when(ends)
            def _():
                all_sent(window(n_z - 2), name)

            @pl.when(jnp.logical_not(ends))
            def _():
                all_sent(window(n_z), name)

        else:
            all_sent(window(n_z - 1), name)

    def position(line, row):
        return 2 * row + (y if line == 0 else 1 - y)

    def columns(pos):
        return pl.ds(pl.multiple_of(pos * span, span), span)

    n_chunks = parts * n_sub
    groups = ((0, parts - 1), (parts - 1, 1))
    arrivals, _ = semaphore_counts(parts, n_z, n_chunks)
    base = {}
    total = 0
    for name, count in arrivals.items():
        base[name] = total
        total += count
    kinds = list(arrivals)

    def remote(src, dst, name, index, device, leave=None):
        if leave is None:
            leave = kinds.index(name)
        return pltpu.make_async_remote_copy(
            src_ref=src, dst_ref=dst, send_sem=send_sem.at[leave],
            recv_sem=recv_sem.at[base[name] + index],
            device_id=device, device_id_type=MESH,
        )

    def all_sent(window, name):
        remote(window, window, name, 0, partner).wait_send()

    def pack_copy():
        window = packed.at[:, :, pl.ds(owner_at, owner_span), :]
        return remote(window, window, "pack", 0, partner)

    emb_columns = pl.ds(pl.multiple_of(x * half, half), half)

    def ids_copy(slot, device):
        return remote(
            ids_ref, ids_in.at[slot], "ids", slot, device, len(kinds) + 2 * parts + slot
        )

    def emb_copy():
        return remote(
            emb_out, emb.at[:, emb_columns], "emb", 0, across,
        )

    def target_copy():
        return remote(target_ref, target, "target", 0, swap)

    quarter = half // 2
    g_own = pl.ds(pl.multiple_of(jnp.where(home, 0, quarter), quarter), quarter)

    def g_window(pos):
        return g_rows.at[:, g_own, columns(pos)]

    def model_window(group, pos):
        first, count = groups[group]
        return model.at[pl.ds(first, count), own_rows, columns(pos)]

    def g_along(d, row, step=None):
        window = g_window(position(0, row))
        return remote(window, window, "gz", d, along(d) if step is None else along(step + n_z))

    def g_beside(line, row):
        window = g_window(position(line, row))
        return remote(window, window, "gy", row, beside)

    def g_partner(line, row):
        window = g_window(position(line, row))
        return remote(window, window, "gp", 0, partner)

    def cross_copy(group):
        window = model_window(group, p)
        return remote(window, window, "cross", group, across)

    def model_along(group, d, row, step=None):
        window = model_window(group, position(0, row))
        return remote(
            window, window, "mz", group * n_z + d,
            along(d) if step is None else along(step + n_z),
        )

    def model_beside(group, line, row):
        window = model_window(group, position(line, row))
        return remote(window, window, "my", group * n_z + row, beside)

    def model_partner(group, line, row):
        window = model_window(group, position(line, row))
        return remote(window, window, "mp", group, partner)

    def corr_copy(part):
        return remote(corr.at[part], role_corr.at[part], "corr", part, swap)

    def term_copy(step, part):
        return remote(
            term_out.at[part], term_in.at[part], "term%d" % step, part, partner,
            len(kinds) + step * parts + part,
        )

    def current_copy(part):
        window = current.at[part, own_rows, :]
        return remote(window, window, "cur", 0, partner)

    def sub_rows(s):
        return pl.ds(pl.multiple_of(s * sub, sub), sub)

    def return_copy(part, s):
        return remote(
            role_corr.at[part, sub_rows(s), :], g_rows.at[part, sub_rows(s), :],
            "ret", part * n_sub + s, swap,
        )

    def share_copy(part, s):
        return remote(
            term_out.at[part, sub_rows(s), :], model.at[part, sub_rows(s), :],
            "share", part * n_sub + s, partner,
        )

    def y_copy(k):
        return remote(y_out.at[k], y_in.at[k], "ry", k, beside)

    def z_copy(k, d):
        return remote(
            kept.at[k, lax.rem(z + d, n_z)], z_in.at[k, d], "rz", k, along(d)
        )

    def final_copy(part):
        at = pl.ds(pl.multiple_of((1 - b) * owner_span, owner_span), owner_span)
        return remote(final.at[part, at, :], final_in.at[part], "final", 0, partner)

    def grad_store(part, s):
        return pltpu.make_async_copy(
            term_in.at[part, sub_rows(s), :], grad_out.at[part, sub_rows(s), :],
            local_sem.at[4],
        )

    barrier = pltpu.get_barrier_semaphore()
    for peer in [partner, across, swap, beside]:
        pl.semaphore_signal(barrier, inc=1, device_id=peer, device_id_type=MESH)
    for d in range(1, n_z):
        pl.semaphore_signal(barrier, inc=1, device_id=along(d), device_id_type=MESH)
    pl.semaphore_wait(barrier, 3 + n_z)

    own_load = pltpu.make_async_copy(own_ref, c_rows, local_sem.at[0])
    table_load = pltpu.make_async_copy(table_ref, table, local_sem.at[1])
    table_load.start()

    @pl.when(home)
    def _():
        ids_copy(1, across).start()
        ids_in[0] = ids_ref[...]

    @pl.when(away)
    def _():
        ids_copy(0, swap).start()
        ids_copy(1, partner).start()

    target_load = pltpu.make_async_copy(target_ref, target, local_sem.at[2])

    packed[0, :, pl.ds(owner_at, owner_span), :] = model_ref[...].astype(BF)
    packed[1, :, pl.ds(owner_at, owner_span), :] = control_ref[...].astype(BF)

    pack_copy().start()
    own_load.start()
    pl.when(home)(target_load.start)
    pack_copy().wait_recv()

    @pl.when(home)
    def _():
        for part in range(parts):
            model[part, own_rows, columns(p)] = packed[0, part].T
        for group in range(2):
            cross_copy(group).start()
        for part in range(parts):
            g_rows[part, :quarter, columns(p)] = packed[1, part].T[:quarter]

    @pl.when(away)
    def _():
        for part in range(parts):
            g_rows[part, quarter:, columns(p)] = packed[1, part].T[quarter:]

    send_tiles(g_along)
    g_beside(0, z).start()
    g_partner(0, z).start()
    for group in range(2):
        pl.when(away)(cross_copy(group).wait_recv)
        model_beside(group, 0, z).start()
        model_partner(group, 0, z).start()
    pl.when(away)(target_copy().start)

    ids_copy(1, across).wait_recv()
    pl.when(away)(ids_copy(0, swap).wait_recv)
    ids_load = pltpu.make_async_copy(ids_in, ids, local_sem.at[3])
    ids_load.start()
    ids_load.wait()
    table_load.wait()
    sublane = lax.broadcasted_iota(jnp.int32, (8, half), 0)

    def pick(slot, first, count, target_rows):
        def block(i, carry):
            at = (first + i) * 16
            eights = []
            for group in range(2):
                value = jnp.zeros((8, half), F32)
                for r in range(8):
                    token = ids[slot, 0, at + group * 8 + r]
                    aligned = token // 8
                    tile = table[aligned].astype(F32)
                    found = jnp.where(sublane == token - 8 * aligned, tile, 0.0)
                    line = jnp.sum(found, axis=0, keepdims=True)
                    value = jnp.where(sublane == r, line, value)
                eights.append(value)
            target_rows(
                pl.ds(pl.multiple_of(at, 16), 16), jnp.concatenate(eights, axis=0).astype(BF)
            )
            return carry

        lax.fori_loop(0, count, block, 0)

    def to_across(at, value):
        emb_out[at, :] = value

    def to_own(at, value):
        emb[at, emb_columns] = value

    n_blocks = rows // 16
    piece = n_blocks // 4

    def g_relay(i):
        d = turn(i)
        row = behind(d)
        g_along(d, row).wait_recv()
        hop_tile(g_along, d, row)
        g_beside(0, row).start()
        g_partner(0, row).start()

    def relay(group, i):
        d = turn(i)
        row = behind(d)
        model_along(group, d, row).wait_recv()
        hop_tile(functools.partial(model_along, group), d, row)
        model_beside(group, 0, row).start()
        model_partner(group, 0, row).start()

    def launch(group):
        send_tiles(functools.partial(model_along, group))

    pick(1, 0, 2 * piece, to_across)
    g_relay(1)
    launch(0)
    pick(1, 2 * piece, n_blocks - 2 * piece, to_across)
    emb_copy().start()
    for d in range(2, n_z):
        g_relay(d)
    launch(1)
    for row in range(n_z):
        if row < 2:
            pick(0, row * piece, piece, to_own)
        g_beside(1, row).wait_recv()
        g_partner(1, row).start()
    g_arrived = g_rows.at[:, pl.ds(pl.multiple_of(jnp.where(home, quarter, 0), quarter), quarter), :]
    remote(g_arrived, g_arrived, "gp", 0, partner).wait_recv()
    along_sent(lambda count: g_rows.at[:, g_own, pl.ds(0, count * span)], "gz")
    all_sent(g_rows.at[:, g_own, pl.ds(0, n_z * span)], "gy")
    all_sent(g_rows.at[:, g_own, :], "gp")
    own_load.wait()

    chunk = half // 6
    for part in (2, 0, 1):

        def correct(i, carry):
            at = pl.ds(pl.multiple_of(i * chunk, chunk), chunk)
            value = (g_rows[part, at, :].astype(F32) - c_rows[part, at, :]).astype(BF)
            corr[part, at, :] = value

            @pl.when(home)
            def _():
                role_corr[part, at, :] = value

            return carry

        lax.fori_loop(0, 6, correct, 0)

        @pl.when(away)
        def _():
            corr_copy(part).start()

    for d in range(1, n_z):
        relay(0, d)
    pick(0, 2 * piece, n_blocks - 2 * piece, to_own)
    emb_copy().wait_recv()
    block = rows // 5

    def normalise(i, carry):
        at = pl.ds(pl.multiple_of(i * block, block), block)
        widened = emb[at, :].astype(F32)
        inv_norm = lax.rsqrt(jnp.mean(widened * widened, axis=1, keepdims=True) + norm_eps)
        value = (widened * inv_norm * gain_ref[...][None, :]).astype(BF)
        normed[at, :] = value
        normed_t[:, at] = value.T
        return carry

    lax.fori_loop(0, 5, normalise, 0)

    def settle(group):
        for row in range(n_z):
            model_beside(group, 1, row).wait_recv()
            model_partner(group, 1, row).start()

    def arrive(group):
        first, count = groups[group]
        window = model.at[pl.ds(first, count), other_rows, :]
        remote(window, window, "mp", group, partner).wait_recv()

    settle(0)
    for d in range(1, n_z):
        relay(1, d)
    arrive(0)

    loss_scale = 1.0 / math.sqrt(2 * rows)
    n_tiles = width // TILE

    def tile_at(j):
        return pl.ds(pl.multiple_of(j * TILE, TILE), TILE)

    def half_product(left, left_rows, right, store):
        def product(j, carry):
            store(j, dot(left[left_rows, :], right[:, tile_at(j)]).astype(BF))
            return carry

        lax.fori_loop(0, n_tiles, product, 0, unroll=True)

    def local_step(step, weights, finish, between):
        def forward(j, carry):
            cols = tile_at(j)
            gate_act, slope = gelu_parts(dot(normed[...], weights[0, :, cols]))
            up_pre = dot(normed[...], weights[1, :, cols])
            act[:, cols] = gate_act.astype(BF)
            slope_up[:, cols] = (slope * up_pre).astype(BF)
            hidden[:, cols] = (gate_act * up_pre).astype(BF)
            return carry

        lax.fori_loop(0, n_tiles, forward, 0, unroll=True)
        if step == 0:
            settle(1)
            arrive(1)

            @pl.when(away)
            def _():
                target_copy().wait_recv()

            @pl.when(home)
            def _():
                target_load.wait()

        def project(j, carry):
            cols = tile_at(j)
            projected = dot(hidden[...], weights[2, cols, :], 1, 1)
            value = (
                (emb[:, cols].astype(F32) + projected - target[:, cols].astype(F32)) * loss_scale
            ).astype(BF)
            out_grad[:, cols] = value
            out_grad_t[cols, :] = value.T
            return carry

        lax.fori_loop(0, depth // TILE, project, 0, unroll=True)

        def term_other(part, left, right):
            def store(j, value):
                term_out[part, :, tile_at(j)] = value

            if step > 0:
                term_copy(step - 1, part).wait_send()
            half_product(left, other_rows, right, store)
            term_copy(step, part).start()

        def term_mine(part, left, right):
            def store(j, value):
                term_own[part, :, tile_at(j)] = value

            half_product(left, own_rows, right, store)

        term_other(2, out_grad_t, hidden)
        term_mine(2, out_grad_t, hidden)
        if step > 0:
            finish(2)

        def backward(j, carry):
            cols = tile_at(j)
            hidden_grad = dot(out_grad[...], weights[2, :, cols])
            gate_grad[:, cols] = (hidden_grad * slope_up[:, cols]).astype(BF)
            up_grad[:, cols] = (hidden_grad * act[:, cols]).astype(BF)
            return carry

        lax.fori_loop(0, n_tiles, backward, 0, unroll=True)
        if step == 0:
            finish(2)
        term_other(0, normed_t, gate_grad)
        term_other(1, normed_t, up_grad)
        between(0)
        term_mine(0, normed_t, gate_grad)
        between(1)
        term_mine(1, normed_t, up_grad)
        between(2)
        finish(0)
        finish(1)

    def update(part):
        term_copy(0, part).wait_recv()

        @pl.when(away)
        def _():
            corr_copy(part).wait_recv()

        def apply(i, carry):
            at = pl.ds(pl.multiple_of(i * chunk, chunk), chunk)
            model_at = pl.ds(pl.multiple_of(half_at + i * chunk, chunk), chunk)
            grads = term_own[part, at, :].astype(F32) + term_in[part, at, :].astype(F32)
            c_rows[part, at, :] = grads
            pseudo = grads + role_corr[part, at, :].astype(F32)
            current[part, model_at, :] = (
                model[part, model_at, :].astype(F32) - learning_rate * pseudo
            ).astype(BF)
            return carry

        lax.fori_loop(0, 6, apply, 0)
        current_copy(part).start()

    second = (steps_ref[role_client] > 1).astype(F32)

    def collect(part):
        term_copy(1, part).wait_recv()
        for s in range(n_sub):
            at = sub_rows(s)
            grads = term_own[part, at, :].astype(F32) + term_in[part, at, :].astype(F32)
            role_corr[part, at, :] = (c_rows[part, at, :] + second * grads).astype(BF)

            @pl.when(away)
            def _():
                return_copy(part, s).start()

    local_step(0, model, update, lambda k: None)
    pack_copy().wait_send()
    emb_copy().wait_send()
    ids_copy(1, across).wait_send()
    along_sent(lambda count: model.at[:, own_rows, pl.ds(0, count * span)], "mz")
    all_sent(model.at[:, own_rows, pl.ds(0, n_z * span)], "my")
    all_sent(model.at[:, own_rows, :], "mp")

    @pl.when(home)
    def _():
        all_sent(model.at[:, own_rows, columns(p)], "cross")

    @pl.when(away)
    def _():
        ids_copy(0, swap).wait_send()
        target_copy().wait_send()
        all_sent(corr, "corr")

    arrived = current.at[:, other_rows, :]
    remote(arrived, arrived, "cur", 0, partner).wait_recv()
    weight = weights_ref[client].astype(F32)
    taken = steps_ref[client].astype(F32)
    inverse = 1.0 / taken

    def place(k):
        return lax.rem(k // n_sub + parts - 1, parts), lax.rem(k, n_sub)

    def share(k):
        part, s = place(k)
        at = sub_rows(s)

        @pl.when(s == 0)
        def _():
            term_copy(1, part).wait_send()

        def spread(source):
            value = source[part, at, :].astype(F32)
            averaged = inverse * value
            summed = value + taken * corr[part, at, :].astype(F32)
            term_in[part, at, :] = averaged.astype(BF)
            mine = jnp.where(b == 0, summed, averaged)
            theirs = jnp.where(b == 0, averaged, summed)
            term_own[part, at, :] = (weight * mine).astype(BF)
            term_out[part, at, :] = (weight * theirs).astype(BF)

        @pl.when(home)
        def _():
            spread(role_corr)

        @pl.when(away)
        def _():
            return_copy(part, s).wait_recv()
            spread(g_rows)

        share_copy(part, s).start()
        grad_store(part, s).start()

    def split(k):
        part, s = place(k)
        at = sub_rows(s)
        share_copy(part, s).wait_recv()
        for row in range(n_z):
            for line in range(2):
                cols = columns(position(line, row))
                value = (
                    term_own[part, at, cols].astype(F32) + model[part, at, cols].astype(F32)
                ).astype(BF)
                if line == 0:
                    kept[k, row] = value
                else:
                    y_out[k, row] = value
        y_copy(k).start()

    def spread_z(k):
        y_copy(k).wait_recv()
        kept[k] = (kept[k].astype(F32) + y_in[k].astype(F32)).astype(BF)
        for d in range(1, n_z):
            z_copy(k, d).start()

    def gather_z(k):
        part, s = place(k)
        arrived = z_in.at[k, pl.ds(1, n_z - 1)]
        remote(arrived, arrived, "rz", k, partner).wait_recv()
        value = kept[k, z].astype(F32)
        for d in range(1, n_z):
            value += z_in[k, d].astype(F32)
        summed[part, sub_rows(s), :] = value
        @pl.when(s == n_sub - 1)
        def _():
            final[part] = summed[part].T
            final_copy(part).start()

    split_lag, y_lag, z_lag = 1, 4, 8

    def advance(k):
        @pl.when(k < n_chunks)
        def _():
            share(k)

        @pl.when((k >= split_lag) & (k - split_lag < n_chunks))
        def _():
            split(k - split_lag)

        @pl.when((k >= y_lag) & (k - y_lag < n_chunks))
        def _():
            spread_z(k - y_lag)

        @pl.when(k >= z_lag)
        def _():
            gather_z(k - z_lag)

    local_step(1, current, collect, advance)
    all_sent(current.at[:, own_rows, :], "cur")

    def loop(k, carry):
        advance(k)
        return carry

    lax.fori_loop(3, n_chunks + z_lag, loop, 0)

    weight_total = weights_ref[0]
    step_total = weights_ref[0] * steps_ref[0]
    for i in range(1, 2 * n_pos):
        weight_total += weights_ref[i]
        step_total += weights_ref[i] * steps_ref[i]
    weight_total = weight_total.astype(F32)
    step_total = step_total.astype(F32)
    control = control_ref[...]
    lost = step_total * (control - control.astype(BF).astype(F32))
    remote(final_in, final_in, "final", 0, partner).wait_recv()
    mine = final[:, pl.ds(owner_at, owner_span), :]
    theirs = final_in[...]
    step_out[...] = (jnp.where(b == 0, mine, theirs) + lost) / weight_total
    control_out[...] = jnp.where(b == 0, theirs, mine) / weight_total

    all_sent(final_in, "final")
    all_sent(y_out, "ry")
    all_sent(z_in.at[:, pl.ds(1, n_z - 1)], "rz")
    all_sent(term_out, "share")

    @pl.when(away)
    def _():
        all_sent(role_corr, "ret")

    pltpu.make_async_copy(term_in, grad_out, local_sem.at[4]).wait()


def widen_kernel(
    step_ref, control_ref, grad_ref, step_out, control_out, grad_out, narrow, wide, small, sem
):
    pieces = grad_ref.shape[0]
    pairs = [(step_ref, small.at[0]), (control_ref, small.at[1])]
    pairs += [(grad_ref.at[i], narrow.at[i]) for i in range(pieces)]
    loads = [pltpu.make_async_copy(src, dst, sem.at[0, i]) for i, (src, dst) in enumerate(pairs)]
    pairs = [(small.at[0], step_out), (small.at[1], control_out)]
    pairs += [(wide.at[i], grad_out.at[i]) for i in range(pieces)]
    stores = [pltpu.make_async_copy(src, dst, sem.at[1, i]) for i, (src, dst) in enumerate(pairs)]
    for load in loads:
        load.start()
    for i, (load, store) in enumerate(zip(loads, stores)):
        load.wait()
        if i >= 2:
            wide[i - 2] = narrow[i - 2].astype(F32)
        store.start()
    for store in stores:
        store.wait()


def paired_body(
    token_ids,
    target,
    embedding,
    norm_gain,
    global_model,
    global_control,
    client_control,
    local_steps,
    client_weight,
):
    n_clients = lax.axis_size("clients")
    n_pos = n_clients // 2
    n_z = n_pos // 2
    parts, half, owner_span = global_model.shape
    width = owner_span * n_clients
    span = 2 * owner_span
    rows = token_ids.shape[1]
    depth = 2 * half
    sub = 64
    n_chunks = parts * (half // sub)
    arrivals, n_send = semaphore_counts(parts, n_z, n_chunks)
    vmem = pltpu.VMEM
    scratch = [
        vmem((embedding.shape[0] // 8, 8, half), BF),
        vmem((2, 1, rows), jnp.int32),
        pltpu.SMEM((2, 1, rows), jnp.int32),
        vmem((rows, half), BF),
        vmem((2, parts, span, half), BF),
        vmem((parts, depth, width), BF),
        vmem((parts, depth, width), BF),
        vmem((parts, half, width), BF),
        vmem((parts, half, width), F32),
        vmem((parts, half, width), BF),
        vmem((parts, half, width), BF),
        vmem((rows, depth), BF),
        vmem((rows, depth), BF),
        vmem((rows, depth), BF),
        vmem((depth, rows), BF),
        vmem((rows, width), BF),
        vmem((rows, width), BF),
        vmem((rows, width), BF),
        vmem((rows, depth), BF),
        vmem((depth, rows), BF),
        vmem((rows, width), BF),
        vmem((rows, width), BF),
        vmem((parts, half, width), BF),
        vmem((parts, half, width), BF),
        vmem((parts, half, width), BF),
        vmem((n_chunks, n_z, sub, span), BF),
        vmem((n_chunks, n_z, sub, span), BF),
        vmem((n_chunks, n_z, sub, span), BF),
        vmem((n_chunks, n_z, sub, span), BF),
        vmem((parts, half, span), F32),
        vmem((parts, span, half), F32),
        vmem((parts, owner_span, half), F32),
        pltpu.SemaphoreType.DMA((5,)),
        pltpu.SemaphoreType.DMA((n_send,)),
        pltpu.SemaphoreType.DMA((sum(arrivals.values()),)),
    ]
    smem = pl.BlockSpec(memory_space=pltpu.SMEM)
    anywhere = pl.BlockSpec(memory_space=pl.ANY)
    inside = pl.BlockSpec(memory_space=pltpu.VMEM)
    step_sum, control_sum, grad_rows = pl.pallas_call(
        functools.partial(round_kernel, n_z),
        out_shape=(
            jax.ShapeDtypeStruct((parts, owner_span, half), F32),
            jax.ShapeDtypeStruct((parts, owner_span, half), F32),
            jax.ShapeDtypeStruct((parts, half, width), BF),
        ),
        in_specs=[smem, smem, inside, anywhere, anywhere, inside, inside, inside, anywhere],
        out_specs=(inside, inside, anywhere),
        scratch_shapes=scratch,
        compiler_params=pltpu.CompilerParams(
            collective_id=0, has_side_effects=True, vmem_limit_bytes=67043328
        ),
    )(
        local_steps,
        client_weight,
        token_ids,
        embedding.reshape(-1, 8, half),
        target[0],
        norm_gain,
        jnp.swapaxes(global_model, 1, 2),
        jnp.swapaxes(global_control, 1, 2),
        client_control[0],
    )
    pieces = 2 * parts
    block = parts * half // pieces
    step_sum, control_sum, update = pl.pallas_call(
        widen_kernel,
        out_shape=(
            jax.ShapeDtypeStruct((parts, owner_span, half), F32),
            jax.ShapeDtypeStruct((parts, owner_span, half), F32),
            jax.ShapeDtypeStruct((pieces, block, width), F32),
        ),
        in_specs=[anywhere, anywhere, anywhere],
        out_specs=(anywhere, anywhere, anywhere),
        scratch_shapes=[
            vmem((pieces, block, width), BF),
            vmem((pieces, block, width), F32),
            vmem((2, parts, owner_span, half), F32),
            pltpu.SemaphoreType.DMA((2, pieces + 2)),
        ],
    )(step_sum, control_sum, grad_rows.reshape(pieces, block, width))
    return (
        jnp.swapaxes(step_sum, 1, 2),
        jnp.swapaxes(control_sum, 1, 2),
        update.reshape(1, parts, half, width),
    )


def solution(mesh):
    placed = (
        P("clients", "fsdp"),
        P("clients", "fsdp", None),
        P(None, "fsdp"),
        P(),
        P(None, "fsdp", "clients"),
        P(None, "fsdp", "clients"),
        P("clients", None, "fsdp", None),
        P(),
        P(),
    )
    paired = mesh.shape["fsdp"] == 2 and mesh.shape["clients"] % 4 == 0
    return jax.shard_map(
        paired_body if paired else general_body,
        mesh=mesh,
        in_specs=placed,
        out_specs=(
            P(None, "fsdp", "clients"),
            P(None, "fsdp", "clients"),
            P("clients", None, "fsdp", None),
        ),
        check_vma=False,
    )
```
